8 devices in a mesh: col: 4 (over z, y, x), row: 2 (over core).
Axes of the slice: x: 2, y: 2, z: 1, core: 2. Of those that a mesh axis runs over, the one named last changes fastest.
Arguments:
- f_rhs: float32 [64, 128, 512], P('row', 'col')
- u_init: float32 [64, 128, 512], P('row', 'col')
- kappa_cell: float32 [64, 128], P('row', 'col')
- solve_mats: bfloat16 [2, 4, 1024, 1600], P('row', 'col')
- omega_relax: float32 [], replicated
Outputs:
- output: float32 [64, 128, 512], P('row', 'col')
All inputs are finite; a program needn't handle non-finite values.
Results may differ from the reference program's by a relative error of at most 0.00175602.
Values are sent between devices in bfloat16 or wider.
A program may use at most 1 GiB of HBM per device.

```python
import jax
import jax.numpy as jnp
from jax import lax

SUB_SIZE = 32
MARGIN = 4
RHS_COUNT = 512
ROW_BLOCKS = 2
COL_BLOCKS = 4
SWEEPS = 6

EXT_SIZE = SUB_SIZE + 2 * MARGIN
GRID_ROWS = SUB_SIZE * ROW_BLOCKS
GRID_COLS = SUB_SIZE * COL_BLOCKS


def face_coeffs(kappa_cell):
    inner_v = 0.5 * (kappa_cell[1:, :] + kappa_cell[:-1, :])
    inner_h = 0.5 * (kappa_cell[:, 1:] + kappa_cell[:, :-1])
    face_n = jnp.concatenate([kappa_cell[:1, :], inner_v], axis=0)
    face_s = jnp.concatenate([inner_v, kappa_cell[-1:, :]], axis=0)
    face_w = jnp.concatenate([kappa_cell[:, :1], inner_h], axis=1)
    face_e = jnp.concatenate([inner_h, kappa_cell[:, -1:]], axis=1)
    return face_n, face_s, face_w, face_e


def apply_operator(values, face_set):
    face_n, face_s, face_w, face_e = face_set
    padded = jnp.pad(values, ((1, 1), (1, 1), (0, 0)))
    diag_sum = (face_n + face_s + face_w + face_e)[:, :, None]
    return (diag_sum * values
            - face_n[:, :, None] * padded[:-2, 1:-1]
            - face_s[:, :, None] * padded[2:, 1:-1]
            - face_w[:, :, None] * padded[1:-1, :-2]
            - face_e[:, :, None] * padded[1:-1, 2:])


def build_solve_mats(kappa_cell):
    face_n, face_s, face_w, face_e = face_coeffs(kappa_cell)
    diag_sum = face_n + face_s + face_w + face_e
    link_s = jnp.concatenate([face_s[:-1, :], jnp.zeros((1, GRID_COLS), jnp.float32)], axis=0)
    link_e = jnp.concatenate([face_e[:, :-1], jnp.zeros((GRID_ROWS, 1), jnp.float32)], axis=1)
    pad_cfg = ((MARGIN, MARGIN), (MARGIN, MARGIN))
    diag_pad = jnp.pad(diag_sum, pad_cfg, constant_values=1.0)
    south_pad = jnp.pad(link_s, pad_cfg)
    east_pad = jnp.pad(link_e, pad_cfg)
    ext_cells = EXT_SIZE * EXT_SIZE
    col_mask = (jnp.arange(EXT_SIZE) < EXT_SIZE - 1).astype(jnp.float32)

    def one_block(block_idx):
        corner_at = (block_idx // COL_BLOCKS * SUB_SIZE, block_idx % COL_BLOCKS * SUB_SIZE)
        diag_w = lax.dynamic_slice(diag_pad, corner_at, (EXT_SIZE, EXT_SIZE)).reshape(ext_cells)
        south_w = lax.dynamic_slice(south_pad, corner_at, (EXT_SIZE, EXT_SIZE)).reshape(ext_cells)
        east_w = (lax.dynamic_slice(east_pad, corner_at, (EXT_SIZE, EXT_SIZE)) * col_mask[None, :]).reshape(ext_cells)
        local_op = (jnp.diag(diag_w)
                    - jnp.diag(east_w[:-1], 1) - jnp.diag(east_w[:-1], -1)
                    - jnp.diag(south_w[:-EXT_SIZE], EXT_SIZE) - jnp.diag(south_w[:-EXT_SIZE], -EXT_SIZE))
        inverse = jnp.linalg.inv(local_op).reshape(EXT_SIZE, EXT_SIZE, ext_cells)
        rows_kept = inverse[MARGIN:MARGIN + SUB_SIZE, MARGIN:MARGIN + SUB_SIZE]
        return rows_kept.reshape(SUB_SIZE * SUB_SIZE, ext_cells)

    all_mats = lax.map(one_block, jnp.arange(ROW_BLOCKS * COL_BLOCKS))
    return all_mats.reshape(ROW_BLOCKS, COL_BLOCKS, SUB_SIZE * SUB_SIZE, ext_cells).astype(jnp.bfloat16)


def setup_inputs(seed: int = 0) -> dict:
    root_key = jax.random.key(seed)
    key_rhs, key_init, key_coef, key_omega = jax.random.split(root_key, 4)
    rhs_scale = 16.0 / (EXT_SIZE * EXT_SIZE)
    grid_shape = (GRID_ROWS, GRID_COLS, RHS_COUNT)
    f_rhs = rhs_scale * (1.0 + jax.random.normal(key_rhs, grid_shape, jnp.float32))
    u_init = jax.random.normal(key_init, grid_shape, jnp.float32)
    kappa_cell = jnp.exp(jax.random.uniform(key_coef, (GRID_ROWS, GRID_COLS), jnp.float32, -0.8, 0.8))
    omega_relax = jax.random.uniform(key_omega, (), jnp.float32, 0.7, 1.0)
    return dict(f_rhs=f_rhs, u_init=u_init, kappa_cell=kappa_cell,
                solve_mats=build_solve_mats(kappa_cell), omega_relax=omega_relax)


def local_solves(residual, solve_mats):
    padded = jnp.pad(residual.astype(jnp.bfloat16), ((MARGIN, MARGIN), (MARGIN, MARGIN), (0, 0)))

    def one_block(block_idx):
        blk_row = block_idx // COL_BLOCKS
        blk_col = block_idx % COL_BLOCKS
        window = lax.dynamic_slice(padded, (blk_row * SUB_SIZE, blk_col * SUB_SIZE, 0),
                                   (EXT_SIZE, EXT_SIZE, RHS_COUNT))
        product = jnp.dot(solve_mats[blk_row, blk_col], window.reshape(EXT_SIZE * EXT_SIZE, RHS_COUNT),
                          preferred_element_type=jnp.float32)
        return product.astype(jnp.bfloat16)

    blocks = lax.map(one_block, jnp.arange(ROW_BLOCKS * COL_BLOCKS))
    blocks = blocks.reshape(ROW_BLOCKS, COL_BLOCKS, SUB_SIZE, SUB_SIZE, RHS_COUNT)
    return blocks.transpose(0, 2, 1, 3, 4).reshape(GRID_ROWS, GRID_COLS, RHS_COUNT)


def reference(f_rhs, u_init, kappa_cell, solve_mats, omega_relax):
    face_set = face_coeffs(kappa_cell)
    residual = f_rhs - apply_operator(u_init, face_set)

    def one_sweep(state_pair, unused):
        u_cur, res_cur = state_pair
        correction = local_solves(res_cur, solve_mats).astype(jnp.float32)
        u_next = u_cur + omega_relax * correction
        res_next = res_cur - omega_relax * apply_operator(correction, face_set)
        return (u_next, res_next), None

    final_pair, unused_out = lax.scan(one_sweep, (u_init, residual), None, length=SWEEPS)
    return final_pair[0]
```

```python
import functools
import jax
import jax.numpy as jnp
from jax import lax
from jax.experimental import pallas as pl
from jax.experimental.pallas import tpu as pltpu
from jax.sharding import PartitionSpec as P

SWEEPS = 6
SUB = 32
MARGIN = 4
EXT = SUB + 2 * MARGIN
CELLS = SUB * SUB
LANES = 128
TILES = 2
GROUP = TILES * LANES
COLS_AT = CELLS
ROWS_AT = CELLS + 256
CORN_AT = ROWS_AT + 128
DEPTH = CORN_AT + 128
PAD = SUB
MESH = pl.DeviceIdType.MESH
F32 = jnp.float32
BF16 = jnp.bfloat16


def own_source(n):
    return ((n >> 5) + MARGIN) * EXT + (n & 31) + MARGIN


def side_column(side, dist):
    return jnp.where(side == 0, MARGIN - 1 - dist, MARGIN + SUB + dist)


def kernel(groups, col_count,
           f_hbm, u_hbm, kap_ref, mat_hbm, om_ref, out_ref,
           mat_v, mat_p, res, zf, u_v, e_v, kb, cd, cn, cs, cw, ce, cedge, crow,
           send_p, send_b, send_u, recv_p, recv_b, recv_u, zrow, kcol_s, kcol_r, krow_r,
           in_sem, mat_sem, sp_sem, rp_sem, sb_sem, rb_sem, su_sem, ru_sem,
           sz_sem, rz_sem, sf_sem, rf_sem, sk_sem, rk_sem):
    col = lax.axis_index('col')
    row = lax.axis_index('row')
    has = (col > 0, col < col_count - 1)
    side_dev = ((col - 1, row), (col + 1, row))
    partner = (col, 1 - row)
    brow = (SUB - 1) * (1 - row)
    om = om_ref[0]

    loads = []
    for g in range(groups):
        for t in range(TILES):
            k = g * TILES + t
            lanes = pl.ds(k * LANES, LANES)
            loads.append((
                pltpu.make_async_copy(u_hbm.at[:, lanes], zf.at[k, pl.ds(PAD, CELLS)], in_sem.at[0, k]),
                pltpu.make_async_copy(f_hbm.at[:, lanes], res.at[k], in_sem.at[1, k]),
                pltpu.make_async_copy(u_hbm.at[:, lanes], u_v.at[k], in_sem.at[2, k])))
    for a, b, c in loads:
        a.start()
        b.start()
    mat_copy = pltpu.make_async_copy(mat_hbm, mat_v, mat_sem)
    mat_copy.start()
    for a, b, c in loads:
        c.start()

    barrier = pltpu.get_barrier_semaphore()
    pl.semaphore_signal(barrier, inc=1, device_id=partner, device_id_type=MESH)
    for s in range(2):
        @pl.when(has[s])
        def _():
            pl.semaphore_signal(barrier, inc=1, device_id=side_dev[s], device_id_type=MESH)
    waits = 1 + has[0].astype(jnp.int32) + has[1].astype(jnp.int32)
    pl.semaphore_wait(barrier, waits)

    zero_row = jnp.zeros((SUB, LANES), F32)
    kap_t = jnp.transpose(jnp.concatenate([kap_ref[...], jnp.zeros((LANES - SUB, SUB), F32)], axis=0))
    kb[pl.ds(0, SUB)] = zero_row
    kb[pl.ds(PAD + CELLS, SUB)] = zero_row
    for r in range(SUB):
        kb[pl.ds(PAD + r * SUB, SUB)] = jnp.broadcast_to(kap_t[:, r:r + 1], (SUB, LANES))

    def kcol_copy(s):
        return pltpu.make_async_remote_copy(kcol_s.at[s], kcol_r.at[1 - s], sk_sem.at[s], rk_sem.at[1 - s],
                                            device_id=side_dev[s], device_id_type=MESH)

    def krow_copy():
        return pltpu.make_async_remote_copy(kb.at[pl.ds(PAD + brow * SUB, SUB)], krow_r, sk_sem.at[2], rk_sem.at[2],
                                            device_id=partner, device_id_type=MESH)

    edge_col = (0, SUB - 1)

    def edge_cells(c, at=0):
        return pl.ds(at + c, SUB, stride=SUB)

    for s in range(2):
        kcol_s[s] = kb[edge_cells(edge_col[s], PAD), :]

        @pl.when(has[s])
        def _():
            kcol_copy(s).start()
    krow_copy().start()

    sub_id = lax.broadcasted_iota(jnp.int32, (SUB, LANES), 0)
    no_w = jnp.where(has[0], 0.0, 1.0)
    no_e = jnp.where(has[1], 0.0, 1.0)

    def coeff_row(q, carry):
        base = pl.multiple_of(q * SUB, SUB)
        here = kb[pl.ds(PAD + base, SUB)]
        up = kb[pl.ds(base, SUB)]
        down = kb[pl.ds(2 * PAD + base, SUB)]
        left = jnp.concatenate([here[:1], here[:-1]], axis=0)
        right = jnp.concatenate([here[1:], here[-1:]], axis=0)
        vn = jnp.where(q == 0, 0.0, 1.0) * (0.5 * (here + up))
        vs = jnp.where(q == SUB - 1, 0.0, 1.0) * (0.5 * (here + down))
        vw = jnp.where(sub_id == 0, 0.0, 0.5 * (here + left))
        ve = jnp.where(sub_id == SUB - 1, 0.0, 0.5 * (here + right))
        rim = jnp.where(jnp.logical_or(jnp.logical_and(q == 0, row == 0),
                                       jnp.logical_and(q == SUB - 1, row == 1)), 1.0, 0.0)
        rim_col = jnp.where(sub_id == 0, no_w, 0.0) + jnp.where(sub_id == SUB - 1, no_e, 0.0)
        rows = pl.ds(base, SUB)
        cn[rows] = vn
        cs[rows] = vs
        cw[rows] = vw
        ce[rows] = ve
        cd[rows] = vn + vs + vw + ve + (rim + rim_col) * here
        return carry

    lax.fori_loop(0, SUB, coeff_row, 0)

    def stencil(g):
        def one_row(q, carry):
            base = pl.multiple_of(q * SUB, SUB)
            rows = pl.ds(base, SUB)
            vd, vn, vs, vw, ve = cd[rows], cn[rows], cs[rows], cw[rows], ce[rows]
            for t in range(TILES):
                k = g * TILES + t
                part = (vd * zf[k, pl.ds(PAD + base, SUB)]
                        - vn * zf[k, pl.ds(base, SUB)]
                        - vs * zf[k, pl.ds(2 * PAD + base, SUB)]
                        - vw * zf[k, pl.ds(PAD - 1 + base, SUB)]
                        - ve * zf[k, pl.ds(PAD + 1 + base, SUB)])
                res[k, rows] = res[k, rows] - part
            return carry

        lax.fori_loop(0, SUB, one_row, 0)

    def zrow_copy(g):
        return pltpu.make_async_remote_copy(
            zf.at[pl.ds(g * TILES, TILES), pl.ds(PAD + brow * SUB, SUB)], zrow.at[pl.ds(g * TILES, TILES)],
            sz_sem.at[g], rz_sem.at[g], device_id=partner, device_id_type=MESH)

    def row_fix(g):
        rows = pl.ds(pl.multiple_of(brow * SUB, SUB), SUB)
        zrows = pl.ds(pl.multiple_of(PAD + brow * SUB, SUB), SUB)
        for t in range(TILES):
            k = g * TILES + t
            res[k, rows] = res[k, rows] - crow[...] * (zf[k, zrows] - zrow[k])

    def p_copy(g, s, slot):
        return pltpu.make_async_remote_copy(send_p.at[g, s], recv_p.at[slot, g, 1 - s], sp_sem.at[g, s],
                                            rp_sem.at[slot, g, 1 - s], device_id=side_dev[s], device_id_type=MESH)

    def b_copy(g, s, slot, first=0):
        rows = pl.ds(first, 128 - first)
        return pltpu.make_async_remote_copy(send_b.at[g, s, rows], recv_b.at[slot, g, 1 - s, rows], sb_sem.at[g, s],
                                            rb_sem.at[slot, g, 1 - s], device_id=side_dev[s], device_id_type=MESH)

    def u_copy(g, s):
        return pltpu.make_async_remote_copy(send_u.at[g, s], recv_u.at[g, 1 - s], su_sem.at[g, s],
                                            ru_sem.at[g, 1 - s], device_id=side_dev[s], device_id_type=MESH)

    def near(s, dist):
        return dist if s == 0 else SUB - 1 - dist

    def fill_edges(g, first):
        for s in range(2):
            for t in range(TILES):
                k = g * TILES + t
                lanes = pl.ds(t * LANES, LANES)
                send_p[g, s, :, lanes] = res[k, edge_cells(near(s, 0)), :]
                zedge = zf[k, edge_cells(near(s, 0), PAD), :]
                if first:
                    send_u[g, s, :, lanes] = zedge
                else:
                    send_b[g, s, pl.ds(0, SUB), lanes] = zedge.astype(BF16)
                for d in range(1, MARGIN):
                    send_b[g, s, pl.ds(d * SUB, SUB), lanes] = res[k, edge_cells(near(s, d)), :].astype(BF16)

    def fwd_copies(g):
        rows = pl.multiple_of((SUB - MARGIN) * SUB * (1 - row), 128)
        half = pl.multiple_of(COLS_AT + 128 * (1 - row), 128)
        return [
            pltpu.make_async_remote_copy(e_v.at[g, pl.ds(rows, 128)], e_v.at[g, pl.ds(ROWS_AT, 128)],
                                         sf_sem.at[g, 0], rf_sem.at[g, 0], device_id=partner, device_id_type=MESH),
            pltpu.make_async_remote_copy(e_v.at[g, pl.ds(half, 128)], e_v.at[g, pl.ds(CORN_AT, 128)],
                                         sf_sem.at[g, 1], rf_sem.at[g, 1], device_id=partner, device_id_type=MESH)]

    def assemble(g, slot, first):
        for s in range(2):
            @pl.when(has[s])
            def _():
                p_copy(g, 1 - s, slot).wait_recv()
                if first:
                    u_copy(g, 1 - s).wait_recv()
                    b_copy(g, 1 - s, slot, SUB).wait_recv()
                else:
                    b_copy(g, 1 - s, slot).wait_recv()
                for t in range(TILES):
                    k = g * TILES + t
                    lanes = pl.ds(t * LANES, LANES)
                    if first:
                        theirs = recv_u[g, s, :, lanes]
                    else:
                        theirs = recv_b[slot, g, s, pl.ds(0, SUB), lanes].astype(F32)
                    cells = edge_cells(edge_col[s])
                    flux = cedge[s] * (zf[k, edge_cells(edge_col[s], PAD), :] - theirs)
                    res[k, cells, :] = res[k, cells, :] - flux
                    halo = (recv_p[slot, g, s, :, lanes] + flux).astype(BF16)
                    for h in range(2):
                        at = COLS_AT + 128 * h + 64 * s
                        e_v[g, pl.ds(at, 16), lanes] = halo[16 * h:16 * h + 16]
                        for d in range(1, MARGIN):
                            e_v[g, pl.ds(at + 16 * d, 16), lanes] = recv_b[slot, g, s, pl.ds(SUB * d + 16 * h, 16), lanes]

        def pack(q, carry):
            rows = pl.ds(pl.multiple_of(q * 64, 64), 64)
            for t in range(TILES):
                e_v[g, rows, pl.ds(t * LANES, LANES)] = res[g * TILES + t, rows].astype(BF16)
            return carry

        lax.fori_loop(0, CELLS // 64, pack, 0)
        for c in fwd_copies(g):
            c.start()

    def solve(g, last):
        for c in fwd_copies(g):
            c.wait()

        def rows_of(m, carry):
            rows = pl.ds(pl.multiple_of(m * 256, 256), 256)
            zrows = pl.ds(pl.multiple_of(PAD + m * 256, PAD), 256)
            z = jnp.dot(mat_p[rows, :], e_v[g], preferred_element_type=F32).astype(BF16).astype(F32)
            for t in range(TILES):
                k = g * TILES + t
                zt = z[:, t * LANES:(t + 1) * LANES]
                if last:
                    out_ref[rows, pl.ds(k * LANES, LANES)] = u_v[k, rows] + om * zt
                else:
                    zf[k, zrows] = zt
                    u_v[k, rows] = u_v[k, rows] + om * zt
            return carry

        lax.fori_loop(0, CELLS // 256, rows_of, 0)

    for k in range(groups * TILES):
        zf[k, pl.ds(0, PAD)] = zero_row
        zf[k, pl.ds(PAD + CELLS, PAD)] = zero_row
    for g in range(groups):
        e_v[g, pl.ds(COLS_AT, 256)] = jnp.zeros((256, GROUP), BF16)

    krow_copy().wait()
    rows_b = pl.ds(pl.multiple_of(PAD + brow * SUB, SUB), SUB)
    crow[...] = 0.5 * (kb[rows_b] + krow_r[...])

    for g in range(groups):
        for t in range(TILES):
            loads[g * TILES + t][0].wait()
        zrow_copy(g).start()
        for t in range(TILES):
            loads[g * TILES + t][1].wait()
        stencil(g)
        zrow_copy(g).wait()
        row_fix(g)
        fill_edges(g, True)
        for s in range(2):
            @pl.when(has[s])
            def _():
                p_copy(g, s, 0).start()
                u_copy(g, s).start()
                b_copy(g, s, 0, SUB).start()

    mat_copy.wait()

    def place(at, width, start, window, source, ok=None):
        n = lax.broadcasted_iota(jnp.int32, (window, width), 1)
        k = lax.broadcasted_iota(jnp.int32, (window, width), 0) + start
        pick = source(n) == k
        if ok is not None:
            pick = jnp.logical_and(pick, ok(n))
        pick = jnp.where(pick, 1.0, 0.0).astype(BF16)

        def rows_of(m, carry):
            rows = pl.ds(pl.multiple_of(m * 256, 256), 256)
            mat_p[rows, pl.ds(at, width)] = jnp.dot(mat_v[rows, pl.ds(start, window)], pick,
                                                    preferred_element_type=F32).astype(BF16)
            return carry

        lax.fori_loop(0, CELLS // 256, rows_of, 0)

    for q in range(4):
        low = (320 * q + 164) // 128 * 128
        high = -(-(320 * q + 476) // 128) * 128
        place(256 * q, 256, low, high - low, lambda n, q=q: own_source(n + 256 * q))

    def side_source(n):
        r = 16 * (n >> 7) + (n & 15)
        return (r + MARGIN) * EXT + side_column((n >> 6) & 1, (n >> 4) & 3)

    place(COLS_AT, 256, 128, 1408, side_source)

    def row_source(n):
        m = n & 127
        first_row = jnp.where(row == 0, MARGIN + SUB, 0)
        halo = (first_row + (m >> 5)) * EXT + MARGIN + (m & 31)
        corner_row = jnp.where(row == 0, MARGIN + SUB, -12) + (m & 15)
        corner = corner_row * EXT + side_column((m >> 6) & 1, (m >> 4) & 3)
        return jnp.where(n < 128, halo, corner)

    def row_ok(n):
        r16 = n & 15
        return jnp.logical_or(n < 128, jnp.where(row == 0, r16, 15 - r16) < MARGIN)

    place(ROWS_AT, 256, pl.multiple_of(1408 * (1 - row), 128), 192, row_source, row_ok)

    for s in range(2):
        @pl.when(has[s])
        def _():
            kcol_copy(1 - s).wait_recv()
            cedge[s] = 0.5 * (kcol_s[s] + kcol_r[s])
            kcol_copy(s).wait_send()
    for k in range(groups * TILES):
        loads[k][2].wait()

    for g in range(groups):
        assemble(g, 0, True)
    for s in range(2):
        @pl.when(has[s])
        def _():
            cedge[s] = om * cedge[s]
    crow[...] = om * crow[...]

    def scale(q, carry):
        rows = pl.ds(pl.multiple_of(q * SUB, SUB), SUB)
        for c in (cd, cn, cs, cw, ce):
            c[rows] = om * c[rows]
        return carry

    lax.fori_loop(0, SUB, scale, 0)

    def wait_sends(g, first):
        for s in range(2):
            @pl.when(has[s])
            def _():
                p_copy(g, s, 0).wait_send()
                if first:
                    u_copy(g, s).wait_send()
                    b_copy(g, s, 0, SUB).wait_send()
                else:
                    b_copy(g, s, 0).wait_send()

    def advance(g, slot, first):
        solve(g, False)
        zrow_copy(g).start()
        stencil(g)
        wait_sends(g, first)
        zrow_copy(g).wait()
        row_fix(g)
        fill_edges(g, False)
        for s in range(2):
            @pl.when(has[s])
            def _():
                p_copy(g, s, slot).start()
                b_copy(g, s, slot).start()

    for g in range(groups):
        advance(g, 1, True)

    def sweep(t, carry):
        slot = lax.rem(t, 2)
        for g in range(groups):
            assemble(g, 1 - slot, False)
            advance(g, slot, False)
        return carry

    lax.fori_loop(2, SWEEPS, sweep, 0)
    for g in range(groups):
        assemble(g, (SWEEPS - 1) % 2, False)
        solve(g, True)
    for g in range(groups):
        wait_sends(g, False)


def solution(mesh):
    col_count = mesh.shape['col']
    grid_spec = P('row', 'col', None)

    def device_fn(f_blk, u_blk, kappa_blk, mat_blk, omega_relax):
        rhs_count = u_blk.shape[2]
        groups = rhs_count // GROUP
        tiles = rhs_count // LANES
        vm = pltpu.VMEM
        dma = pltpu.SemaphoreType.DMA
        coeff = vm((CELLS, LANES), F32)
        out = pl.pallas_call(
            functools.partial(kernel, groups, col_count),
            out_shape=jax.ShapeDtypeStruct((CELLS, rhs_count), F32),
            in_specs=[pl.BlockSpec(memory_space=pl.ANY), pl.BlockSpec(memory_space=pl.ANY),
                      pl.BlockSpec(memory_space=pltpu.VMEM), pl.BlockSpec(memory_space=pl.ANY),
                      pl.BlockSpec(memory_space=pltpu.SMEM)],
            out_specs=pl.BlockSpec(memory_space=pltpu.VMEM),
            scratch_shapes=[
                vm((CELLS, EXT * EXT), BF16),
                vm((CELLS, DEPTH), BF16),
                vm((tiles, CELLS, LANES), F32),
                vm((tiles, CELLS + 2 * PAD, LANES), F32),
                vm((tiles, CELLS, LANES), F32),
                vm((groups, DEPTH, GROUP), BF16),
                vm((CELLS + 2 * PAD, LANES), F32),
                coeff, coeff, coeff, coeff, coeff,
                vm((2, SUB, LANES), F32),
                vm((SUB, LANES), F32),
                vm((groups, 2, SUB, GROUP), F32),
                vm((groups, 2, 128, GROUP), BF16),
                vm((groups, 2, SUB, GROUP), F32),
                vm((2, groups, 2, SUB, GROUP), F32),
                vm((2, groups, 2, 128, GROUP), BF16),
                vm((groups, 2, SUB, GROUP), F32),
                vm((tiles, SUB, LANES), F32),
                vm((2, SUB, LANES), F32),
                vm((2, SUB, LANES), F32),
                vm((SUB, LANES), F32),
                dma((3, tiles)), dma,
                dma((groups, 2)), dma((2, groups, 2)),
                dma((groups, 2)), dma((2, groups, 2)),
                dma((groups, 2)), dma((groups, 2)),
                dma((groups,)), dma((groups,)),
                dma((groups, 2)), dma((groups, 2)),
                dma((3,)), dma((3,)),
            ],
            compiler_params=pltpu.CompilerParams(collective_id=0, has_side_effects=True,
                                                 vmem_limit_bytes=60 * 1024 * 1024),
        )(f_blk.reshape(CELLS, rhs_count), u_blk.reshape(CELLS, rhs_count), kappa_blk,
          mat_blk.reshape(CELLS, EXT * EXT), omega_relax.reshape(1))
        return out.reshape(SUB, SUB, rhs_count)

    return jax.shard_map(device_fn, mesh=mesh,
                         in_specs=(grid_spec, grid_spec, P('row', 'col'), P('row', 'col', None, None), P()),
                         out_specs=grid_spec, check_vma=False)
```

```python
import functools
import jax
import jax.numpy as jnp
from jax import lax
from jax.experimental import pallas as pl
from jax.experimental.pallas import tpu as pltpu
from jax.sharding import PartitionSpec as P

SWEEPS = 6
SUB = 32
MARGIN = 4
EXT = SUB + 2 * MARGIN
CELLS = SUB * SUB
LANES = 128
TILES = 2
GROUP = TILES * LANES
COLS_AT = CELLS
ROWS_AT = CELLS + 256
CORN_AT = ROWS_AT + 128
DEPTH = CORN_AT + 128
PAD = SUB
MESH = pl.DeviceIdType.MESH
F32 = jnp.float32
BF16 = jnp.bfloat16


def own_source(n):
    return ((n >> 5) + MARGIN) * EXT + (n & 31) + MARGIN


def side_column(side, dist):
    return jnp.where(side == 0, MARGIN - 1 - dist, MARGIN + SUB + dist)


def kernel(groups, col_count,
           f_hbm, u_hbm, kap_ref, mat_hbm, om_ref, u_out, z_out,
           mat_v, mat_p, acc, res, zf, u_v, e_v, z_v, kb, cd, cn, cs, cw, ce, cedge, cedge_om, crow,
           send_p, send_b, send_u, recv_p, recv_b, recv_u, zrow_s, zrow, kcol_s, kcol_r, krow_r,
           in_sem, mat_sem, out_sem, s_sem, r_sem, su_sem, ru_sem,
           sz_sem, rz_sem, sf_sem, rf_sem, sk_sem, rk_sem):
    col = lax.axis_index('col')
    row = lax.axis_index('row')
    has = (col > 0, col < col_count - 1)
    side_dev = ((col - 1, row), (col + 1, row))
    partner = (col, 1 - row)
    brow = (SUB - 1) * (1 - row)
    om = om_ref[0]

    loads = []
    for g in range(groups):
        for t in range(TILES):
            k = g * TILES + t
            lanes = pl.ds(k * LANES, LANES)
            loads.append((
                pltpu.make_async_copy(u_hbm.at[:, lanes], zf.at[k, pl.ds(PAD, CELLS)], in_sem.at[0, k]),
                pltpu.make_async_copy(f_hbm.at[:, lanes], res.at[k], in_sem.at[1, k]),
                pltpu.make_async_copy(u_hbm.at[:, lanes], u_v.at[k], in_sem.at[2, k])))
    for a, b, c in loads:
        a.start()
        b.start()
    mat_copy = pltpu.make_async_copy(mat_hbm, mat_v, mat_sem)
    mat_copy.start()
    for a, b, c in loads:
        c.start()

    barrier = pltpu.get_barrier_semaphore()
    pl.semaphore_signal(barrier, inc=1, device_id=partner, device_id_type=MESH)
    for s in range(2):
        @pl.when(has[s])
        def _():
            pl.semaphore_signal(barrier, inc=1, device_id=side_dev[s], device_id_type=MESH)
    waits = 1 + has[0].astype(jnp.int32) + has[1].astype(jnp.int32)
    pl.semaphore_wait(barrier, waits)

    zero_row = jnp.zeros((SUB, LANES), F32)
    kap_t = jnp.transpose(jnp.concatenate([kap_ref[...], jnp.zeros((LANES - SUB, SUB), F32)], axis=0))
    kb[pl.ds(0, SUB)] = zero_row
    kb[pl.ds(PAD + CELLS, SUB)] = zero_row
    for r in range(SUB):
        kb[pl.ds(PAD + r * SUB, SUB)] = jnp.broadcast_to(kap_t[:, r:r + 1], (SUB, LANES))

    def kcol_copy(s):
        return pltpu.make_async_remote_copy(kcol_s.at[s], kcol_r.at[1 - s], sk_sem.at[s], rk_sem.at[1 - s],
                                            device_id=side_dev[s], device_id_type=MESH)

    def krow_copy():
        return pltpu.make_async_remote_copy(kb.at[pl.ds(PAD + brow * SUB, SUB)], krow_r, sk_sem.at[2], rk_sem.at[2],
                                            device_id=partner, device_id_type=MESH)

    edge_col = (0, SUB - 1)

    def edge_cells(c, at=0):
        return pl.ds(at + c, SUB, stride=SUB)

    for s in range(2):
        kcol_s[s] = kb[edge_cells(edge_col[s], PAD), :]

        @pl.when(has[s])
        def _():
            kcol_copy(s).start()
    krow_copy().start()

    sub_id = lax.broadcasted_iota(jnp.int32, (SUB, LANES), 0)
    no_w = jnp.where(has[0], 0.0, 1.0)
    no_e = jnp.where(has[1], 0.0, 1.0)

    def coeff_row(q, carry):
        base = pl.multiple_of(q * SUB, SUB)
        here = kb[pl.ds(PAD + base, SUB)]
        up = kb[pl.ds(base, SUB)]
        down = kb[pl.ds(2 * PAD + base, SUB)]
        left = jnp.concatenate([here[:1], here[:-1]], axis=0)
        right = jnp.concatenate([here[1:], here[-1:]], axis=0)
        vn = jnp.where(q == 0, 0.0, 1.0) * (0.5 * (here + up))
        vs = jnp.where(q == SUB - 1, 0.0, 1.0) * (0.5 * (here + down))
        vw = jnp.where(sub_id == 0, 0.0, 0.5 * (here + left))
        ve = jnp.where(sub_id == SUB - 1, 0.0, 0.5 * (here + right))
        rim = jnp.where(jnp.logical_or(jnp.logical_and(q == 0, row == 0),
                                       jnp.logical_and(q == SUB - 1, row == 1)), 1.0, 0.0)
        rim_col = jnp.where(sub_id == 0, no_w, 0.0) + jnp.where(sub_id == SUB - 1, no_e, 0.0)
        rows = pl.ds(base, SUB)
        cn[rows] = vn
        cs[rows] = vs
        cw[rows] = vw
        ce[rows] = ve
        cd[rows] = vn + vs + vw + ve + (rim + rim_col) * here
        return carry

    lax.fori_loop(0, SUB, coeff_row, 0)

    def stencil(g, first, count, unroll):
        def one_row(q, carry):
            for at, n in zip(first, count):
                base = pl.multiple_of(q * SUB + at, 8)
                rows = pl.ds(base, n)
                vd, vn, vs, vw, ve = cd[rows], cn[rows], cs[rows], cw[rows], ce[rows]
                for t in range(TILES):
                    k = g * TILES + t
                    part = (vd * zf[k, pl.ds(PAD + base, n)]
                            - vn * zf[k, pl.ds(base, n)]
                            - vs * zf[k, pl.ds(2 * PAD + base, n)]
                            - vw * zf[k, pl.ds(PAD - 1 + base, n)]
                            - ve * zf[k, pl.ds(PAD + 1 + base, n)])
                    res[k, rows] = res[k, rows] - part
            return carry

        lax.fori_loop(0, SUB, one_row, 0, unroll=unroll)

    def stencil_sides(g):
        stencil(g, (0, SUB - 8), (8, 8), 4)

    def stencil_middle(g):
        stencil(g, (8,), (16,), 4)

    def zrow_copy(g):
        return pltpu.make_async_remote_copy(
            zrow_s.at[g], zrow.at[g], sz_sem.at[g], rz_sem.at[g], device_id=partner, device_id_type=MESH)

    brows = pl.ds(pl.multiple_of(brow * SUB, SUB), SUB)

    def row_fix(g):
        for t in range(TILES):
            k = g * TILES + t
            res[k, brows] = res[k, brows] - crow[...] * (zrow_s[g, t] - zrow[g, t])

    def near(s, dist):
        return dist if s == 0 else SUB - 1 - dist

    far = row
    closer = 1 - row

    def message(g, s, slot, i):
        half = (far, closer)[(i - 1) // 2]
        if i in (1, 3):
            rows = pl.ds(pl.multiple_of(16 * half, 16), 16)
            src, dst = send_p, recv_p
        else:
            rows = pl.ds(0, SUB) if i == 0 else pl.ds(pl.multiple_of(SUB + 48 * half, 16), 48)
            src, dst = send_b, recv_b
        return pltpu.make_async_remote_copy(src.at[g, s, rows], dst.at[slot, g, 1 - s, rows], s_sem.at[g, s, i],
                                            r_sem.at[slot, g, 1 - s, i], device_id=side_dev[s], device_id_type=MESH)

    def u_copy(g, s):
        return pltpu.make_async_remote_copy(send_u.at[g, s], recv_u.at[g, 1 - s], su_sem.at[g, s],
                                            ru_sem.at[g, 1 - s], device_id=side_dev[s], device_id_type=MESH)

    def fill_z(g, first):
        for s in range(2):
            for t in range(TILES):
                lanes = pl.ds(t * LANES, LANES)
                zedge = zf[g * TILES + t, edge_cells(near(s, 0), PAD), :]
                if first:
                    send_u[g, s, :, lanes] = zedge
                else:
                    send_b[g, s, pl.ds(0, SUB), lanes] = zedge.astype(BF16)

    def fill_half(g, h):
        at = pl.multiple_of(CELLS // 2 * h, CELLS // 2)
        p_at = pl.multiple_of(16 * h, 16)
        e_at = pl.multiple_of(SUB + 48 * h, 16)
        for s in range(2):
            for t in range(TILES):
                k = g * TILES + t
                lanes = pl.ds(t * LANES, LANES)
                for d in range(MARGIN):
                    part = res[k, pl.ds(at + near(s, d), 16, stride=SUB), :]
                    if d == 0:
                        send_p[g, s, pl.ds(p_at, 16), lanes] = part
                    else:
                        send_b[g, s, pl.ds(e_at + 16 * (d - 1), 16), lanes] = part.astype(BF16)

    def start(g, slot, which):
        for s in range(2):
            @pl.when(has[s])
            def _():
                for i in which:
                    message(g, s, slot, i).start()

    def fwd_copies(g):
        rows = pl.multiple_of((SUB - MARGIN) * SUB * (1 - row), 128)
        half = pl.multiple_of(COLS_AT + 128 * (1 - row), 128)
        return [
            pltpu.make_async_remote_copy(e_v.at[g, pl.ds(rows, 128)], e_v.at[g, pl.ds(ROWS_AT, 128)],
                                         sf_sem.at[g, 0], rf_sem.at[g, 0], device_id=partner, device_id_type=MESH),
            pltpu.make_async_remote_copy(e_v.at[g, pl.ds(half, 128)], e_v.at[g, pl.ds(CORN_AT, 128)],
                                         sf_sem.at[g, 1], rf_sem.at[g, 1], device_id=partner, device_id_type=MESH)]

    def assemble(g, slot, first):
        for s in range(2):
            @pl.when(has[s])
            def _():
                if first:
                    u_copy(g, 1 - s).wait_recv()
                for i in range(1 if first else 0, 5):
                    message(g, 1 - s, slot, i).wait_recv()
                for t in range(TILES):
                    k = g * TILES + t
                    lanes = pl.ds(t * LANES, LANES)
                    if first:
                        theirs = recv_u[g, s, :, lanes]
                    else:
                        theirs = recv_b[slot, g, s, pl.ds(0, SUB), lanes].astype(F32)
                    cells = edge_cells(edge_col[s])
                    coeff = cedge[s] if first else cedge_om[s]
                    flux = coeff * (zf[k, edge_cells(edge_col[s], PAD), :] - theirs)
                    res[k, cells, :] = res[k, cells, :] - flux
                    halo = (recv_p[slot, g, s, :, lanes] + flux).astype(BF16)
                    for h in range(2):
                        at = COLS_AT + 128 * h + 64 * s
                        e_v[g, pl.ds(at, 16), lanes] = halo[16 * h:16 * h + 16]
                        e_v[g, pl.ds(at + 16, 48), lanes] = recv_b[slot, g, s, pl.ds(SUB + 48 * h, 48), lanes]

        def pack(rows):
            for t in range(TILES):
                e_v[g, rows, pl.ds(t * LANES, LANES)] = res[g * TILES + t, rows].astype(BF16)

        fwd_rows, fwd_corners = fwd_copies(g)
        fwd_corners.start()
        pack(pl.ds(pl.multiple_of((SUB - MARGIN) * SUB * (1 - row), 128), 128))
        rest = pl.multiple_of(128 * row, 128)

        def pack_rest(q, carry):
            pack(pl.ds(pl.multiple_of(rest + q * 128, 128), 128))
            return carry

        fwd_rows.start()
        lax.fori_loop(0, CELLS // 128 - 1, pack_rest, 0)

    def solve(g):
        acc[...] = jnp.dot(mat_p[:, :ROWS_AT], e_v[g, pl.ds(0, ROWS_AT)], preferred_element_type=F32)
        for c in fwd_copies(g):
            c.wait()
        acc[...] += jnp.dot(mat_p[:, ROWS_AT:], e_v[g, pl.ds(ROWS_AT, DEPTH - ROWS_AT)], preferred_element_type=F32)

    def round_row(g):
        for t in range(TILES):
            zrow_s[g, t] = acc[brows, pl.ds(t * LANES, LANES)].astype(BF16).astype(F32)

    def update(g):
        def rows_of(q, carry):
            rows = pl.ds(pl.multiple_of(q * 64, 64), 64)
            for t in range(TILES):
                k = g * TILES + t
                z = acc[rows, pl.ds(t * LANES, LANES)].astype(BF16).astype(F32)
                zf[k, pl.ds(pl.multiple_of(PAD + q * 64, PAD), 64)] = z
                u_v[k, rows] = u_v[k, rows] + om * z
            return carry

        lax.fori_loop(0, CELLS // 64, rows_of, 0)

    for k in range(groups * TILES):
        zf[k, pl.ds(0, PAD)] = zero_row
        zf[k, pl.ds(PAD + CELLS, PAD)] = zero_row
    for g in range(groups):
        e_v[g, pl.ds(COLS_AT, 256)] = jnp.zeros((256, GROUP), BF16)

    krow_copy().wait()
    rows_b = pl.ds(pl.multiple_of(PAD + brow * SUB, SUB), SUB)
    crow[...] = 0.5 * (kb[rows_b] + krow_r[...])

    def send_bands(g, slot):
        stencil_sides(g)
        fill_half(g, far)
        start(g, slot, (1, 2))
        zrow_copy(g).wait()
        row_fix(g)
        fill_half(g, closer)
        start(g, slot, (3, 4))
        stencil_middle(g)

    for g in range(groups):
        for t in range(TILES):
            loads[g * TILES + t][0].wait()
        for t in range(TILES):
            zrow_s[g, t] = zf[g * TILES + t, rows_b]
        zrow_copy(g).start()
        fill_z(g, True)
        for s in range(2):
            @pl.when(has[s])
            def _():
                u_copy(g, s).start()
        for t in range(TILES):
            loads[g * TILES + t][1].wait()
        send_bands(g, 0)

    mat_copy.wait()

    def place(at, width, start, window, source, ok=None):
        n = lax.broadcasted_iota(jnp.int32, (window, width), 1)
        k = lax.broadcasted_iota(jnp.int32, (window, width), 0) + start
        pick = source(n) == k
        if ok is not None:
            pick = jnp.logical_and(pick, ok(n))
        pick = jnp.where(pick, 1.0, 0.0).astype(BF16)

        def rows_of(m, carry):
            rows = pl.ds(pl.multiple_of(m * 256, 256), 256)
            mat_p[rows, pl.ds(at, width)] = lax.dot_general(mat_v[pl.ds(start, window), rows], pick,
                                                            (((0,), (0,)), ((), ())),
                                                            preferred_element_type=F32).astype(BF16)
            return carry

        lax.fori_loop(0, CELLS // 256, rows_of, 0)

    for q in range(4):
        low = (320 * q + 164) // 128 * 128
        high = -(-(320 * q + 476) // 128) * 128
        place(256 * q, 256, low, high - low, lambda n, q=q: own_source(n + 256 * q))

    def side_source(n):
        r = 16 * (n >> 7) + (n & 15)
        return (r + MARGIN) * EXT + side_column((n >> 6) & 1, (n >> 4) & 3)

    place(COLS_AT, 256, 128, 1408, side_source)

    def row_source(n):
        m = n & 127
        first_row = jnp.where(row == 0, MARGIN + SUB, 0)
        halo = (first_row + (m >> 5)) * EXT + MARGIN + (m & 31)
        corner_row = jnp.where(row == 0, MARGIN + SUB, -12) + (m & 15)
        corner = corner_row * EXT + side_column((m >> 6) & 1, (m >> 4) & 3)
        return jnp.where(n < 128, halo, corner)

    def row_ok(n):
        r16 = n & 15
        return jnp.logical_or(n < 128, jnp.where(row == 0, r16, 15 - r16) < MARGIN)

    place(ROWS_AT, 256, pl.multiple_of(1408 * (1 - row), 128), 192, row_source, row_ok)

    for s in range(2):
        @pl.when(has[s])
        def _():
            kcol_copy(1 - s).wait_recv()
            cedge[s] = 0.5 * (kcol_s[s] + kcol_r[s])
            cedge_om[s] = om * cedge[s]
            kcol_copy(s).wait_send()
    crow[...] = om * crow[...]

    def scale(q, carry):
        rows = pl.ds(pl.multiple_of(q * SUB, SUB), SUB)
        for c in (cd, cn, cs, cw, ce):
            c[rows] = om * c[rows]
        return carry

    lax.fori_loop(0, SUB, scale, 0)
    for k in range(groups * TILES):
        loads[k][2].wait()

    def wait_sends(g, which):
        for s in range(2):
            @pl.when(has[s])
            def _():
                for i in which:
                    message(g, s, 0, i).wait_send()

    def advance(g, slot, first):
        solve(g)
        round_row(g)
        zrow_copy(g).start()
        update(g)
        if first:
            wait_sends(g, (1, 2, 3, 4))
        else:
            wait_sends(g, (0, 1, 2, 3, 4))
        fill_z(g, False)
        start(g, slot, (0,))
        send_bands(g, slot)

    for g in range(groups):
        assemble(g, 0, True)
        advance(g, 1, True)

    def step(i, carry):
        t = i // groups
        g = lax.rem(i, groups)
        slot = lax.rem(t, 2)
        assemble(g, 1 - slot, False)
        advance(g, slot, False)
        return carry

    lax.fori_loop(2 * groups, SWEEPS * groups, step, 0)

    u_copies = [pltpu.make_async_copy(u_v.at[k], u_out.at[:, pl.ds(k * LANES, LANES)], in_sem.at[0, k])
                for k in range(groups * TILES)]
    z_copies = [pltpu.make_async_copy(z_v.at[g], z_out.at[:, pl.ds(g * GROUP, GROUP)], out_sem.at[g])
                for g in range(groups)]
    for g in range(groups):
        for t in range(TILES):
            u_copies[g * TILES + t].start()
    for g in range(groups):
        assemble(g, (SWEEPS - 1) % 2, False)
        solve(g)
        z_v[g] = acc[...].astype(BF16)
        z_copies[g].start()
    for g in range(groups):
        wait_sends(g, (0, 1, 2, 3, 4))
        for s in range(2):
            @pl.when(has[s])
            def _():
                u_copy(g, s).wait_send()
    for c in u_copies + z_copies:
        c.wait()


def solution(mesh):
    col_count = mesh.shape['col']
    grid_spec = P('row', 'col', None)

    def device_fn(f_blk, u_blk, kappa_blk, mat_blk, omega_relax):
        rhs_count = u_blk.shape[2]
        groups = rhs_count // GROUP
        tiles = rhs_count // LANES
        vm = pltpu.VMEM
        dma = pltpu.SemaphoreType.DMA
        coeff = vm((CELLS, LANES), F32)
        u_last, z_last = pl.pallas_call(
            functools.partial(kernel, groups, col_count),
            out_shape=(jax.ShapeDtypeStruct((CELLS, rhs_count), F32), jax.ShapeDtypeStruct((CELLS, rhs_count), BF16)),
            in_specs=[pl.BlockSpec(memory_space=pl.ANY), pl.BlockSpec(memory_space=pl.ANY),
                      pl.BlockSpec(memory_space=pltpu.VMEM), pl.BlockSpec(memory_space=pl.ANY),
                      pl.BlockSpec(memory_space=pltpu.SMEM)],
            out_specs=(pl.BlockSpec(memory_space=pl.ANY), pl.BlockSpec(memory_space=pl.ANY)),
            scratch_shapes=[
                vm((EXT * EXT, CELLS), BF16),
                vm((CELLS, DEPTH), BF16),
                vm((CELLS, GROUP), F32),
                vm((tiles, CELLS, LANES), F32),
                vm((tiles, CELLS + 2 * PAD, LANES), F32),
                vm((tiles, CELLS, LANES), F32),
                vm((groups, DEPTH, GROUP), BF16),
                vm((groups, CELLS, GROUP), BF16),
                vm((CELLS + 2 * PAD, LANES), F32),
                coeff, coeff, coeff, coeff, coeff,
                vm((2, SUB, LANES), F32),
                vm((2, SUB, LANES), F32),
                vm((SUB, LANES), F32),
                vm((groups, 2, SUB, GROUP), F32),
                vm((groups, 2, 128, GROUP), BF16),
                vm((groups, 2, SUB, GROUP), F32),
                vm((2, groups, 2, SUB, GROUP), F32),
                vm((2, groups, 2, 128, GROUP), BF16),
                vm((groups, 2, SUB, GROUP), F32),
                vm((groups, TILES, SUB, LANES), F32),
                vm((groups, TILES, SUB, LANES), F32),
                vm((2, SUB, LANES), F32),
                vm((2, SUB, LANES), F32),
                vm((SUB, LANES), F32),
                dma((3, tiles)), dma, dma((groups,)),
                dma((groups, 2, 5)), dma((2, groups, 2, 5)),
                dma((groups, 2)), dma((groups, 2)),
                dma((groups,)), dma((groups,)),
                dma((groups, 2)), dma((groups, 2)),
                dma((3,)), dma((3,)),
            ],
            compiler_params=pltpu.CompilerParams(collective_id=0, has_side_effects=True,
                                                 vmem_limit_bytes=60 * 1024 * 1024),
        )(f_blk.reshape(CELLS, rhs_count), u_blk.reshape(CELLS, rhs_count), kappa_blk,
          mat_blk.reshape(CELLS, EXT * EXT).T, omega_relax.reshape(1))
        return (u_last + omega_relax * z_last.astype(F32)).reshape(SUB, SUB, rhs_count)

    return jax.shard_map(device_fn, mesh=mesh,
                         in_specs=(grid_spec, grid_spec, P('row', 'col'), P('row', 'col', None, None), P()),
                         out_specs=grid_spec, check_vma=False)
```

```python
import functools
import jax
import jax.numpy as jnp
from jax import lax
from jax.experimental import pallas as pl
from jax.experimental.pallas import tpu as pltpu
from jax.sharding import PartitionSpec as P

SWEEPS = 6
SUB = 32
MARGIN = 4
EXT = SUB + 2 * MARGIN
CELLS = SUB * SUB
LANES = 128
TILES = 2
GROUP = TILES * LANES
COLS_AT = CELLS
ROWS_AT = CELLS + 256
CORN_AT = ROWS_AT + 128
DEPTH = CORN_AT + 128
PAD = SUB
MESH = pl.DeviceIdType.MESH
F32 = jnp.float32
BF16 = jnp.bfloat16


def own_source(n):
    return ((n >> 5) + MARGIN) * EXT + (n & 31) + MARGIN


def side_column(side, dist):
    return jnp.where(side == 0, MARGIN - 1 - dist, MARGIN + SUB + dist)


def kernel(groups, col_count,
           f_hbm, u_hbm, kap_ref, mat_hbm, om_ref, u_out, z_out,
           mat_v, mat_t, mat_p, acc, res, zf, u_v, e_v, z_v, kb, cd, cn, cs, cw, ce, cedge, cedge_om, crow,
           send_p, send_b, send_u, recv_p, recv_b, recv_u, zrow_s, zrow, kcol_s, kcol_r, krow_r,
           in_sem, mat_sem, out_sem, s_sem, r_sem, su_sem, ru_sem,
           sz_sem, rz_sem, sf_sem, rf_sem, sk_sem, rk_sem):
    col = lax.axis_index('col')
    row = lax.axis_index('row')
    has = (col > 0, col < col_count - 1)
    side_dev = ((col - 1, row), (col + 1, row))
    partner = (col, 1 - row)
    brow = (SUB - 1) * (1 - row)
    om = om_ref[0]

    loads = []
    for g in range(groups):
        for t in range(TILES):
            k = g * TILES + t
            lanes = pl.ds(k * LANES, LANES)
            loads.append((
                pltpu.make_async_copy(u_hbm.at[:, lanes], zf.at[k, pl.ds(PAD, CELLS)], in_sem.at[0, k]),
                pltpu.make_async_copy(f_hbm.at[:, lanes], res.at[k], in_sem.at[1, k]),
                pltpu.make_async_copy(u_hbm.at[:, lanes], u_v.at[k], in_sem.at[2, k])))
    for a, b, c in loads:
        a.start()
        b.start()
    mat_copy = pltpu.make_async_copy(mat_hbm, mat_v, mat_sem)
    mat_copy.start()
    for a, b, c in loads:
        c.start()

    barrier = pltpu.get_barrier_semaphore()
    pl.semaphore_signal(barrier, inc=1, device_id=partner, device_id_type=MESH)
    for s in range(2):
        @pl.when(has[s])
        def _():
            pl.semaphore_signal(barrier, inc=1, device_id=side_dev[s], device_id_type=MESH)
    waits = 1 + has[0].astype(jnp.int32) + has[1].astype(jnp.int32)
    pl.semaphore_wait(barrier, waits)

    zero_row = jnp.zeros((SUB, LANES), F32)
    kap_t = jnp.transpose(jnp.concatenate([kap_ref[...], jnp.zeros((LANES - SUB, SUB), F32)], axis=0))
    kb[pl.ds(0, SUB)] = zero_row
    kb[pl.ds(PAD + CELLS, SUB)] = zero_row
    for r in range(SUB):
        kb[pl.ds(PAD + r * SUB, SUB)] = jnp.broadcast_to(kap_t[:, r:r + 1], (SUB, LANES))

    def kcol_copy(s):
        return pltpu.make_async_remote_copy(kcol_s.at[s], kcol_r.at[1 - s], sk_sem.at[s], rk_sem.at[1 - s],
                                            device_id=side_dev[s], device_id_type=MESH)

    def krow_copy():
        return pltpu.make_async_remote_copy(kb.at[pl.ds(PAD + brow * SUB, SUB)], krow_r, sk_sem.at[2], rk_sem.at[2],
                                            device_id=partner, device_id_type=MESH)

    edge_col = (0, SUB - 1)

    def edge_cells(c, at=0):
        return pl.ds(at + c, SUB, stride=SUB)

    for s in range(2):
        kcol_s[s] = kb[edge_cells(edge_col[s], PAD), :]

        @pl.when(has[s])
        def _():
            kcol_copy(s).start()
    krow_copy().start()

    sub_id = lax.broadcasted_iota(jnp.int32, (SUB, LANES), 0)
    no_w = jnp.where(has[0], 0.0, 1.0)
    no_e = jnp.where(has[1], 0.0, 1.0)

    def coeff_row(q, carry):
        base = pl.multiple_of(q * SUB, SUB)
        here = kb[pl.ds(PAD + base, SUB)]
        up = kb[pl.ds(base, SUB)]
        down = kb[pl.ds(2 * PAD + base, SUB)]
        left = jnp.concatenate([here[:1], here[:-1]], axis=0)
        right = jnp.concatenate([here[1:], here[-1:]], axis=0)
        vn = jnp.where(q == 0, 0.0, 1.0) * (0.5 * (here + up))
        vs = jnp.where(q == SUB - 1, 0.0, 1.0) * (0.5 * (here + down))
        vw = jnp.where(sub_id == 0, 0.0, 0.5 * (here + left))
        ve = jnp.where(sub_id == SUB - 1, 0.0, 0.5 * (here + right))
        rim = jnp.where(jnp.logical_or(jnp.logical_and(q == 0, row == 0),
                                       jnp.logical_and(q == SUB - 1, row == 1)), 1.0, 0.0)
        rim_col = jnp.where(sub_id == 0, no_w, 0.0) + jnp.where(sub_id == SUB - 1, no_e, 0.0)
        rows = pl.ds(base, SUB)
        cn[rows] = vn
        cs[rows] = vs
        cw[rows] = vw
        ce[rows] = ve
        cd[rows] = vn + vs + vw + ve + (rim + rim_col) * here
        return carry

    lax.fori_loop(0, SUB, coeff_row, 0)

    def stencil(g, first, count, unroll):
        def one_row(q, carry):
            for at, n in zip(first, count):
                base = pl.multiple_of(q * SUB + at, 8)
                rows = pl.ds(base, n)
                vd, vn, vs, vw, ve = cd[rows], cn[rows], cs[rows], cw[rows], ce[rows]
                for t in range(TILES):
                    k = g * TILES + t
                    part = (vd * zf[k, pl.ds(PAD + base, n)]
                            - vn * zf[k, pl.ds(base, n)]
                            - vs * zf[k, pl.ds(2 * PAD + base, n)]
                            - vw * zf[k, pl.ds(PAD - 1 + base, n)]
                            - ve * zf[k, pl.ds(PAD + 1 + base, n)])
                    res[k, rows] = res[k, rows] - part
            return carry

        lax.fori_loop(0, SUB, one_row, 0, unroll=unroll)

    def stencil_sides(g):
        stencil(g, (0, SUB - 8), (8, 8), 4)

    def stencil_middle(g):
        stencil(g, (8,), (16,), 4)

    def zrow_copy(g):
        return pltpu.make_async_remote_copy(
            zrow_s.at[g], zrow.at[g], sz_sem.at[g], rz_sem.at[g], device_id=partner, device_id_type=MESH)

    brows = pl.ds(pl.multiple_of(brow * SUB, SUB), SUB)

    def row_fix(g):
        for t in range(TILES):
            k = g * TILES + t
            res[k, brows] = res[k, brows] - crow[...] * (zrow_s[g, t] - zrow[g, t])

    def near(s, dist):
        return dist if s == 0 else SUB - 1 - dist

    far = row
    closer = 1 - row

    def message(g, s, slot, i):
        half = (far, closer)[(i - 1) // 2]
        if i in (1, 3):
            rows = pl.ds(pl.multiple_of(16 * half, 16), 16)
            src, dst = send_p, recv_p
        else:
            rows = pl.ds(0, SUB) if i == 0 else pl.ds(pl.multiple_of(SUB + 48 * half, 16), 48)
            src, dst = send_b, recv_b
        return pltpu.make_async_remote_copy(src.at[g, s, rows], dst.at[slot, g, 1 - s, rows], s_sem.at[g, s, i],
                                            r_sem.at[slot, g, 1 - s, i], device_id=side_dev[s], device_id_type=MESH)

    def u_copy(g, s):
        return pltpu.make_async_remote_copy(send_u.at[g, s], recv_u.at[g, 1 - s], su_sem.at[g, s],
                                            ru_sem.at[g, 1 - s], device_id=side_dev[s], device_id_type=MESH)

    def fill_z(g, first):
        for s in range(2):
            for t in range(TILES):
                lanes = pl.ds(t * LANES, LANES)
                zedge = zf[g * TILES + t, edge_cells(near(s, 0), PAD), :]
                if first:
                    send_u[g, s, :, lanes] = zedge
                else:
                    send_b[g, s, pl.ds(0, SUB), lanes] = zedge.astype(BF16)

    def fill_half(g, h):
        at = pl.multiple_of(CELLS // 2 * h, CELLS // 2)
        p_at = pl.multiple_of(16 * h, 16)
        e_at = pl.multiple_of(SUB + 48 * h, 16)
        for s in range(2):
            for t in range(TILES):
                k = g * TILES + t
                lanes = pl.ds(t * LANES, LANES)
                for d in range(MARGIN):
                    part = res[k, pl.ds(at + near(s, d), 16, stride=SUB), :]
                    if d == 0:
                        send_p[g, s, pl.ds(p_at, 16), lanes] = part
                    else:
                        send_b[g, s, pl.ds(e_at + 16 * (d - 1), 16), lanes] = part.astype(BF16)

    def start(g, slot, which):
        for s in range(2):
            @pl.when(has[s])
            def _():
                for i in which:
                    message(g, s, slot, i).start()

    def fwd_copies(g):
        rows = pl.multiple_of((SUB - MARGIN) * SUB * (1 - row), 128)
        half = pl.multiple_of(COLS_AT + 128 * (1 - row), 128)
        return [
            pltpu.make_async_remote_copy(e_v.at[g, pl.ds(rows, 128)], e_v.at[g, pl.ds(ROWS_AT, 128)],
                                         sf_sem.at[g, 0], rf_sem.at[g, 0], device_id=partner, device_id_type=MESH),
            pltpu.make_async_remote_copy(e_v.at[g, pl.ds(half, 128)], e_v.at[g, pl.ds(CORN_AT, 128)],
                                         sf_sem.at[g, 1], rf_sem.at[g, 1], device_id=partner, device_id_type=MESH)]

    def assemble(g, slot, first):
        for s in range(2):
            @pl.when(has[s])
            def _():
                if first:
                    u_copy(g, 1 - s).wait_recv()
                for i in range(1 if first else 0, 5):
                    message(g, 1 - s, slot, i).wait_recv()
                for t in range(TILES):
                    k = g * TILES + t
                    lanes = pl.ds(t * LANES, LANES)
                    if first:
                        theirs = recv_u[g, s, :, lanes]
                    else:
                        theirs = recv_b[slot, g, s, pl.ds(0, SUB), lanes].astype(F32)
                    cells = edge_cells(edge_col[s])
                    coeff = cedge[s] if first else cedge_om[s]
                    flux = coeff * (zf[k, edge_cells(edge_col[s], PAD), :] - theirs)
                    res[k, cells, :] = res[k, cells, :] - flux
                    halo = (recv_p[slot, g, s, :, lanes] + flux).astype(BF16)
                    for h in range(2):
                        at = COLS_AT + 128 * h + 64 * s
                        e_v[g, pl.ds(at, 16), lanes] = halo[16 * h:16 * h + 16]
                        e_v[g, pl.ds(at + 16, 48), lanes] = recv_b[slot, g, s, pl.ds(SUB + 48 * h, 48), lanes]

        def pack(rows):
            for t in range(TILES):
                e_v[g, rows, pl.ds(t * LANES, LANES)] = res[g * TILES + t, rows].astype(BF16)

        fwd_rows, fwd_corners = fwd_copies(g)
        fwd_corners.start()
        pack(pl.ds(pl.multiple_of((SUB - MARGIN) * SUB * (1 - row), 128), 128))
        rest = pl.multiple_of(128 * row, 128)

        def pack_rest(q, carry):
            pack(pl.ds(pl.multiple_of(rest + q * 128, 128), 128))
            return carry

        fwd_rows.start()
        lax.fori_loop(0, CELLS // 128 - 1, pack_rest, 0)

    def solve(g):
        acc[...] = jnp.dot(mat_p[:, :ROWS_AT], e_v[g, pl.ds(0, ROWS_AT)], preferred_element_type=F32)
        for c in fwd_copies(g):
            c.wait()
        acc[...] += jnp.dot(mat_p[:, ROWS_AT:], e_v[g, pl.ds(ROWS_AT, DEPTH - ROWS_AT)], preferred_element_type=F32)

    def round_row(g):
        for t in range(TILES):
            zrow_s[g, t] = acc[brows, pl.ds(t * LANES, LANES)].astype(BF16).astype(F32)

    def update(g):
        def rows_of(q, carry):
            rows = pl.ds(pl.multiple_of(q * 64, 64), 64)
            for t in range(TILES):
                k = g * TILES + t
                z = acc[rows, pl.ds(t * LANES, LANES)].astype(BF16).astype(F32)
                zf[k, pl.ds(pl.multiple_of(PAD + q * 64, PAD), 64)] = z
                u_v[k, rows] = u_v[k, rows] + om * z
            return carry

        lax.fori_loop(0, CELLS // 64, rows_of, 0)

    for k in range(groups * TILES):
        zf[k, pl.ds(0, PAD)] = zero_row
        zf[k, pl.ds(PAD + CELLS, PAD)] = zero_row
    for g in range(groups):
        e_v[g, pl.ds(COLS_AT, 256)] = jnp.zeros((256, GROUP), BF16)

    krow_copy().wait()
    rows_b = pl.ds(pl.multiple_of(PAD + brow * SUB, SUB), SUB)
    crow[...] = 0.5 * (kb[rows_b] + krow_r[...])

    def send_bands(g, slot):
        stencil_sides(g)
        fill_half(g, far)
        start(g, slot, (1, 2))
        zrow_copy(g).wait()
        row_fix(g)
        fill_half(g, closer)
        start(g, slot, (3, 4))
        stencil_middle(g)

    for g in range(groups):
        for t in range(TILES):
            loads[g * TILES + t][0].wait()
        for t in range(TILES):
            zrow_s[g, t] = zf[g * TILES + t, rows_b]
        zrow_copy(g).start()
        fill_z(g, True)
        for s in range(2):
            @pl.when(has[s])
            def _():
                u_copy(g, s).start()
        for t in range(TILES):
            loads[g * TILES + t][1].wait()
        send_bands(g, 0)

    mat_copy.wait()
    for at in range(0, EXT * EXT, 256):
        span = pl.ds(at, min(256, EXT * EXT - at))
        mat_t[:, span] = mat_v[span].T

    def place(at, width, start, window, source, ok=None):
        n = lax.broadcasted_iota(jnp.int32, (window, width), 1)
        k = lax.broadcasted_iota(jnp.int32, (window, width), 0) + start
        pick = source(n) == k
        if ok is not None:
            pick = jnp.logical_and(pick, ok(n))
        pick = jnp.where(pick, 1.0, 0.0).astype(BF16)

        acc[...] = jnp.dot(mat_t[:, pl.ds(start, window)], pick, preferred_element_type=F32)
        mat_p[:, pl.ds(at, width)] = acc[...].astype(BF16)

    for q in range(4):
        low = (320 * q + 164) // 128 * 128
        high = -(-(320 * q + 476) // 128) * 128
        place(256 * q, 256, low, high - low, lambda n, q=q: own_source(n + 256 * q))

    def side_source(n):
        r = 16 * (n >> 7) + (n & 15)
        return (r + MARGIN) * EXT + side_column((n >> 6) & 1, (n >> 4) & 3)

    place(COLS_AT, 256, 128, 1408, side_source)

    def row_source(n):
        m = n & 127
        first_row = jnp.where(row == 0, MARGIN + SUB, 0)
        halo = (first_row + (m >> 5)) * EXT + MARGIN + (m & 31)
        corner_row = jnp.where(row == 0, MARGIN + SUB, -12) + (m & 15)
        corner = corner_row * EXT + side_column((m >> 6) & 1, (m >> 4) & 3)
        return jnp.where(n < 128, halo, corner)

    def row_ok(n):
        r16 = n & 15
        return jnp.logical_or(n < 128, jnp.where(row == 0, r16, 15 - r16) < MARGIN)

    place(ROWS_AT, 256, pl.multiple_of(1408 * (1 - row), 128), 192, row_source, row_ok)

    for s in range(2):
        @pl.when(has[s])
        def _():
            kcol_copy(1 - s).wait_recv()
            cedge[s] = 0.5 * (kcol_s[s] + kcol_r[s])
            cedge_om[s] = om * cedge[s]
            kcol_copy(s).wait_send()
    crow[...] = om * crow[...]

    def scale(q, carry):
        rows = pl.ds(pl.multiple_of(q * SUB, SUB), SUB)
        for c in (cd, cn, cs, cw, ce):
            c[rows] = om * c[rows]
        return carry

    lax.fori_loop(0, SUB, scale, 0)
    for k in range(groups * TILES):
        loads[k][2].wait()

    def wait_sends(g, which):
        for s in range(2):
            @pl.when(has[s])
            def _():
                for i in which:
                    message(g, s, 0, i).wait_send()

    def advance(g, slot, first):
        solve(g)
        round_row(g)
        zrow_copy(g).start()
        update(g)
        if first:
            wait_sends(g, (1, 2, 3, 4))
        else:
            wait_sends(g, (0, 1, 2, 3, 4))
        fill_z(g, False)
        start(g, slot, (0,))
        send_bands(g, slot)

    for g in range(groups):
        assemble(g, 0, True)
        advance(g, 1, True)

    def step(i, carry):
        t = i // groups
        g = lax.rem(i, groups)
        slot = lax.rem(t, 2)
        assemble(g, 1 - slot, False)
        advance(g, slot, False)
        return carry

    lax.fori_loop(2 * groups, SWEEPS * groups, step, 0)

    u_copies = [pltpu.make_async_copy(u_v.at[k], u_out.at[:, pl.ds(k * LANES, LANES)], in_sem.at[0, k])
                for k in range(groups * TILES)]
    z_copies = [pltpu.make_async_copy(z_v.at[g], z_out.at[:, pl.ds(g * GROUP, GROUP)], out_sem.at[g])
                for g in range(groups)]
    for g in range(groups):
        for t in range(TILES):
            u_copies[g * TILES + t].start()
    for g in range(groups):
        assemble(g, (SWEEPS - 1) % 2, False)
        solve(g)
        z_v[g] = acc[...].astype(BF16)
        z_copies[g].start()
    for g in range(groups):
        wait_sends(g, (0, 1, 2, 3, 4))
        for s in range(2):
            @pl.when(has[s])
            def _():
                u_copy(g, s).wait_send()
    for c in u_copies + z_copies:
        c.wait()


def solution(mesh):
    col_count = mesh.shape['col']
    grid_spec = P('row', 'col', None)

    def device_fn(f_blk, u_blk, kappa_blk, mat_blk, omega_relax):
        rhs_count = u_blk.shape[2]
        groups = rhs_count // GROUP
        tiles = rhs_count // LANES
        vm = pltpu.VMEM
        dma = pltpu.SemaphoreType.DMA
        coeff = vm((CELLS, LANES), F32)
        u_last, z_last = pl.pallas_call(
            functools.partial(kernel, groups, col_count),
            out_shape=(jax.ShapeDtypeStruct((CELLS, rhs_count), F32), jax.ShapeDtypeStruct((CELLS, rhs_count), BF16)),
            in_specs=[pl.BlockSpec(memory_space=pltpu.HBM), pl.BlockSpec(memory_space=pltpu.HBM),
                      pl.BlockSpec(memory_space=pltpu.VMEM), pl.BlockSpec(memory_space=pltpu.HBM),
                      pl.BlockSpec(memory_space=pltpu.SMEM)],
            out_specs=(pl.BlockSpec(memory_space=pl.ANY), pl.BlockSpec(memory_space=pl.ANY)),
            scratch_shapes=[
                vm((EXT * EXT, CELLS), BF16),
                vm((CELLS, EXT * EXT), BF16),
                vm((CELLS, DEPTH), BF16),
                vm((CELLS, GROUP), F32),
                vm((tiles, CELLS, LANES), F32),
                vm((tiles, CELLS + 2 * PAD, LANES), F32),
                vm((tiles, CELLS, LANES), F32),
                vm((groups, DEPTH, GROUP), BF16),
                vm((groups, CELLS, GROUP), BF16),
                vm((CELLS + 2 * PAD, LANES), F32),
                coeff, coeff, coeff, coeff, coeff,
                vm((2, SUB, LANES), F32),
                vm((2, SUB, LANES), F32),
                vm((SUB, LANES), F32),
                vm((groups, 2, SUB, GROUP), F32),
                vm((groups, 2, 128, GROUP), BF16),
                vm((groups, 2, SUB, GROUP), F32),
                vm((2, groups, 2, SUB, GROUP), F32),
                vm((2, groups, 2, 128, GROUP), BF16),
                vm((groups, 2, SUB, GROUP), F32),
                vm((groups, TILES, SUB, LANES), F32),
                vm((groups, TILES, SUB, LANES), F32),
                vm((2, SUB, LANES), F32),
                vm((2, SUB, LANES), F32),
                vm((SUB, LANES), F32),
                dma((3, tiles)), dma, dma((groups,)),
                dma((groups, 2, 5)), dma((2, groups, 2, 5)),
                dma((groups, 2)), dma((groups, 2)),
                dma((groups,)), dma((groups,)),
                dma((groups, 2)), dma((groups, 2)),
                dma((3,)), dma((3,)),
            ],
            compiler_params=pltpu.CompilerParams(collective_id=0, has_side_effects=True,
                                                 vmem_limit_bytes=50 * 1024 * 1024),
        )(f_blk.reshape(CELLS, rhs_count), u_blk.reshape(CELLS, rhs_count), kappa_blk,
          mat_blk.reshape(CELLS, EXT * EXT).T, omega_relax.reshape(1))
        return (u_last + omega_relax * z_last.astype(F32)).reshape(SUB, SUB, rhs_count)

    return jax.shard_map(device_fn, mesh=mesh,
                         in_specs=(grid_spec, grid_spec, P('row', 'col'), P('row', 'col', None, None), P()),
                         out_specs=grid_spec, check_vma=False)
```

```python
import functools
import jax
import jax.numpy as jnp
from jax import lax
from jax.experimental import pallas as pl
from jax.experimental.pallas import tpu as pltpu
from jax.sharding import PartitionSpec as P

SWEEPS = 6
SUB = 32
MARGIN = 4
EXT = SUB + 2 * MARGIN
CELLS = SUB * SUB
LANES = 128
TILES = 2
GROUP = TILES * LANES
COLS_AT = CELLS
ROWS_AT = CELLS + 256
CORN_AT = ROWS_AT + 128
DEPTH = CORN_AT + 128
PAD = SUB
MESH = pl.DeviceIdType.MESH
F32 = jnp.float32
BF16 = jnp.bfloat16


def own_source(n):
    return ((n >> 5) + MARGIN) * EXT + (n & 31) + MARGIN


def mod(t, n):
    return t % n if isinstance(t, int) else lax.rem(t, n)


def side_column(side, dist):
    return jnp.where(side == 0, MARGIN - 1 - dist, MARGIN + SUB + dist)


def kernel(groups, col_count,
           f_hbm, u_hbm, kap_ref, mat_hbm, om_ref, u_out, z_out,
           mat_v, mat_t, mat_p, acc, res, zf, u_v, e_v, z_v, kb, cd, cn, cs, cw, ce, cedge, cedge_om, crow,
           send_p, send_b, send_u, recv_p, recv_b, recv_u, zrow_s, zrow, kcol_s, kcol_r, krow_r,
           via_p, via_b, via_u,
           in_sem, mat_sem, out_sem, s_sem, r_sem,
           sz_sem, rz_sem, sf_sem, rf_sem, sk_sem, rk_sem, vs_sem, vr_sem):
    col = lax.axis_index('col')
    row = lax.axis_index('row')
    has = (col > 0, col < col_count - 1)
    side_dev = ((col - 1, row), (col + 1, row))
    partner = (col, 1 - row)
    brow = (SUB - 1) * (1 - row)
    om = om_ref[0]

    routed = row == 1
    detour = (jnp.logical_and(routed, col == 2), jnp.logical_and(routed, col == 1))
    is_via = jnp.logical_and(routed, jnp.logical_or(col == 0, col == 3))
    mate = (lax.rem(col + 2, 4), row)
    via_to = (jnp.where(col == 0, 1, 2), row)
    via_side = jnp.where(col == 0, 1, 0)

    loads = []
    for g in range(groups):
        for t in range(TILES):
            k = g * TILES + t
            lanes = pl.ds(k * LANES, LANES)
            loads.append((
                pltpu.make_async_copy(u_hbm.at[:, lanes], zf.at[k, pl.ds(PAD, CELLS)], in_sem.at[0, k]),
                pltpu.make_async_copy(f_hbm.at[:, lanes], res.at[k], in_sem.at[1, k]),
                pltpu.make_async_copy(u_hbm.at[:, lanes], u_v.at[k], in_sem.at[2, k])))
    for a, b, c in loads:
        a.start()
        b.start()
    mat_copy = pltpu.make_async_copy(mat_hbm, mat_v, mat_sem)
    mat_copy.start()
    for a, b, c in loads:
        c.start()

    barrier = pltpu.get_barrier_semaphore()
    pl.semaphore_signal(barrier, inc=1, device_id=partner, device_id_type=MESH)
    for s in range(2):
        @pl.when(has[s])
        def _():
            pl.semaphore_signal(barrier, inc=1, device_id=side_dev[s], device_id_type=MESH)
    @pl.when(routed)
    def _():
        pl.semaphore_signal(barrier, inc=1, device_id=mate, device_id_type=MESH)
    waits = 1 + has[0].astype(jnp.int32) + has[1].astype(jnp.int32) + routed.astype(jnp.int32)
    pl.semaphore_wait(barrier, waits)

    zero_row = jnp.zeros((SUB, LANES), F32)
    kap_t = jnp.transpose(jnp.concatenate([kap_ref[...], jnp.zeros((LANES - SUB, SUB), F32)], axis=0))
    kb[pl.ds(0, SUB)] = zero_row
    kb[pl.ds(PAD + CELLS, SUB)] = zero_row
    for r in range(SUB):
        kb[pl.ds(PAD + r * SUB, SUB)] = jnp.broadcast_to(kap_t[:, r:r + 1], (SUB, LANES))

    def kcol_copy(s):
        return pltpu.make_async_remote_copy(kcol_s.at[s], kcol_r.at[1 - s], sk_sem.at[s], rk_sem.at[1 - s],
                                            device_id=side_dev[s], device_id_type=MESH)

    def krow_copy():
        return pltpu.make_async_remote_copy(kb.at[pl.ds(PAD + brow * SUB, SUB)], krow_r, sk_sem.at[2], rk_sem.at[2],
                                            device_id=partner, device_id_type=MESH)

    edge_col = (0, SUB - 1)

    def edge_cells(c, at=0):
        return pl.ds(at + c, SUB, stride=SUB)

    for s in range(2):
        kcol_s[s] = kb[edge_cells(edge_col[s], PAD), :]

        @pl.when(has[s])
        def _():
            kcol_copy(s).start()
    krow_copy().start()

    sub_id = lax.broadcasted_iota(jnp.int32, (SUB, LANES), 0)
    no_w = jnp.where(has[0], 0.0, 1.0)
    no_e = jnp.where(has[1], 0.0, 1.0)

    def coeff_row(q, carry):
        base = pl.multiple_of(q * SUB, SUB)
        here = kb[pl.ds(PAD + base, SUB)]
        up = kb[pl.ds(base, SUB)]
        down = kb[pl.ds(2 * PAD + base, SUB)]
        left = jnp.concatenate([here[:1], here[:-1]], axis=0)
        right = jnp.concatenate([here[1:], here[-1:]], axis=0)
        vn = jnp.where(q == 0, 0.0, 1.0) * (0.5 * (here + up))
        vs = jnp.where(q == SUB - 1, 0.0, 1.0) * (0.5 * (here + down))
        vw = jnp.where(sub_id == 0, 0.0, 0.5 * (here + left))
        ve = jnp.where(sub_id == SUB - 1, 0.0, 0.5 * (here + right))
        rim = jnp.where(jnp.logical_or(jnp.logical_and(q == 0, row == 0),
                                       jnp.logical_and(q == SUB - 1, row == 1)), 1.0, 0.0)
        rim_col = jnp.where(sub_id == 0, no_w, 0.0) + jnp.where(sub_id == SUB - 1, no_e, 0.0)
        rows = pl.ds(base, SUB)
        cn[rows] = vn
        cs[rows] = vs
        cw[rows] = vw
        ce[rows] = ve
        cd[rows] = vn + vs + vw + ve + (rim + rim_col) * here
        return carry

    lax.fori_loop(0, SUB, coeff_row, 0)

    def stencil(g, first, count, unroll):
        def one_row(q, carry):
            for at, n in zip(first, count):
                base = pl.multiple_of(q * SUB + at, 8)
                rows = pl.ds(base, n)
                vd, vn, vs, vw, ve = cd[rows], cn[rows], cs[rows], cw[rows], ce[rows]
                for t in range(TILES):
                    k = g * TILES + t
                    part = (vd * zf[k, pl.ds(PAD + base, n)]
                            - vn * zf[k, pl.ds(base, n)]
                            - vs * zf[k, pl.ds(2 * PAD + base, n)]
                            - vw * zf[k, pl.ds(PAD - 1 + base, n)]
                            - ve * zf[k, pl.ds(PAD + 1 + base, n)])
                    res[k, rows] = res[k, rows] - part
            return carry

        lax.fori_loop(0, SUB, one_row, 0, unroll=unroll)

    def stencil_sides(g):
        stencil(g, (0, SUB - 8), (8, 8), 4)

    def stencil_middle(g):
        stencil(g, (8,), (16,), 4)

    def zrow_copy(g):
        return pltpu.make_async_remote_copy(
            zrow_s.at[g], zrow.at[g], sz_sem.at[g], rz_sem.at[g], device_id=partner, device_id_type=MESH)

    brows = pl.ds(pl.multiple_of(brow * SUB, SUB), SUB)

    def row_fix(g):
        for t in range(TILES):
            k = g * TILES + t
            res[k, brows] = res[k, brows] - crow[...] * (zrow_s[g, t] - zrow[g, t])

    def near(s, dist):
        return dist if s == 0 else SUB - 1 - dist

    far = row
    closer = 1 - row

    def part(g, i):
        half = (far, closer)[(i - 1) // 2 % 2]
        if i in (1, 3):
            return 1, pl.ds(pl.multiple_of(16 * half, 16), 16)
        if i in (2, 4):
            return 0, pl.ds(pl.multiple_of(SUB + 48 * half, 16), 48)
        return (0 if i == 0 else 2), pl.ds(0, SUB)

    def message(g, s, t, i):
        kind, rows = part(g, i)
        slot = mod(t, 2)
        src = (send_b, send_p, send_u)[kind].at[g, s, rows]
        dst = (recv_b, recv_p, recv_u)[kind].at[slot, g, 1 - s, rows]
        return pltpu.make_async_remote_copy(src, dst, s_sem.at[g, s, i], r_sem.at[slot, g, 1 - s, i],
                                            device_id=side_dev[s], device_id_type=MESH)

    def message_out(g, s, t, i):
        kind, rows = part(g, i)
        slot = mod(t, 3)
        src = (send_b, send_p, send_u)[kind].at[g, s, rows]
        dst = (via_b, via_p, via_u)[kind].at[slot, g, rows]
        return pltpu.make_async_remote_copy(src, dst, s_sem.at[g, s, i], vr_sem.at[slot, g, i],
                                            device_id=mate, device_id_type=MESH)

    def message_on(g, t, i):
        kind, rows = part(g, i)
        slot = mod(t, 2)
        src = (via_b, via_p, via_u)[kind].at[mod(t, 3), g, rows]
        dst = (recv_b, recv_p, recv_u)[kind].at[slot, g, via_side, rows]
        return pltpu.make_async_remote_copy(src, dst, vs_sem.at[g, i], r_sem.at[slot, g, via_side, i],
                                            device_id=via_to, device_id_type=MESH)

    SWEEP_PARTS = (0, 1, 2, 3, 4)
    FIRST_PARTS = (5, 1, 2, 3, 4)

    def pass_on(g, t, parts):
        @pl.when(is_via)
        def _():
            for i in parts:
                message_out(g, 0, t, i).wait_recv()
                message_on(g, t, i).start()

    def fill_z(g, first):
        for s in range(2):
            for t in range(TILES):
                lanes = pl.ds(t * LANES, LANES)
                zedge = zf[g * TILES + t, edge_cells(near(s, 0), PAD), :]
                if first:
                    send_u[g, s, :, lanes] = zedge
                else:
                    send_b[g, s, pl.ds(0, SUB), lanes] = zedge.astype(BF16)

    def fill_half(g, h):
        at = pl.multiple_of(CELLS // 2 * h, CELLS // 2)
        p_at = pl.multiple_of(16 * h, 16)
        e_at = pl.multiple_of(SUB + 48 * h, 16)
        for s in range(2):
            for t in range(TILES):
                k = g * TILES + t
                lanes = pl.ds(t * LANES, LANES)
                for d in range(MARGIN):
                    part = res[k, pl.ds(at + near(s, d), 16, stride=SUB), :]
                    if d == 0:
                        send_p[g, s, pl.ds(p_at, 16), lanes] = part
                    else:
                        send_b[g, s, pl.ds(e_at + 16 * (d - 1), 16), lanes] = part.astype(BF16)

    def start(g, t, which):
        for s in range(2):
            @pl.when(jnp.logical_and(has[s], jnp.logical_not(detour[s])))
            def _():
                for i in which:
                    message(g, s, t, i).start()

            @pl.when(detour[s])
            def _():
                for i in which:
                    message_out(g, s, t, i).start()

    def fwd_copies(g):
        rows = pl.multiple_of((SUB - MARGIN) * SUB * (1 - row), 128)
        half = pl.multiple_of(COLS_AT + 128 * (1 - row), 128)
        return [
            pltpu.make_async_remote_copy(e_v.at[g, pl.ds(rows, 128)], e_v.at[g, pl.ds(ROWS_AT, 128)],
                                         sf_sem.at[g, 0], rf_sem.at[g, 0], device_id=partner, device_id_type=MESH),
            pltpu.make_async_remote_copy(e_v.at[g, pl.ds(half, 128)], e_v.at[g, pl.ds(CORN_AT, 128)],
                                         sf_sem.at[g, 1], rf_sem.at[g, 1], device_id=partner, device_id_type=MESH)]

    def assemble(g, sent, first):
        slot = mod(sent, 2)
        for s in range(2):
            @pl.when(has[s])
            def _():
                for i in FIRST_PARTS if first else SWEEP_PARTS:
                    message(g, 1 - s, sent, i).wait_recv()
                for t in range(TILES):
                    k = g * TILES + t
                    lanes = pl.ds(t * LANES, LANES)
                    if first:
                        theirs = recv_u[slot, g, s, :, lanes]
                    else:
                        theirs = recv_b[slot, g, s, pl.ds(0, SUB), lanes].astype(F32)
                    cells = edge_cells(edge_col[s])
                    coeff = cedge[s] if first else cedge_om[s]
                    flux = coeff * (zf[k, edge_cells(edge_col[s], PAD), :] - theirs)
                    res[k, cells, :] = res[k, cells, :] - flux
                    halo = (recv_p[slot, g, s, :, lanes] + flux).astype(BF16)
                    for h in range(2):
                        at = COLS_AT + 128 * h + 64 * s
                        e_v[g, pl.ds(at, 16), lanes] = halo[16 * h:16 * h + 16]
                        e_v[g, pl.ds(at + 16, 48), lanes] = recv_b[slot, g, s, pl.ds(SUB + 48 * h, 48), lanes]

        def pack(rows):
            for t in range(TILES):
                e_v[g, rows, pl.ds(t * LANES, LANES)] = res[g * TILES + t, rows].astype(BF16)

        fwd_rows, fwd_corners = fwd_copies(g)
        fwd_corners.start()
        pack(pl.ds(pl.multiple_of((SUB - MARGIN) * SUB * (1 - row), 128), 128))
        rest = pl.multiple_of(128 * row, 128)

        def pack_rest(q, carry):
            pack(pl.ds(pl.multiple_of(rest + q * 128, 128), 128))
            return carry

        fwd_rows.start()
        lax.fori_loop(0, CELLS // 128 - 1, pack_rest, 0)

    def solve(g):
        acc[...] = jnp.dot(mat_p[:, :ROWS_AT], e_v[g, pl.ds(0, ROWS_AT)], preferred_element_type=F32)
        for c in fwd_copies(g):
            c.wait()
        acc[...] += jnp.dot(mat_p[:, ROWS_AT:], e_v[g, pl.ds(ROWS_AT, DEPTH - ROWS_AT)], preferred_element_type=F32)

    def round_row(g):
        for t in range(TILES):
            zrow_s[g, t] = acc[brows, pl.ds(t * LANES, LANES)].astype(BF16).astype(F32)

    def update(g):
        def rows_of(q, carry):
            rows = pl.ds(pl.multiple_of(q * 64, 64), 64)
            for t in range(TILES):
                k = g * TILES + t
                z = acc[rows, pl.ds(t * LANES, LANES)].astype(BF16).astype(F32)
                zf[k, pl.ds(pl.multiple_of(PAD + q * 64, PAD), 64)] = z
                u_v[k, rows] = u_v[k, rows] + om * z
            return carry

        lax.fori_loop(0, CELLS // 64, rows_of, 0)

    for k in range(groups * TILES):
        zf[k, pl.ds(0, PAD)] = zero_row
        zf[k, pl.ds(PAD + CELLS, PAD)] = zero_row
    for g in range(groups):
        e_v[g, pl.ds(COLS_AT, 256)] = jnp.zeros((256, GROUP), BF16)

    krow_copy().wait()
    rows_b = pl.ds(pl.multiple_of(PAD + brow * SUB, SUB), SUB)
    crow[...] = 0.5 * (kb[rows_b] + krow_r[...])

    def send_bands(g, t):
        stencil_sides(g)
        fill_half(g, far)
        start(g, t, (1, 2))
        zrow_copy(g).wait()
        row_fix(g)
        fill_half(g, closer)
        start(g, t, (3, 4))
        stencil_middle(g)

    for g in range(groups):
        for t in range(TILES):
            loads[g * TILES + t][0].wait()
        for t in range(TILES):
            zrow_s[g, t] = zf[g * TILES + t, rows_b]
        zrow_copy(g).start()
        fill_z(g, True)
        start(g, 0, (5,))
        for t in range(TILES):
            loads[g * TILES + t][1].wait()
        send_bands(g, 0)

    mat_copy.wait()
    for at in range(0, EXT * EXT, 256):
        span = pl.ds(at, min(256, EXT * EXT - at))
        mat_t[:, span] = mat_v[span].T
    pass_on(0, 0, FIRST_PARTS)

    def place(at, width, start, window, source, ok=None):
        n = lax.broadcasted_iota(jnp.int32, (window, width), 1)
        k = lax.broadcasted_iota(jnp.int32, (window, width), 0) + start
        pick = source(n) == k
        if ok is not None:
            pick = jnp.logical_and(pick, ok(n))
        pick = jnp.where(pick, 1.0, 0.0).astype(BF16)

        acc[...] = jnp.dot(mat_t[:, pl.ds(start, window)], pick, preferred_element_type=F32)
        mat_p[:, pl.ds(at, width)] = acc[...].astype(BF16)

    for q in range(4):
        low = (320 * q + 164) // 128 * 128
        high = -(-(320 * q + 476) // 128) * 128
        place(256 * q, 256, low, high - low, lambda n, q=q: own_source(n + 256 * q))

    def side_source(n):
        r = 16 * (n >> 7) + (n & 15)
        return (r + MARGIN) * EXT + side_column((n >> 6) & 1, (n >> 4) & 3)

    pass_on(1, 0, FIRST_PARTS)
    place(COLS_AT, 256, 128, 1408, side_source)

    def row_source(n):
        m = n & 127
        first_row = jnp.where(row == 0, MARGIN + SUB, 0)
        halo = (first_row + (m >> 5)) * EXT + MARGIN + (m & 31)
        corner_row = jnp.where(row == 0, MARGIN + SUB, -12) + (m & 15)
        corner = corner_row * EXT + side_column((m >> 6) & 1, (m >> 4) & 3)
        return jnp.where(n < 128, halo, corner)

    def row_ok(n):
        r16 = n & 15
        return jnp.logical_or(n < 128, jnp.where(row == 0, r16, 15 - r16) < MARGIN)

    place(ROWS_AT, 256, pl.multiple_of(1408 * (1 - row), 128), 192, row_source, row_ok)

    for s in range(2):
        @pl.when(has[s])
        def _():
            kcol_copy(1 - s).wait_recv()
            cedge[s] = 0.5 * (kcol_s[s] + kcol_r[s])
            cedge_om[s] = om * cedge[s]
            kcol_copy(s).wait_send()
    crow[...] = om * crow[...]

    def scale(q, carry):
        rows = pl.ds(pl.multiple_of(q * SUB, SUB), SUB)
        for c in (cd, cn, cs, cw, ce):
            c[rows] = om * c[rows]
        return carry

    lax.fori_loop(0, SUB, scale, 0)
    for k in range(groups * TILES):
        loads[k][2].wait()

    def wait_sends(g, which):
        for s in range(2):
            @pl.when(has[s])
            def _():
                for i in which:
                    message(g, s, 0, i).wait_send()

        @pl.when(is_via)
        def _():
            for i in which:
                message_on(g, 0, i).wait_send()

    def advance(g, t, first, relay):
        solve(g)
        round_row(g)
        zrow_copy(g).start()
        update(g)
        wait_sends(g, FIRST_PARTS if first else SWEEP_PARTS)
        fill_z(g, False)
        start(g, t, (0,))
        if relay is not None:
            pass_on(*relay)
        send_bands(g, t)

    assemble(0, 0, True)
    advance(0, 1, True, None)
    assemble(1, 0, True)
    advance(1, 1, True, (0, 1, SWEEP_PARTS))

    def step(i, carry):
        t = i // groups
        g = lax.rem(i, groups)
        assemble(g, t - 1, False)
        advance(g, t, False, (1 - g, jnp.where(g == 0, t - 1, t), SWEEP_PARTS))
        return carry

    lax.fori_loop(2 * groups, SWEEPS * groups, step, 0)

    u_copies = [pltpu.make_async_copy(u_v.at[k], u_out.at[:, pl.ds(k * LANES, LANES)], in_sem.at[0, k])
                for k in range(groups * TILES)]
    z_copies = [pltpu.make_async_copy(z_v.at[g], z_out.at[:, pl.ds(g * GROUP, GROUP)], out_sem.at[g])
                for g in range(groups)]
    for g in range(groups):
        for t in range(TILES):
            u_copies[g * TILES + t].start()
    for g in range(groups):
        assemble(g, SWEEPS - 1, False)
        solve(g)
        z_v[g] = acc[...].astype(BF16)
        z_copies[g].start()
        if g == 0:
            pass_on(1, SWEEPS - 1, SWEEP_PARTS)
    for g in range(groups):
        wait_sends(g, SWEEP_PARTS)
    for c in u_copies + z_copies:
        c.wait()


def solution(mesh):
    col_count = mesh.shape['col']
    grid_spec = P('row', 'col', None)

    def device_fn(f_blk, u_blk, kappa_blk, mat_blk, omega_relax):
        rhs_count = u_blk.shape[2]
        groups = rhs_count // GROUP
        tiles = rhs_count // LANES
        vm = pltpu.VMEM
        dma = pltpu.SemaphoreType.DMA
        coeff = vm((CELLS, LANES), F32)
        u_last, z_last = pl.pallas_call(
            functools.partial(kernel, groups, col_count),
            out_shape=(jax.ShapeDtypeStruct((CELLS, rhs_count), F32), jax.ShapeDtypeStruct((CELLS, rhs_count), BF16)),
            in_specs=[pl.BlockSpec(memory_space=pltpu.HBM), pl.BlockSpec(memory_space=pltpu.HBM),
                      pl.BlockSpec(memory_space=pltpu.VMEM), pl.BlockSpec(memory_space=pltpu.HBM),
                      pl.BlockSpec(memory_space=pltpu.SMEM)],
            out_specs=(pl.BlockSpec(memory_space=pl.ANY), pl.BlockSpec(memory_space=pl.ANY)),
            scratch_shapes=[
                vm((EXT * EXT, CELLS), BF16),
                vm((CELLS, EXT * EXT), BF16),
                vm((CELLS, DEPTH), BF16),
                vm((CELLS, GROUP), F32),
                vm((tiles, CELLS, LANES), F32),
                vm((tiles, CELLS + 2 * PAD, LANES), F32),
                vm((tiles, CELLS, LANES), F32),
                vm((groups, DEPTH, GROUP), BF16),
                vm((groups, CELLS, GROUP), BF16),
                vm((CELLS + 2 * PAD, LANES), F32),
                coeff, coeff, coeff, coeff, coeff,
                vm((2, SUB, LANES), F32),
                vm((2, SUB, LANES), F32),
                vm((SUB, LANES), F32),
                vm((groups, 2, SUB, GROUP), F32),
                vm((groups, 2, 128, GROUP), BF16),
                vm((groups, 2, SUB, GROUP), F32),
                vm((2, groups, 2, SUB, GROUP), F32),
                vm((2, groups, 2, 128, GROUP), BF16),
                vm((1, groups, 2, SUB, GROUP), F32),
                vm((groups, TILES, SUB, LANES), F32),
                vm((groups, TILES, SUB, LANES), F32),
                vm((2, SUB, LANES), F32),
                vm((2, SUB, LANES), F32),
                vm((SUB, LANES), F32),
                vm((3, groups, SUB, GROUP), F32),
                vm((3, groups, 128, GROUP), BF16),
                vm((1, groups, SUB, GROUP), F32),
                dma((3, tiles)), dma, dma((groups,)),
                dma((groups, 2, 6)), dma((2, groups, 2, 6)),
                dma((groups,)), dma((groups,)),
                dma((groups, 2)), dma((groups, 2)),
                dma((3,)), dma((3,)),
                dma((groups, 6)), dma((3, groups, 6)),
            ],
            compiler_params=pltpu.CompilerParams(collective_id=0, has_side_effects=True,
                                                 vmem_limit_bytes=50 * 1024 * 1024),
        )(f_blk.reshape(CELLS, rhs_count), u_blk.reshape(CELLS, rhs_count), kappa_blk,
          mat_blk.reshape(CELLS, EXT * EXT).T, omega_relax.reshape(1))
        return (u_last + omega_relax * z_last.astype(F32)).reshape(SUB, SUB, rhs_count)

    return jax.shard_map(device_fn, mesh=mesh,
                         in_specs=(grid_spec, grid_spec, P('row', 'col'), P('row', 'col', None, None), P()),
                         out_specs=grid_spec, check_vma=False)
```

```python
import functools
import jax
import jax.numpy as jnp
from jax import lax
from jax.experimental import pallas as pl
from jax.experimental.pallas import tpu as pltpu
from jax.sharding import PartitionSpec as P

SWEEPS = 6
SUB = 32
MARGIN = 4
EXT = SUB + 2 * MARGIN
CELLS = SUB * SUB
LANES = 128
TILES = 2
GROUP = TILES * LANES
STEPS = MARGIN + 1
HALF_COLS = 2 * STEPS * 16
COLS_AT = CELLS
ROWS_AT = CELLS + 384
CORN_AT = ROWS_AT + 128
DEPTH = CORN_AT + 256
PAD = SUB
MESH = pl.DeviceIdType.MESH
F32 = jnp.float32
BF16 = jnp.bfloat16


def own_source(n):
    return ((n >> 5) + MARGIN) * EXT + (n & 31) + MARGIN


def mod(t, n):
    return t % n if isinstance(t, int) else lax.rem(t, n)


def column_source(m):
    side = m >= STEPS * 16
    k = jnp.where(side, m - STEPS * 16, m)
    return k & 15, jnp.where(side, MARGIN + SUB - 1 + (k >> 4), MARGIN - (k >> 4))


def kernel(groups, col_count,
           f_hbm, u_hbm, kap_ref, mat_hbm, om_ref, u_out, z_out,
           mat_v, mat_t, mat_p, wide, acc, res, zf, u_v, e_v, z_v, kb, cd, cn, cs, cw, ce, cedge, cedge_om, crow,
           send_p, send_b, send_u, recv_p, recv_b, recv_u, zrow_s, zrow, kcol_s, kcol_r, krow_r,
           via_p, via_b, via_u,
           in_sem, mat_sem, out_sem, s_sem, r_sem,
           sz_sem, rz_sem, sf_sem, rf_sem, sk_sem, rk_sem, vs_sem, vr_sem):
    col = lax.axis_index('col')
    row = lax.axis_index('row')
    has = (col > 0, col < col_count - 1)
    side_dev = ((col - 1, row), (col + 1, row))
    partner = (col, 1 - row)
    brow = (SUB - 1) * (1 - row)
    om = om_ref[0]

    routed = row == 1
    detour = (jnp.logical_and(routed, col == 2), jnp.logical_and(routed, col == 1))
    is_via = jnp.logical_and(routed, jnp.logical_or(col == 0, col == 3))
    mate = (lax.rem(col + 2, 4), row)
    via_to = (jnp.where(col == 0, 1, 2), row)
    via_side = jnp.where(col == 0, 1, 0)

    loads = []
    for g in range(groups):
        for t in range(TILES):
            k = g * TILES + t
            lanes = pl.ds(k * LANES, LANES)
            loads.append((
                pltpu.make_async_copy(u_hbm.at[:, lanes], zf.at[k, pl.ds(PAD, CELLS)], in_sem.at[0, k]),
                pltpu.make_async_copy(f_hbm.at[:, lanes], res.at[k], in_sem.at[1, k]),
                pltpu.make_async_copy(u_hbm.at[:, lanes], u_v.at[k], in_sem.at[2, k])))
    for a, b, c in loads:
        a.start()
        b.start()
    mat_copy = pltpu.make_async_copy(mat_hbm, mat_v, mat_sem)
    mat_copy.start()
    for a, b, c in loads:
        c.start()

    barrier = pltpu.get_barrier_semaphore()
    pl.semaphore_signal(barrier, inc=1, device_id=partner, device_id_type=MESH)
    for s in range(2):
        @pl.when(has[s])
        def _():
            pl.semaphore_signal(barrier, inc=1, device_id=side_dev[s], device_id_type=MESH)
    @pl.when(routed)
    def _():
        pl.semaphore_signal(barrier, inc=1, device_id=mate, device_id_type=MESH)
    waits = 1 + has[0].astype(jnp.int32) + has[1].astype(jnp.int32) + routed.astype(jnp.int32)
    pl.semaphore_wait(barrier, waits)

    zero_row = jnp.zeros((SUB, LANES), F32)
    kap_t = jnp.transpose(jnp.concatenate([kap_ref[...], jnp.zeros((LANES - SUB, SUB), F32)], axis=0))
    kb[pl.ds(0, SUB)] = zero_row
    kb[pl.ds(PAD + CELLS, SUB)] = zero_row
    for r in range(SUB):
        kb[pl.ds(PAD + r * SUB, SUB)] = jnp.broadcast_to(kap_t[:, r:r + 1], (SUB, LANES))

    def kcol_copy(s):
        return pltpu.make_async_remote_copy(kcol_s.at[s], kcol_r.at[1 - s], sk_sem.at[s], rk_sem.at[1 - s],
                                            device_id=side_dev[s], device_id_type=MESH)

    def krow_copy():
        return pltpu.make_async_remote_copy(kb.at[pl.ds(PAD + brow * SUB, SUB)], krow_r, sk_sem.at[2], rk_sem.at[2],
                                            device_id=partner, device_id_type=MESH)

    edge_col = (0, SUB - 1)

    def edge_cells(c, at=0):
        return pl.ds(at + c, SUB, stride=SUB)

    for s in range(2):
        kcol_s[s] = kb[edge_cells(edge_col[s], PAD), :]

        @pl.when(has[s])
        def _():
            kcol_copy(s).start()
    krow_copy().start()

    sub_id = lax.broadcasted_iota(jnp.int32, (SUB, LANES), 0)
    no_w = jnp.where(has[0], 0.0, 1.0)
    no_e = jnp.where(has[1], 0.0, 1.0)

    def coeff_row(q, carry):
        base = pl.multiple_of(q * SUB, SUB)
        here = kb[pl.ds(PAD + base, SUB)]
        up = kb[pl.ds(base, SUB)]
        down = kb[pl.ds(2 * PAD + base, SUB)]
        left = jnp.concatenate([here[:1], here[:-1]], axis=0)
        right = jnp.concatenate([here[1:], here[-1:]], axis=0)
        vn = jnp.where(q == 0, 0.0, 1.0) * (0.5 * (here + up))
        vs = jnp.where(q == SUB - 1, 0.0, 1.0) * (0.5 * (here + down))
        vw = jnp.where(sub_id == 0, 0.0, 0.5 * (here + left))
        ve = jnp.where(sub_id == SUB - 1, 0.0, 0.5 * (here + right))
        rim = jnp.where(jnp.logical_or(jnp.logical_and(q == 0, row == 0),
                                       jnp.logical_and(q == SUB - 1, row == 1)), 1.0, 0.0)
        rim_col = jnp.where(sub_id == 0, no_w, 0.0) + jnp.where(sub_id == SUB - 1, no_e, 0.0)
        rows = pl.ds(base, SUB)
        cn[rows] = vn
        cs[rows] = vs
        cw[rows] = vw
        ce[rows] = ve
        cd[rows] = vn + vs + vw + ve + (rim + rim_col) * here
        return carry

    lax.fori_loop(0, SUB, coeff_row, 0)

    def stencil(g, first, count, unroll):
        def one_row(q, carry):
            for at, n in zip(first, count):
                base = pl.multiple_of(q * SUB + at, 8)
                rows = pl.ds(base, n)
                vd, vn, vs, vw, ve = cd[rows], cn[rows], cs[rows], cw[rows], ce[rows]
                for t in range(TILES):
                    k = g * TILES + t
                    part = (vd * zf[k, pl.ds(PAD + base, n)]
                            - vn * zf[k, pl.ds(base, n)]
                            - vs * zf[k, pl.ds(2 * PAD + base, n)]
                            - vw * zf[k, pl.ds(PAD - 1 + base, n)]
                            - ve * zf[k, pl.ds(PAD + 1 + base, n)])
                    res[k, rows] = res[k, rows] - part
            return carry

        lax.fori_loop(0, SUB, one_row, 0, unroll=unroll)

    def stencil_sides(g):
        stencil(g, (0, SUB - 8), (8, 8), 4)

    def stencil_middle(g):
        stencil(g, (8,), (16,), 4)

    def zrow_copy(g):
        return pltpu.make_async_remote_copy(
            zrow_s.at[g], zrow.at[g], sz_sem.at[g], rz_sem.at[g], device_id=partner, device_id_type=MESH)

    brows = pl.ds(pl.multiple_of(brow * SUB, SUB), SUB)

    def row_fix(g):
        for t in range(TILES):
            k = g * TILES + t
            res[k, brows] = res[k, brows] - crow[...] * (zrow_s[g, t] - zrow[g, t])

    def near(s, dist):
        return dist if s == 0 else SUB - 1 - dist

    far = row
    closer = 1 - row

    def part(g, i):
        half = (closer, far)[(i - 1) // 2 % 2]
        if i in (1, 3):
            return 1, pl.ds(pl.multiple_of(16 * half, 16), 16)
        if i in (2, 4):
            return 0, pl.ds(pl.multiple_of(SUB + 48 * half, 16), 48)
        return (0 if i == 0 else 2), pl.ds(0, SUB)

    def message(g, s, t, i):
        kind, rows = part(g, i)
        slot = mod(t, 2)
        src = (send_b, send_p, send_u)[kind].at[g, s, rows]
        dst = (recv_b, recv_p, recv_u)[kind].at[slot, g, 1 - s, rows]
        return pltpu.make_async_remote_copy(src, dst, s_sem.at[g, s, i], r_sem.at[slot, g, 1 - s, i],
                                            device_id=side_dev[s], device_id_type=MESH)

    def message_out(g, s, t, i):
        kind, rows = part(g, i)
        slot = mod(t, 3)
        src = (send_b, send_p, send_u)[kind].at[g, s, rows]
        dst = (via_b, via_p, via_u)[kind].at[slot, g, rows]
        return pltpu.make_async_remote_copy(src, dst, s_sem.at[g, s, i], vr_sem.at[slot, g, i],
                                            device_id=mate, device_id_type=MESH)

    def message_on(g, t, i):
        kind, rows = part(g, i)
        slot = mod(t, 2)
        src = (via_b, via_p, via_u)[kind].at[mod(t, 3), g, rows]
        dst = (recv_b, recv_p, recv_u)[kind].at[slot, g, via_side, rows]
        return pltpu.make_async_remote_copy(src, dst, vs_sem.at[g, i], r_sem.at[slot, g, via_side, i],
                                            device_id=via_to, device_id_type=MESH)

    SWEEP_PARTS = (0, 1, 2, 3, 4)
    FIRST_PARTS = (5, 1, 2, 3, 4)

    def pass_on(g, t, parts):
        @pl.when(is_via)
        def _():
            for i in parts:
                message_out(g, 0, t, i).wait_recv()
                message_on(g, t, i).start()

    def fill_z(g, first):
        for s in range(2):
            for t in range(TILES):
                lanes = pl.ds(t * LANES, LANES)
                zedge = zf[g * TILES + t, edge_cells(near(s, 0), PAD), :]
                if first:
                    send_u[g, s, :, lanes] = zedge
                else:
                    send_b[g, s, pl.ds(0, SUB), lanes] = zedge.astype(BF16)

    def fill_half(g, h):
        at = pl.multiple_of(CELLS // 2 * h, CELLS // 2)
        p_at = pl.multiple_of(16 * h, 16)
        e_at = pl.multiple_of(SUB + 48 * h, 16)
        for s in range(2):
            for t in range(TILES):
                k = g * TILES + t
                lanes = pl.ds(t * LANES, LANES)
                for d in range(MARGIN):
                    part = res[k, pl.ds(at + near(s, d), 16, stride=SUB), :]
                    if d == 0:
                        send_p[g, s, pl.ds(p_at, 16), lanes] = part
                    else:
                        send_b[g, s, pl.ds(e_at + 16 * (d - 1), 16), lanes] = part.astype(BF16)

    def start(g, t, which):
        for s in range(2):
            @pl.when(jnp.logical_and(has[s], jnp.logical_not(detour[s])))
            def _():
                for i in which:
                    message(g, s, t, i).start()

            @pl.when(detour[s])
            def _():
                for i in which:
                    message_out(g, s, t, i).start()

    def fwd_rows(g):
        rows = pl.multiple_of((SUB - MARGIN) * SUB * (1 - row), 128)
        return pltpu.make_async_remote_copy(e_v.at[g, pl.ds(rows, 128)], e_v.at[g, pl.ds(ROWS_AT, 128)],
                                            sf_sem.at[g, 0], rf_sem.at[g, 0], device_id=partner, device_id_type=MESH)

    def fwd_corners(g):
        rows = pl.multiple_of(COLS_AT + HALF_COLS * closer, 32)
        return pltpu.make_async_remote_copy(e_v.at[g, pl.ds(rows, HALF_COLS)], e_v.at[g, pl.ds(CORN_AT, HALF_COLS)],
                                            sf_sem.at[g, 1], rf_sem.at[g, 1], device_id=partner, device_id_type=MESH)

    def assemble(g, sent, first):
        slot = mod(sent, 2)
        for half, parts in ((closer, ((5 if first else 0), 1, 2)), (far, (3, 4))):
            for s in range(2):
                @pl.when(has[s])
                def _():
                    for i in parts:
                        message(g, 1 - s, sent, i).wait_recv()
                    rows = pl.ds(pl.multiple_of(16 * half, 16), 16)
                    e_rows = pl.ds(pl.multiple_of(SUB + 48 * half, 16), 48)
                    at = pl.multiple_of(CELLS // 2 * half, CELLS // 2)
                    e_at = pl.multiple_of(COLS_AT + STEPS * 16 * s + HALF_COLS * half, 16)
                    cells = pl.ds(at + edge_col[s], 16, stride=SUB)
                    zcells = pl.ds(PAD + at + edge_col[s], 16, stride=SUB)
                    coeff = (cedge if first else cedge_om)[s, rows]
                    for t in range(TILES):
                        k = g * TILES + t
                        lanes = pl.ds(t * LANES, LANES)
                        if first:
                            theirs = recv_u[slot, g, s, rows, lanes]
                        else:
                            theirs = recv_b[slot, g, s, rows, lanes].astype(F32)
                        flux = coeff * (zf[k, zcells, :] - theirs)
                        own = res[k, cells, :] - flux
                        res[k, cells, :] = own
                        e_v[g, pl.ds(e_at, 16), lanes] = own.astype(BF16)
                        e_v[g, pl.ds(e_at + 16, 16), lanes] = (recv_p[slot, g, s, rows, lanes] + flux).astype(BF16)
                        e_v[g, pl.ds(e_at + 32, 48), lanes] = recv_b[slot, g, s, e_rows, lanes]
            if half is closer:
                fwd_corners(g).start()

    def pack(g):
        def one_row(q, carry):
            rows = pl.ds(pl.multiple_of(q * SUB, SUB), SUB)
            for t in range(TILES):
                e_v[g, rows, pl.ds(t * LANES, LANES)] = (keep * res[g * TILES + t, rows]).astype(BF16)
            return carry

        lax.fori_loop(0, SUB, one_row, 0, unroll=4)
        fwd_rows(g).start()

    def solve_own(g):
        acc[g] = jnp.dot(mat_p[:, :COLS_AT], e_v[g, pl.ds(0, COLS_AT)], preferred_element_type=F32)

    def solve_rest(g):
        fwd_rows(g).wait()
        fwd_corners(g).wait()
        acc[g] += jnp.dot(mat_p[:, COLS_AT:], e_v[g, pl.ds(COLS_AT, DEPTH - COLS_AT)], preferred_element_type=F32)

    def round_row(g):
        for t in range(TILES):
            zrow_s[g, t] = acc[g, brows, pl.ds(t * LANES, LANES)].astype(BF16).astype(F32)

    def update(g):
        def rows_of(q, carry):
            rows = pl.ds(pl.multiple_of(q * 64, 64), 64)
            for t in range(TILES):
                k = g * TILES + t
                z = acc[g, rows, pl.ds(t * LANES, LANES)].astype(BF16).astype(F32)
                zf[k, pl.ds(pl.multiple_of(PAD + q * 64, PAD), 64)] = z
                u_v[k, rows] = u_v[k, rows] + om * z
            return carry

        lax.fori_loop(0, CELLS // 64, rows_of, 0)

    for k in range(groups * TILES):
        zf[k, pl.ds(0, PAD)] = zero_row
        zf[k, pl.ds(PAD + CELLS, PAD)] = zero_row
    for g in range(groups):
        e_v[g, pl.ds(COLS_AT, ROWS_AT - COLS_AT)] = jnp.zeros((ROWS_AT - COLS_AT, GROUP), BF16)
        e_v[g, pl.ds(CORN_AT, DEPTH - CORN_AT)] = jnp.zeros((DEPTH - CORN_AT, GROUP), BF16)
    keep = (1.0 - jnp.where(jnp.logical_and(sub_id == 0, has[0]), 1.0, 0.0)
            - jnp.where(jnp.logical_and(sub_id == SUB - 1, has[1]), 1.0, 0.0))

    krow_copy().wait()
    rows_b = pl.ds(pl.multiple_of(PAD + brow * SUB, SUB), SUB)
    crow[...] = 0.5 * (kb[rows_b] + krow_r[...])

    def send_bands(g, t):
        stencil_sides(g)
        zrow_copy(g).wait()
        row_fix(g)
        fill_half(g, closer)
        start(g, t, (1, 2))
        fill_half(g, far)
        start(g, t, (3, 4))
        stencil_middle(g)
        pack(g)

    for g in range(groups):
        for t in range(TILES):
            loads[g * TILES + t][0].wait()
        for t in range(TILES):
            zrow_s[g, t] = zf[g * TILES + t, rows_b]
        zrow_copy(g).start()
        fill_z(g, True)
        start(g, 0, (5,))
        for t in range(TILES):
            loads[g * TILES + t][1].wait()
        send_bands(g, 0)

    mat_copy.wait()
    for at in range(0, EXT * EXT, 256):
        span = pl.ds(at, min(256, EXT * EXT - at))
        mat_t[:, span] = mat_v[span].T
    pass_on(0, 0, FIRST_PARTS)

    def place(at, width, start, window, source, ok=None):
        n = lax.broadcasted_iota(jnp.int32, (window, width), 1)
        k = lax.broadcasted_iota(jnp.int32, (window, width), 0) + start
        pick = source(n) == k
        if ok is not None:
            pick = jnp.logical_and(pick, ok(n))
        pick = jnp.where(pick, 1.0, 0.0).astype(BF16)

        wide[:, pl.ds(0, width)] = jnp.dot(mat_t[:, pl.ds(start, window)], pick, preferred_element_type=F32)
        mat_p[:, pl.ds(at, width)] = wide[:, pl.ds(0, width)].astype(BF16)

    for q in range(4):
        low = (320 * q + 164) // 128 * 128
        high = -(-(320 * q + 476) // 128) * 128
        place(256 * q, 256, low, high - low, lambda n, q=q: own_source(n + 256 * q))

    for g in range(groups):
        solve_own(g)

    def column(n):
        half = n >= HALF_COLS
        r, c = column_source(jnp.where(half, n - HALF_COLS, n))
        return (MARGIN + r + jnp.where(half, 16, 0)) * EXT + c

    pass_on(1, 0, FIRST_PARTS)
    place(COLS_AT, 384, 128, 1408, column, lambda n: n < 2 * HALF_COLS)

    def halo(n):
        first_row = jnp.where(row == 0, MARGIN + SUB, 0)
        r, c = column_source(n - 128)
        corner_row = jnp.where(row == 0, MARGIN + SUB, -12) + r
        return jnp.where(n < 128, (first_row + (n >> 5)) * EXT + MARGIN + (n & 31), corner_row * EXT + c)

    def halo_ok(n):
        r = n & 15
        corner = jnp.logical_and(n < 128 + HALF_COLS, jnp.where(row == 0, r, 15 - r) < MARGIN)
        return jnp.logical_or(n < 128, corner)

    place(ROWS_AT, 384, pl.multiple_of(1408 * (1 - row), 128), 192, halo, halo_ok)

    for s in range(2):
        @pl.when(has[s])
        def _():
            kcol_copy(1 - s).wait_recv()
            cedge[s] = 0.5 * (kcol_s[s] + kcol_r[s])
            cedge_om[s] = om * cedge[s]
            kcol_copy(s).wait_send()
    crow[...] = om * crow[...]

    def scale(q, carry):
        rows = pl.ds(pl.multiple_of(q * SUB, SUB), SUB)
        for c in (cd, cn, cs, cw, ce):
            c[rows] = om * c[rows]
        return carry

    lax.fori_loop(0, SUB, scale, 0)
    for k in range(groups * TILES):
        loads[k][2].wait()

    def wait_sends(g, which):
        for s in range(2):
            @pl.when(has[s])
            def _():
                for i in which:
                    message(g, s, 0, i).wait_send()

        @pl.when(is_via)
        def _():
            for i in which:
                message_on(g, 0, i).wait_send()

    def advance(g, t, first, relay):
        solve_rest(g)
        round_row(g)
        zrow_copy(g).start()
        update(g)
        wait_sends(g, FIRST_PARTS if first else SWEEP_PARTS)
        fill_z(g, False)
        start(g, t, (0,))
        if relay is not None:
            pass_on(*relay)
        send_bands(g, t)
        solve_own(g)

    assemble(0, 0, True)
    advance(0, 1, True, None)
    assemble(1, 0, True)
    advance(1, 1, True, (0, 1, SWEEP_PARTS))

    def step(i, carry):
        t = i // groups
        g = lax.rem(i, groups)
        assemble(g, t - 1, False)
        advance(g, t, False, (1 - g, jnp.where(g == 0, t - 1, t), SWEEP_PARTS))
        return carry

    lax.fori_loop(2 * groups, SWEEPS * groups, step, 0)

    u_copies = [pltpu.make_async_copy(u_v.at[k], u_out.at[:, pl.ds(k * LANES, LANES)], in_sem.at[0, k])
                for k in range(groups * TILES)]
    z_copies = [pltpu.make_async_copy(z_v.at[g], z_out.at[:, pl.ds(g * GROUP, GROUP)], out_sem.at[g])
                for g in range(groups)]
    for g in range(groups):
        for t in range(TILES):
            u_copies[g * TILES + t].start()
    for g in range(groups):
        assemble(g, SWEEPS - 1, False)
        solve_rest(g)
        z_v[g] = acc[g].astype(BF16)
        z_copies[g].start()
        if g == 0:
            pass_on(1, SWEEPS - 1, SWEEP_PARTS)
    for g in range(groups):
        wait_sends(g, SWEEP_PARTS)
    for c in u_copies + z_copies:
        c.wait()


def solution(mesh):
    col_count = mesh.shape['col']
    grid_spec = P('row', 'col', None)

    def device_fn(f_blk, u_blk, kappa_blk, mat_blk, omega_relax):
        rhs_count = u_blk.shape[2]
        groups = rhs_count // GROUP
        tiles = rhs_count // LANES
        vm = pltpu.VMEM
        dma = pltpu.SemaphoreType.DMA
        coeff = vm((CELLS, LANES), F32)
        u_last, z_last = pl.pallas_call(
            functools.partial(kernel, groups, col_count),
            out_shape=(jax.ShapeDtypeStruct((CELLS, rhs_count), F32), jax.ShapeDtypeStruct((CELLS, rhs_count), BF16)),
            in_specs=[pl.BlockSpec(memory_space=pltpu.HBM), pl.BlockSpec(memory_space=pltpu.HBM),
                      pl.BlockSpec(memory_space=pltpu.VMEM), pl.BlockSpec(memory_space=pltpu.HBM),
                      pl.BlockSpec(memory_space=pltpu.SMEM)],
            out_specs=(pl.BlockSpec(memory_space=pl.ANY), pl.BlockSpec(memory_space=pl.ANY)),
            scratch_shapes=[
                vm((EXT * EXT, CELLS), BF16),
                vm((CELLS, EXT * EXT), BF16),
                vm((CELLS, DEPTH), BF16),
                vm((CELLS, 384), F32),
                vm((groups, CELLS, GROUP), F32),
                vm((tiles, CELLS, LANES), F32),
                vm((tiles, CELLS + 2 * PAD, LANES), F32),
                vm((tiles, CELLS, LANES), F32),
                vm((groups, DEPTH, GROUP), BF16),
                vm((groups, CELLS, GROUP), BF16),
                vm((CELLS + 2 * PAD, LANES), F32),
                coeff, coeff, coeff, coeff, coeff,
                vm((2, SUB, LANES), F32),
                vm((2, SUB, LANES), F32),
                vm((SUB, LANES), F32),
                vm((groups, 2, SUB, GROUP), F32),
                vm((groups, 2, 128, GROUP), BF16),
                vm((groups, 2, SUB, GROUP), F32),
                vm((2, groups, 2, SUB, GROUP), F32),
                vm((2, groups, 2, 128, GROUP), BF16),
                vm((1, groups, 2, SUB, GROUP), F32),
                vm((groups, TILES, SUB, LANES), F32),
                vm((groups, TILES, SUB, LANES), F32),
                vm((2, SUB, LANES), F32),
                vm((2, SUB, LANES), F32),
                vm((SUB, LANES), F32),
                vm((3, groups, SUB, GROUP), F32),
                vm((3, groups, 128, GROUP), BF16),
                vm((1, groups, SUB, GROUP), F32),
                dma((3, tiles)), dma, dma((groups,)),
                dma((groups, 2, 6)), dma((2, groups, 2, 6)),
                dma((groups,)), dma((groups,)),
                dma((groups, 2)), dma((groups, 2)),
                dma((3,)), dma((3,)),
                dma((groups, 6)), dma((3, groups, 6)),
            ],
            compiler_params=pltpu.CompilerParams(collective_id=0, has_side_effects=True,
                                                 vmem_limit_bytes=50 * 1024 * 1024),
        )(f_blk.reshape(CELLS, rhs_count), u_blk.reshape(CELLS, rhs_count), kappa_blk,
          mat_blk.reshape(CELLS, EXT * EXT).T, omega_relax.reshape(1))
        return (u_last + omega_relax * z_last.astype(F32)).reshape(SUB, SUB, rhs_count)

    return jax.shard_map(device_fn, mesh=mesh,
                         in_specs=(grid_spec, grid_spec, P('row', 'col'), P('row', 'col', None, None), P()),
                         out_specs=grid_spec, check_vma=False)
```

```python
import functools
import jax
import jax.numpy as jnp
from jax import lax
from jax.experimental import pallas as pl
from jax.experimental.pallas import tpu as pltpu
from jax.sharding import PartitionSpec as P

SWEEPS = 6
SUB = 32
MARGIN = 4
EXT = SUB + 2 * MARGIN
CELLS = SUB * SUB
LANES = 128
TILES = 2
GROUP = TILES * LANES
STEPS = MARGIN + 1
HALF_COLS = 2 * STEPS * 16
COLS_AT = CELLS
ROWS_AT = CELLS + 384
CORN_AT = ROWS_AT + 128
DEPTH = CORN_AT + 256
PAD = SUB
MESH = pl.DeviceIdType.MESH
F32 = jnp.float32
BF16 = jnp.bfloat16


def own_source(n):
    return ((n >> 5) + MARGIN) * EXT + (n & 31) + MARGIN


def mod(t, n):
    return t % n if isinstance(t, int) else lax.rem(t, n)


def column_source(m):
    side = m >= STEPS * 16
    k = jnp.where(side, m - STEPS * 16, m)
    return k & 15, jnp.where(side, MARGIN + SUB - 1 + (k >> 4), MARGIN - (k >> 4))


def kernel(groups, col_count,
           f_hbm, u_hbm, kap_ref, mat_hbm, om_ref, u_out, z_out,
           mat_v, mat_t, mat_p, wide, acc, res, zf, u_v, e_v, z_v, kb, cd, cn, cs, cw, ce, cedge, cedge_om, crow,
           send_p, send_b, send_u, recv_p, recv_b, recv_u, zrow_s, zrow, kcol_s, kcol_r, krow_r,
           via_p, via_b, via_u,
           in_sem, mat_sem, out_sem, s_sem, r_sem,
           sz_sem, rz_sem, sf_sem, rf_sem, sk_sem, rk_sem, vs_sem, vr_sem):
    col = lax.axis_index('col')
    row = lax.axis_index('row')
    has = (col > 0, col < col_count - 1)
    side_dev = ((col - 1, row), (col + 1, row))
    partner = (col, 1 - row)
    brow = (SUB - 1) * (1 - row)
    om = om_ref[0]

    routed = row == 1
    detour = (jnp.logical_and(routed, col == 2), jnp.logical_and(routed, col == 1))
    is_via = jnp.logical_and(routed, jnp.logical_or(col == 0, col == 3))
    mate = (lax.rem(col + 2, 4), row)
    via_to = (jnp.where(col == 0, 1, 2), row)
    via_side = jnp.where(col == 0, 1, 0)

    loads = []
    for g in range(groups):
        for t in range(TILES):
            k = g * TILES + t
            lanes = pl.ds(k * LANES, LANES)
            loads.append((
                pltpu.make_async_copy(u_hbm.at[:, lanes], zf.at[k, pl.ds(PAD, CELLS)], in_sem.at[0, k]),
                pltpu.make_async_copy(f_hbm.at[:, lanes], res.at[k], in_sem.at[1, k]),
                pltpu.make_async_copy(u_hbm.at[:, lanes], u_v.at[k], in_sem.at[2, k])))
    for a, b, c in loads:
        a.start()
        b.start()
    mat_copy = pltpu.make_async_copy(mat_hbm, mat_v, mat_sem)
    mat_copy.start()
    for a, b, c in loads:
        c.start()

    barrier = pltpu.get_barrier_semaphore()
    pl.semaphore_signal(barrier, inc=1, device_id=partner, device_id_type=MESH)
    for s in range(2):
        @pl.when(has[s])
        def _():
            pl.semaphore_signal(barrier, inc=1, device_id=side_dev[s], device_id_type=MESH)
    @pl.when(routed)
    def _():
        pl.semaphore_signal(barrier, inc=1, device_id=mate, device_id_type=MESH)
    waits = 1 + has[0].astype(jnp.int32) + has[1].astype(jnp.int32) + routed.astype(jnp.int32)
    pl.semaphore_wait(barrier, waits)

    zero_row = jnp.zeros((SUB, LANES), F32)
    kap_t = jnp.transpose(jnp.concatenate([kap_ref[...], jnp.zeros((LANES - SUB, SUB), F32)], axis=0))
    kb[pl.ds(0, SUB)] = zero_row
    kb[pl.ds(PAD + CELLS, SUB)] = zero_row
    for r in range(SUB):
        kb[pl.ds(PAD + r * SUB, SUB)] = jnp.broadcast_to(kap_t[:, r:r + 1], (SUB, LANES))

    def kcol_copy(s):
        return pltpu.make_async_remote_copy(kcol_s.at[s], kcol_r.at[1 - s], sk_sem.at[s], rk_sem.at[1 - s],
                                            device_id=side_dev[s], device_id_type=MESH)

    def krow_copy():
        return pltpu.make_async_remote_copy(kb.at[pl.ds(PAD + brow * SUB, SUB)], krow_r, sk_sem.at[2], rk_sem.at[2],
                                            device_id=partner, device_id_type=MESH)

    edge_col = (0, SUB - 1)

    def edge_cells(c, at=0):
        return pl.ds(at + c, SUB, stride=SUB)

    for s in range(2):
        kcol_s[s] = kb[edge_cells(edge_col[s], PAD), :]

        @pl.when(has[s])
        def _():
            kcol_copy(s).start()
    krow_copy().start()

    sub_id = lax.broadcasted_iota(jnp.int32, (SUB, LANES), 0)
    no_w = jnp.where(has[0], 0.0, 1.0)
    no_e = jnp.where(has[1], 0.0, 1.0)

    def coeff_row(q, carry):
        base = pl.multiple_of(q * SUB, SUB)
        here = kb[pl.ds(PAD + base, SUB)]
        up = kb[pl.ds(base, SUB)]
        down = kb[pl.ds(2 * PAD + base, SUB)]
        left = jnp.concatenate([here[:1], here[:-1]], axis=0)
        right = jnp.concatenate([here[1:], here[-1:]], axis=0)
        vn = jnp.where(q == 0, 0.0, 1.0) * (0.5 * (here + up))
        vs = jnp.where(q == SUB - 1, 0.0, 1.0) * (0.5 * (here + down))
        vw = jnp.where(sub_id == 0, 0.0, 0.5 * (here + left))
        ve = jnp.where(sub_id == SUB - 1, 0.0, 0.5 * (here + right))
        rim = jnp.where(jnp.logical_or(jnp.logical_and(q == 0, row == 0),
                                       jnp.logical_and(q == SUB - 1, row == 1)), 1.0, 0.0)
        rim_col = jnp.where(sub_id == 0, no_w, 0.0) + jnp.where(sub_id == SUB - 1, no_e, 0.0)
        rows = pl.ds(base, SUB)
        cn[rows] = vn
        cs[rows] = vs
        cw[rows] = vw
        ce[rows] = ve
        cd[rows] = vn + vs + vw + ve + (rim + rim_col) * here
        return carry

    lax.fori_loop(0, SUB, coeff_row, 0)

    def stencil(g, first, count, unroll):
        def one_row(q, carry):
            for at, n in zip(first, count):
                base = pl.multiple_of(q * SUB + at, 8)
                rows = pl.ds(base, n)
                vd, vn, vs, vw, ve = cd[rows], cn[rows], cs[rows], cw[rows], ce[rows]
                for t in range(TILES):
                    k = g * TILES + t
                    part = (vd * zf[k, pl.ds(PAD + base, n)]
                            - vn * zf[k, pl.ds(base, n)]
                            - vs * zf[k, pl.ds(2 * PAD + base, n)]
                            - vw * zf[k, pl.ds(PAD - 1 + base, n)]
                            - ve * zf[k, pl.ds(PAD + 1 + base, n)])
                    res[k, rows] = res[k, rows] - part
            return carry

        lax.fori_loop(0, SUB, one_row, 0, unroll=unroll)

    def stencil_sides(g):
        stencil(g, (0, SUB - 8), (8, 8), 8)

    def stencil_middle(g):
        stencil(g, (8,), (16,), 8)

    def zrow_copy(g):
        return pltpu.make_async_remote_copy(
            zrow_s.at[g], zrow.at[g], sz_sem.at[g], rz_sem.at[g], device_id=partner, device_id_type=MESH)

    brows = pl.ds(pl.multiple_of(brow * SUB, SUB), SUB)

    def row_fix(g):
        for t in range(TILES):
            k = g * TILES + t
            res[k, brows] = res[k, brows] - crow[...] * (zrow_s[g, t] - zrow[g, t])

    def near(s, dist):
        return dist if s == 0 else SUB - 1 - dist

    far = row
    closer = 1 - row

    def part(g, i):
        half = (closer, far)[(i - 1) // 2 % 2]
        if i in (1, 3):
            return 1, pl.ds(pl.multiple_of(16 * half, 16), 16)
        if i in (2, 4):
            return 0, pl.ds(pl.multiple_of(SUB + 48 * half, 16), 48)
        return (0 if i == 0 else 2), pl.ds(0, SUB)

    def message(g, s, t, i):
        kind, rows = part(g, i)
        slot = mod(t, 2)
        src = (send_b, send_p, send_u)[kind].at[g, s, rows]
        dst = (recv_b, recv_p, recv_u)[kind].at[slot, g, 1 - s, rows]
        return pltpu.make_async_remote_copy(src, dst, s_sem.at[g, s, i], r_sem.at[slot, g, 1 - s, i],
                                            device_id=side_dev[s], device_id_type=MESH)

    def message_out(g, s, t, i):
        kind, rows = part(g, i)
        slot = mod(t, 3)
        src = (send_b, send_p, send_u)[kind].at[g, s, rows]
        dst = (via_b, via_p, via_u)[kind].at[slot, g, rows]
        return pltpu.make_async_remote_copy(src, dst, s_sem.at[g, s, i], vr_sem.at[slot, g, i],
                                            device_id=mate, device_id_type=MESH)

    def message_on(g, t, i):
        kind, rows = part(g, i)
        slot = mod(t, 2)
        src = (via_b, via_p, via_u)[kind].at[mod(t, 3), g, rows]
        dst = (recv_b, recv_p, recv_u)[kind].at[slot, g, via_side, rows]
        return pltpu.make_async_remote_copy(src, dst, vs_sem.at[g, i], r_sem.at[slot, g, via_side, i],
                                            device_id=via_to, device_id_type=MESH)

    SWEEP_PARTS = (0, 1, 2, 3, 4)
    FIRST_PARTS = (5, 1, 2, 3, 4)

    def pass_on(g, t, parts):
        @pl.when(is_via)
        def _():
            for i in parts:
                message_out(g, 0, t, i).wait_recv()
                message_on(g, t, i).start()

    def fill_z(g, first):
        for s in range(2):
            for t in range(TILES):
                lanes = pl.ds(t * LANES, LANES)
                zedge = zf[g * TILES + t, edge_cells(near(s, 0), PAD), :]
                if first:
                    send_u[g, s, :, lanes] = zedge
                else:
                    send_b[g, s, pl.ds(0, SUB), lanes] = zedge.astype(BF16)

    def fill_half(g, h):
        at = pl.multiple_of(CELLS // 2 * h, CELLS // 2)
        p_at = pl.multiple_of(16 * h, 16)
        e_at = pl.multiple_of(SUB + 48 * h, 16)
        for s in range(2):
            for t in range(TILES):
                k = g * TILES + t
                lanes = pl.ds(t * LANES, LANES)
                for d in range(MARGIN):
                    part = res[k, pl.ds(at + near(s, d), 16, stride=SUB), :]
                    if d == 0:
                        send_p[g, s, pl.ds(p_at, 16), lanes] = part
                    else:
                        send_b[g, s, pl.ds(e_at + 16 * (d - 1), 16), lanes] = part.astype(BF16)

    def start(g, t, which):
        for s, turn in ((1, col < 2), (0, has[0]), (1, jnp.logical_and(col >= 2, has[1]))):
            @pl.when(jnp.logical_and(turn, jnp.logical_not(detour[s])))
            def _():
                for i in which:
                    message(g, s, t, i).start()

            @pl.when(jnp.logical_and(turn, detour[s]))
            def _():
                for i in which:
                    message_out(g, s, t, i).start()

    def fwd_rows(g):
        rows = pl.multiple_of((SUB - MARGIN) * SUB * (1 - row), 128)
        return pltpu.make_async_remote_copy(e_v.at[g, pl.ds(rows, 128)], e_v.at[g, pl.ds(ROWS_AT, 128)],
                                            sf_sem.at[g, 0], rf_sem.at[g, 0], device_id=partner, device_id_type=MESH)

    def fwd_corners(g):
        rows = pl.multiple_of(COLS_AT + HALF_COLS * closer, 32)
        return pltpu.make_async_remote_copy(e_v.at[g, pl.ds(rows, HALF_COLS)], e_v.at[g, pl.ds(CORN_AT, HALF_COLS)],
                                            sf_sem.at[g, 1], rf_sem.at[g, 1], device_id=partner, device_id_type=MESH)

    def assemble(g, sent, first, half, parts):
        slot = mod(sent, 2)
        for s in range(2):
            @pl.when(has[s])
            def _():
                for i in parts:
                    message(g, 1 - s, sent, i).wait_recv()
                rows = pl.ds(pl.multiple_of(16 * half, 16), 16)
                e_rows = pl.ds(pl.multiple_of(SUB + 48 * half, 16), 48)
                at = pl.multiple_of(CELLS // 2 * half, CELLS // 2)
                e_at = pl.multiple_of(COLS_AT + STEPS * 16 * s + HALF_COLS * half, 16)
                cells = pl.ds(at + edge_col[s], 16, stride=SUB)
                zcells = pl.ds(PAD + at + edge_col[s], 16, stride=SUB)
                coeff = (cedge if first else cedge_om)[s, rows]
                for t in range(TILES):
                    k = g * TILES + t
                    lanes = pl.ds(t * LANES, LANES)
                    if first:
                        theirs = recv_u[slot, g, s, rows, lanes]
                    else:
                        theirs = recv_b[slot, g, s, rows, lanes].astype(F32)
                    flux = coeff * (zf[k, zcells, :] - theirs)
                    own = res[k, cells, :] - flux
                    res[k, cells, :] = own
                    e_v[g, pl.ds(e_at, 16), lanes] = own.astype(BF16)
                    e_v[g, pl.ds(e_at + 16, 16), lanes] = (recv_p[slot, g, s, rows, lanes] + flux).astype(BF16)
                    e_v[g, pl.ds(e_at + 32, 48), lanes] = recv_b[slot, g, s, e_rows, lanes]

    def assemble_closer(g, sent, first):
        assemble(g, sent, first, closer, ((5 if first else 0), 1, 2))
        fwd_corners(g).start()

    def assemble_far(g, sent, first):
        assemble(g, sent, first, far, (3, 4))

    def pack(g):
        def one_row(q, carry):
            rows = pl.ds(pl.multiple_of(q * SUB, SUB), SUB)
            for t in range(TILES):
                e_v[g, rows, pl.ds(t * LANES, LANES)] = (keep * res[g * TILES + t, rows]).astype(BF16)
            return carry

        lax.fori_loop(0, SUB, one_row, 0, unroll=4)
        fwd_rows(g).start()

    def solve_own(g):
        def rows_of(m, carry):
            rows = pl.ds(pl.multiple_of(m * (CELLS // 2), CELLS // 2), CELLS // 2)
            acc[g, rows] = jnp.dot(mat_p[rows, :COLS_AT], e_v[g, pl.ds(0, COLS_AT)], preferred_element_type=F32)
            return carry

        lax.fori_loop(0, 2, rows_of, 0)

    def solve_rest(g):
        fwd_rows(g).wait()
        fwd_corners(g).wait()
        acc[g] += jnp.dot(mat_p[:, COLS_AT:], e_v[g, pl.ds(COLS_AT, DEPTH - COLS_AT)], preferred_element_type=F32)

    def round_row(g):
        for t in range(TILES):
            zrow_s[g, t] = acc[g, brows, pl.ds(t * LANES, LANES)].astype(BF16).astype(F32)

    def update(g):
        def rows_of(q, carry):
            rows = pl.ds(pl.multiple_of(q * 64, 64), 64)
            for t in range(TILES):
                k = g * TILES + t
                z = acc[g, rows, pl.ds(t * LANES, LANES)].astype(BF16).astype(F32)
                zf[k, pl.ds(pl.multiple_of(PAD + q * 64, PAD), 64)] = z
            return carry

        lax.fori_loop(0, CELLS // 64, rows_of, 0)

    for k in range(groups * TILES):
        zf[k, pl.ds(0, PAD)] = zero_row
        zf[k, pl.ds(PAD + CELLS, PAD)] = zero_row
    for g in range(groups):
        e_v[g, pl.ds(COLS_AT, ROWS_AT - COLS_AT)] = jnp.zeros((ROWS_AT - COLS_AT, GROUP), BF16)
        e_v[g, pl.ds(CORN_AT, DEPTH - CORN_AT)] = jnp.zeros((DEPTH - CORN_AT, GROUP), BF16)
    keep = (1.0 - jnp.where(jnp.logical_and(sub_id == 0, has[0]), 1.0, 0.0)
            - jnp.where(jnp.logical_and(sub_id == SUB - 1, has[1]), 1.0, 0.0))

    krow_copy().wait()
    rows_b = pl.ds(pl.multiple_of(PAD + brow * SUB, SUB), SUB)
    crow[...] = 0.5 * (kb[rows_b] + krow_r[...])

    def send_bands(g, t):
        stencil_sides(g)
        zrow_copy(g).wait()
        row_fix(g)
        fill_half(g, closer)
        start(g, t, (1, 2))
        fill_half(g, far)
        start(g, t, (3, 4))

    for g in range(groups):
        for t in range(TILES):
            loads[g * TILES + t][0].wait()
        for t in range(TILES):
            zrow_s[g, t] = zf[g * TILES + t, rows_b]
        zrow_copy(g).start()
        fill_z(g, True)
        start(g, 0, (5,))
        for t in range(TILES):
            loads[g * TILES + t][1].wait()
        send_bands(g, 0)

    mat_copy.wait()
    for at in range(0, EXT * EXT, 256):
        span = pl.ds(at, min(256, EXT * EXT - at))
        mat_t[:, span] = mat_v[span].T
    pass_on(0, 0, FIRST_PARTS)

    def place(at, width, start, window, source, ok=None):
        n = lax.broadcasted_iota(jnp.int32, (window, width), 1)
        k = lax.broadcasted_iota(jnp.int32, (window, width), 0) + start
        pick = source(n) == k
        if ok is not None:
            pick = jnp.logical_and(pick, ok(n))
        pick = jnp.where(pick, 1.0, 0.0).astype(BF16)

        wide[:, pl.ds(0, width)] = jnp.dot(mat_t[:, pl.ds(start, window)], pick, preferred_element_type=F32)
        mat_p[:, pl.ds(at, width)] = wide[:, pl.ds(0, width)].astype(BF16)

    for q in range(4):
        low = (320 * q + 164) // 128 * 128
        high = -(-(320 * q + 476) // 128) * 128
        place(256 * q, 256, low, high - low, lambda n, q=q: own_source(n + 256 * q))

    for g in range(groups):
        stencil_middle(g)
        pack(g)
        solve_own(g)

    def column(n):
        half = n >= HALF_COLS
        r, c = column_source(jnp.where(half, n - HALF_COLS, n))
        return (MARGIN + r + jnp.where(half, 16, 0)) * EXT + c

    pass_on(1, 0, FIRST_PARTS)
    place(COLS_AT, 384, 128, 1408, column, lambda n: n < 2 * HALF_COLS)

    def halo(n):
        first_row = jnp.where(row == 0, MARGIN + SUB, 0)
        r, c = column_source(n - 128)
        corner_row = jnp.where(row == 0, MARGIN + SUB, -12) + r
        return jnp.where(n < 128, (first_row + (n >> 5)) * EXT + MARGIN + (n & 31), corner_row * EXT + c)

    def halo_ok(n):
        r = n & 15
        corner = jnp.logical_and(n < 128 + HALF_COLS, jnp.where(row == 0, r, 15 - r) < MARGIN)
        return jnp.logical_or(n < 128, corner)

    place(ROWS_AT, 384, pl.multiple_of(1408 * (1 - row), 128), 192, halo, halo_ok)

    for s in range(2):
        @pl.when(has[s])
        def _():
            kcol_copy(1 - s).wait_recv()
            cedge[s] = 0.5 * (kcol_s[s] + kcol_r[s])
            cedge_om[s] = om * cedge[s]
            kcol_copy(s).wait_send()
    crow[...] = om * crow[...]

    def scale(q, carry):
        rows = pl.ds(pl.multiple_of(q * SUB, SUB), SUB)
        for c in (cd, cn, cs, cw, ce):
            c[rows] = om * c[rows]
        return carry

    lax.fori_loop(0, SUB, scale, 0)
    for k in range(groups * TILES):
        loads[k][2].wait()

    def wait_sends(g, which):
        for s in range(2):
            @pl.when(has[s])
            def _():
                for i in which:
                    message(g, s, 0, i).wait_send()

        @pl.when(is_via)
        def _():
            for i in which:
                message_on(g, 0, i).wait_send()

    def finish(g):
        stencil_middle(g)
        pack(g)

        def add_to_u(q, carry):
            rows = pl.ds(pl.multiple_of(q * SUB, SUB), SUB)
            for t in range(TILES):
                k = g * TILES + t
                u_v[k, rows] = u_v[k, rows] + om * zf[k, pl.ds(pl.multiple_of(PAD + q * SUB, PAD), SUB)]
            return carry

        lax.fori_loop(0, SUB, add_to_u, 0, unroll=4)
        solve_own(g)

    def advance(g, t, first, relay):
        if relay is not None:
            pass_on(relay[0], relay[1], (0, 1, 2))
        solve_rest(g)
        round_row(g)
        zrow_copy(g).start()
        update(g)
        wait_sends(g, FIRST_PARTS if first else SWEEP_PARTS)
        fill_z(g, False)
        start(g, t, (0,))
        if relay is not None:
            pass_on(relay[0], relay[1], (3, 4))
        send_bands(g, t)

    assemble_closer(0, 0, True)
    assemble_far(0, 0, True)
    advance(0, 1, True, None)
    assemble_closer(1, 0, True)
    finish(0)
    assemble_far(1, 0, True)
    advance(1, 1, True, (0, 1))

    def step(i, carry):
        t = i // groups
        g = lax.rem(i, groups)
        assemble_closer(g, t - 1, False)
        finish(1 - g)
        assemble_far(g, t - 1, False)
        advance(g, t, False, (1 - g, jnp.where(g == 0, t - 1, t)))
        return carry

    lax.fori_loop(2 * groups, SWEEPS * groups, step, 0)

    u_copies = [pltpu.make_async_copy(u_v.at[k], u_out.at[:, pl.ds(k * LANES, LANES)], in_sem.at[0, k])
                for k in range(groups * TILES)]
    z_copies = [pltpu.make_async_copy(z_v.at[g], z_out.at[:, pl.ds(g * GROUP, GROUP)], out_sem.at[g])
                for g in range(groups)]
    for g in range(groups):
        for t in range(TILES):
            if g == 0:
                u_copies[t].start()
        assemble_closer(g, SWEEPS - 1, False)
        if g == 0:
            finish(1)
            for t in range(TILES):
                u_copies[TILES + t].start()
        assemble_far(g, SWEEPS - 1, False)
        if g == 0:
            pass_on(1, SWEEPS - 1, (0, 1, 2))
        solve_rest(g)
        z_v[g] = acc[g].astype(BF16)
        z_copies[g].start()
        if g == 0:
            pass_on(1, SWEEPS - 1, (3, 4))
    for g in range(groups):
        wait_sends(g, SWEEP_PARTS)
    for c in u_copies + z_copies:
        c.wait()


def solution(mesh):
    col_count = mesh.shape['col']
    grid_spec = P('row', 'col', None)

    def device_fn(f_blk, u_blk, kappa_blk, mat_blk, omega_relax):
        rhs_count = u_blk.shape[2]
        groups = rhs_count // GROUP
        tiles = rhs_count // LANES
        vm = pltpu.VMEM
        dma = pltpu.SemaphoreType.DMA
        coeff = vm((CELLS, LANES), F32)
        u_last, z_last = pl.pallas_call(
            functools.partial(kernel, groups, col_count),
            out_shape=(jax.ShapeDtypeStruct((CELLS, rhs_count), F32), jax.ShapeDtypeStruct((CELLS, rhs_count), BF16)),
            in_specs=[pl.BlockSpec(memory_space=pltpu.HBM), pl.BlockSpec(memory_space=pltpu.HBM),
                      pl.BlockSpec(memory_space=pltpu.VMEM), pl.BlockSpec(memory_space=pltpu.HBM),
                      pl.BlockSpec(memory_space=pltpu.SMEM)],
            out_specs=(pl.BlockSpec(memory_space=pl.ANY), pl.BlockSpec(memory_space=pl.ANY)),
            scratch_shapes=[
                vm((EXT * EXT, CELLS), BF16),
                vm((CELLS, EXT * EXT), BF16),
                vm((CELLS, DEPTH), BF16),
                vm((CELLS, 384), F32),
                vm((groups, CELLS, GROUP), F32),
                vm((tiles, CELLS, LANES), F32),
                vm((tiles, CELLS + 2 * PAD, LANES), F32),
                vm((tiles, CELLS, LANES), F32),
                vm((groups, DEPTH, GROUP), BF16),
                vm((groups, CELLS, GROUP), BF16),
                vm((CELLS + 2 * PAD, LANES), F32),
                coeff, coeff, coeff, coeff, coeff,
                vm((2, SUB, LANES), F32),
                vm((2, SUB, LANES), F32),
                vm((SUB, LANES), F32),
                vm((groups, 2, SUB, GROUP), F32),
                vm((groups, 2, 128, GROUP), BF16),
                vm((groups, 2, SUB, GROUP), F32),
                vm((2, groups, 2, SUB, GROUP), F32),
                vm((2, groups, 2, 128, GROUP), BF16),
                vm((1, groups, 2, SUB, GROUP), F32),
                vm((groups, TILES, SUB, LANES), F32),
                vm((groups, TILES, SUB, LANES), F32),
                vm((2, SUB, LANES), F32),
                vm((2, SUB, LANES), F32),
                vm((SUB, LANES), F32),
                vm((3, groups, SUB, GROUP), F32),
                vm((3, groups, 128, GROUP), BF16),
                vm((1, groups, SUB, GROUP), F32),
                dma((3, tiles)), dma, dma((groups,)),
                dma((groups, 2, 6)), dma((2, groups, 2, 6)),
                dma((groups,)), dma((groups,)),
                dma((groups, 2)), dma((groups, 2)),
                dma((3,)), dma((3,)),
                dma((groups, 6)), dma((3, groups, 6)),
            ],
            compiler_params=pltpu.CompilerParams(collective_id=0, has_side_effects=True,
                                                 vmem_limit_bytes=50 * 1024 * 1024),
        )(f_blk.reshape(CELLS, rhs_count), u_blk.reshape(CELLS, rhs_count), kappa_blk,
          mat_blk.reshape(CELLS, EXT * EXT).T, omega_relax.reshape(1))
        return (u_last + omega_relax * z_last.astype(F32)).reshape(SUB, SUB, rhs_count)

    return jax.shard_map(device_fn, mesh=mesh,
                         in_specs=(grid_spec, grid_spec, P('row', 'col'), P('row', 'col', None, None), P()),
                         out_specs=grid_spec, check_vma=False)
```

```python
import functools
import jax
import jax.numpy as jnp
from jax import lax
from jax.experimental import pallas as pl
from jax.experimental.pallas import tpu as pltpu
from jax.sharding import PartitionSpec as P

SWEEPS = 6
SUB = 32
MARGIN = 4
EXT = SUB + 2 * MARGIN
CELLS = SUB * SUB
LANES = 128
TILES = 2
GROUP = TILES * LANES
STEPS = MARGIN + 1
HALF_COLS = 2 * STEPS * 16
COLS_AT = CELLS
ROWS_AT = CELLS + 384
CORN_AT = ROWS_AT + 128
DEPTH = CORN_AT + 256
PAD = SUB
MESH = pl.DeviceIdType.MESH
F32 = jnp.float32
BF16 = jnp.bfloat16


def own_source(n):
    return ((n >> 5) + MARGIN) * EXT + (n & 31) + MARGIN


def mod(t, n):
    return t % n if isinstance(t, int) else lax.rem(t, n)


def column_source(m):
    side = m >= STEPS * 16
    k = jnp.where(side, m - STEPS * 16, m)
    return k & 15, jnp.where(side, MARGIN + SUB - 1 + (k >> 4), MARGIN - (k >> 4))


def kernel(groups, col_count,
           f_hbm, u_hbm, kap_ref, mat_hbm, om_ref, u_out, z_out,
           mat_v, mat_t, mat_p, wide, acc, res, zf, u_v, e_v, z_v, kb, coef, cedge, cedge_om, crow,
           send_p, send_b, send_u, recv_p, recv_b, recv_u, zrow_s, zrow, kcol_s, kcol_r, krow_r,
           via_p, via_b, via_u,
           in_sem, mat_sem, out_sem, s_sem, r_sem,
           sz_sem, rz_sem, sf_sem, rf_sem, sk_sem, rk_sem, vs_sem, vr_sem):
    col = lax.axis_index('col')
    row = lax.axis_index('row')
    has = (col > 0, col < col_count - 1)
    side_dev = ((col - 1, row), (col + 1, row))
    partner = (col, 1 - row)
    brow = (SUB - 1) * (1 - row)
    om = om_ref[0]

    routed = row == 1
    detour = (jnp.logical_and(routed, col == 2), jnp.logical_and(routed, col == 1))
    is_via = jnp.logical_and(routed, jnp.logical_or(col == 0, col == 3))
    mate = (lax.rem(col + 2, 4), row)
    via_to = (jnp.where(col == 0, 1, 2), row)
    via_side = jnp.where(col == 0, 1, 0)

    loads = []
    for g in range(groups):
        for t in range(TILES):
            k = g * TILES + t
            lanes = pl.ds(k * LANES, LANES)
            loads.append((
                pltpu.make_async_copy(u_hbm.at[:, lanes], zf.at[k, pl.ds(PAD, CELLS)], in_sem.at[0, k]),
                pltpu.make_async_copy(f_hbm.at[:, lanes], res.at[k], in_sem.at[1, k]),
                pltpu.make_async_copy(u_hbm.at[:, lanes], u_v.at[k], in_sem.at[2, k])))
    for a, b, c in loads:
        a.start()
        b.start()
    mat_copy = pltpu.make_async_copy(mat_hbm, mat_v, mat_sem)
    mat_copy.start()
    for a, b, c in loads:
        c.start()

    barrier = pltpu.get_barrier_semaphore()
    pl.semaphore_signal(barrier, inc=1, device_id=partner, device_id_type=MESH)
    for s in range(2):
        @pl.when(has[s])
        def _():
            pl.semaphore_signal(barrier, inc=1, device_id=side_dev[s], device_id_type=MESH)
    @pl.when(routed)
    def _():
        pl.semaphore_signal(barrier, inc=1, device_id=mate, device_id_type=MESH)
    waits = 1 + has[0].astype(jnp.int32) + has[1].astype(jnp.int32) + routed.astype(jnp.int32)
    pl.semaphore_wait(barrier, waits)

    zero_row = jnp.zeros((SUB, LANES), F32)
    kap_t = jnp.transpose(jnp.concatenate([kap_ref[...], jnp.zeros((LANES - SUB, SUB), F32)], axis=0))
    kb[pl.ds(0, SUB)] = zero_row
    kb[pl.ds(PAD + CELLS, SUB)] = zero_row
    for r in range(SUB):
        kb[pl.ds(PAD + r * SUB, SUB)] = jnp.broadcast_to(kap_t[:, r:r + 1], (SUB, LANES))

    def kcol_copy(s):
        return pltpu.make_async_remote_copy(kcol_s.at[s], kcol_r.at[1 - s], sk_sem.at[s], rk_sem.at[1 - s],
                                            device_id=side_dev[s], device_id_type=MESH)

    def krow_copy():
        return pltpu.make_async_remote_copy(kb.at[pl.ds(PAD + brow * SUB, SUB)], krow_r, sk_sem.at[2], rk_sem.at[2],
                                            device_id=partner, device_id_type=MESH)

    edge_col = (0, SUB - 1)

    def edge_cells(c, at=0):
        return pl.ds(at + c, SUB, stride=SUB)

    for s in range(2):
        kcol_s[s] = kb[edge_cells(edge_col[s], PAD), :]

        @pl.when(has[s])
        def _():
            kcol_copy(s).start()
    krow_copy().start()

    sub_id = lax.broadcasted_iota(jnp.int32, (SUB, LANES), 0)
    no_w = jnp.where(has[0], 0.0, 1.0)
    no_e = jnp.where(has[1], 0.0, 1.0)

    def coeff_row(q, carry):
        base = pl.multiple_of(q * SUB, SUB)
        here = kb[pl.ds(PAD + base, SUB)]
        up = kb[pl.ds(base, SUB)]
        down = kb[pl.ds(2 * PAD + base, SUB)]
        left = jnp.concatenate([here[:1], here[:-1]], axis=0)
        right = jnp.concatenate([here[1:], here[-1:]], axis=0)
        vn = jnp.where(q == 0, 0.0, 1.0) * (0.5 * (here + up))
        vs = jnp.where(q == SUB - 1, 0.0, 1.0) * (0.5 * (here + down))
        vw = jnp.where(sub_id == 0, 0.0, 0.5 * (here + left))
        ve = jnp.where(sub_id == SUB - 1, 0.0, 0.5 * (here + right))
        rim = jnp.where(jnp.logical_or(jnp.logical_and(q == 0, row == 0),
                                       jnp.logical_and(q == SUB - 1, row == 1)), 1.0, 0.0)
        rim_col = jnp.where(sub_id == 0, no_w, 0.0) + jnp.where(sub_id == SUB - 1, no_e, 0.0)
        rows = pl.ds(base, SUB)
        vd = vn + vs + vw + ve + (rim + rim_col) * here
        for j, v in enumerate((vd, vn, vs, vw, ve)):
            coef[0, j, rows] = v
            coef[1, j, rows] = om * v
        return carry

    lax.fori_loop(0, SUB, coeff_row, 0)

    def stencil(g, scaled, first, count, unroll):
        def one_row(q, carry):
            for at, n in zip(first, count):
                base = pl.multiple_of(q * SUB + at, 8)
                rows = pl.ds(base, n)
                vd, vn, vs, vw, ve = (coef[scaled, j, rows] for j in range(5))
                for t in range(TILES):
                    k = g * TILES + t
                    part = (vd * zf[k, pl.ds(PAD + base, n)]
                            - vn * zf[k, pl.ds(base, n)]
                            - vs * zf[k, pl.ds(2 * PAD + base, n)]
                            - vw * zf[k, pl.ds(PAD - 1 + base, n)]
                            - ve * zf[k, pl.ds(PAD + 1 + base, n)])
                    res[k, rows] = res[k, rows] - part
            return carry

        lax.fori_loop(0, SUB, one_row, 0, unroll=unroll)

    def stencil_sides(g, scaled):
        stencil(g, scaled, (0, SUB - 8), (8, 8), 8)

    def stencil_middle(g, scaled):
        stencil(g, scaled, (8,), (16,), 8)

    def zrow_copy(g):
        return pltpu.make_async_remote_copy(
            zrow_s.at[g], zrow.at[g], sz_sem.at[g], rz_sem.at[g], device_id=partner, device_id_type=MESH)

    brows = pl.ds(pl.multiple_of(brow * SUB, SUB), SUB)

    def row_fix(g, scaled):
        for t in range(TILES):
            k = g * TILES + t
            res[k, brows] = res[k, brows] - crow[scaled] * (zrow_s[g, t] - zrow[g, t])

    def near(s, dist):
        return dist if s == 0 else SUB - 1 - dist

    far = row
    closer = 1 - row

    def part(g, i):
        half = (closer, far)[(i - 1) // 2 % 2]
        if i in (1, 3):
            return 1, pl.ds(pl.multiple_of(16 * half, 16), 16)
        if i in (2, 4):
            return 0, pl.ds(pl.multiple_of(SUB + 48 * half, 16), 48)
        return (0 if i == 0 else 2), pl.ds(0, SUB)

    def message(g, s, t, i):
        kind, rows = part(g, i)
        slot = mod(t, 2)
        src = (send_b, send_p, send_u)[kind].at[g, s, rows]
        dst = (recv_b, recv_p, recv_u)[kind].at[slot, g, 1 - s, rows]
        return pltpu.make_async_remote_copy(src, dst, s_sem.at[g, s, i], r_sem.at[slot, g, 1 - s, i],
                                            device_id=side_dev[s], device_id_type=MESH)

    def message_out(g, s, t, i):
        kind, rows = part(g, i)
        slot = mod(t, 3)
        src = (send_b, send_p, send_u)[kind].at[g, s, rows]
        dst = (via_b, via_p, via_u)[kind].at[slot, g, rows]
        return pltpu.make_async_remote_copy(src, dst, s_sem.at[g, s, i], vr_sem.at[slot, g, i],
                                            device_id=mate, device_id_type=MESH)

    def message_on(g, t, i):
        kind, rows = part(g, i)
        slot = mod(t, 2)
        src = (via_b, via_p, via_u)[kind].at[mod(t, 3), g, rows]
        dst = (recv_b, recv_p, recv_u)[kind].at[slot, g, via_side, rows]
        return pltpu.make_async_remote_copy(src, dst, vs_sem.at[g, i], r_sem.at[slot, g, via_side, i],
                                            device_id=via_to, device_id_type=MESH)

    SWEEP_PARTS = (0, 1, 2, 3, 4)
    FIRST_PARTS = (5, 1, 2, 3, 4)

    def pass_on(g, t, parts):
        @pl.when(is_via)
        def _():
            for i in parts:
                message_out(g, 0, t, i).wait_recv()
                message_on(g, t, i).start()

    def fill_z(g, first):
        for s in range(2):
            for t in range(TILES):
                lanes = pl.ds(t * LANES, LANES)
                zedge = zf[g * TILES + t, edge_cells(near(s, 0), PAD), :]
                if first:
                    send_u[g, s, :, lanes] = zedge
                else:
                    send_b[g, s, pl.ds(0, SUB), lanes] = zedge.astype(BF16)

    def fill_half(g, h):
        at = pl.multiple_of(CELLS // 2 * h, CELLS // 2)
        p_at = pl.multiple_of(16 * h, 16)
        e_at = pl.multiple_of(SUB + 48 * h, 16)
        for s in range(2):
            for t in range(TILES):
                k = g * TILES + t
                lanes = pl.ds(t * LANES, LANES)
                for d in range(MARGIN):
                    part = res[k, pl.ds(at + near(s, d), 16, stride=SUB), :]
                    if d == 0:
                        send_p[g, s, pl.ds(p_at, 16), lanes] = part
                    else:
                        send_b[g, s, pl.ds(e_at + 16 * (d - 1), 16), lanes] = part.astype(BF16)

    def start(g, t, which):
        for s, turn in ((1, col < 2), (0, has[0]), (1, jnp.logical_and(col >= 2, has[1]))):
            @pl.when(jnp.logical_and(turn, jnp.logical_not(detour[s])))
            def _():
                for i in which:
                    message(g, s, t, i).start()

            @pl.when(jnp.logical_and(turn, detour[s]))
            def _():
                for i in which:
                    message_out(g, s, t, i).start()

    def fwd_rows(g):
        rows = pl.multiple_of((SUB - MARGIN) * SUB * (1 - row), 128)
        return pltpu.make_async_remote_copy(e_v.at[g, pl.ds(rows, 128)], e_v.at[g, pl.ds(ROWS_AT, 128)],
                                            sf_sem.at[g, 0], rf_sem.at[g, 0], device_id=partner, device_id_type=MESH)

    def fwd_corners(g):
        rows = pl.multiple_of(COLS_AT + HALF_COLS * closer, 32)
        return pltpu.make_async_remote_copy(e_v.at[g, pl.ds(rows, HALF_COLS)], e_v.at[g, pl.ds(CORN_AT, HALF_COLS)],
                                            sf_sem.at[g, 1], rf_sem.at[g, 1], device_id=partner, device_id_type=MESH)

    def assemble(g, sent, first, half, parts):
        slot = mod(sent, 2)
        for s in range(2):
            @pl.when(has[s])
            def _():
                for i in parts:
                    message(g, 1 - s, sent, i).wait_recv()
                rows = pl.ds(pl.multiple_of(16 * half, 16), 16)
                e_rows = pl.ds(pl.multiple_of(SUB + 48 * half, 16), 48)
                at = pl.multiple_of(CELLS // 2 * half, CELLS // 2)
                e_at = pl.multiple_of(COLS_AT + STEPS * 16 * s + HALF_COLS * half, 16)
                cells = pl.ds(at + edge_col[s], 16, stride=SUB)
                zcells = pl.ds(PAD + at + edge_col[s], 16, stride=SUB)
                coeff = (cedge if first else cedge_om)[s, rows]
                for t in range(TILES):
                    k = g * TILES + t
                    lanes = pl.ds(t * LANES, LANES)
                    if first:
                        theirs = recv_u[slot, g, s, rows, lanes]
                    else:
                        theirs = recv_b[slot, g, s, rows, lanes].astype(F32)
                    flux = coeff * (zf[k, zcells, :] - theirs)
                    own = res[k, cells, :] - flux
                    res[k, cells, :] = own
                    e_v[g, pl.ds(e_at, 16), lanes] = own.astype(BF16)
                    e_v[g, pl.ds(e_at + 16, 16), lanes] = (recv_p[slot, g, s, rows, lanes] + flux).astype(BF16)
                    e_v[g, pl.ds(e_at + 32, 48), lanes] = recv_b[slot, g, s, e_rows, lanes]

    def assemble_closer(g, sent, first):
        assemble(g, sent, first, closer, ((5 if first else 0), 1, 2))
        fwd_corners(g).start()

    def assemble_far(g, sent, first):
        assemble(g, sent, first, far, (3, 4))

    def pack(g):
        def one_row(q, carry):
            rows = pl.ds(pl.multiple_of(q * SUB, SUB), SUB)
            for t in range(TILES):
                e_v[g, rows, pl.ds(t * LANES, LANES)] = (keep * res[g * TILES + t, rows]).astype(BF16)
            return carry

        lax.fori_loop(0, SUB, one_row, 0, unroll=4)
        fwd_rows(g).start()

    def solve_own(g):
        def rows_of(m, carry):
            rows = pl.ds(pl.multiple_of(m * (CELLS // 2), CELLS // 2), CELLS // 2)
            acc[g, rows] = jnp.dot(mat_p[rows, :COLS_AT], e_v[g, pl.ds(0, COLS_AT)], preferred_element_type=F32)
            return carry

        lax.fori_loop(0, 2, rows_of, 0)

    def solve_rest(g):
        fwd_rows(g).wait()
        fwd_corners(g).wait()
        acc[g] += jnp.dot(mat_p[:, COLS_AT:], e_v[g, pl.ds(COLS_AT, DEPTH - COLS_AT)], preferred_element_type=F32)

    def round_row(g):
        for t in range(TILES):
            zrow_s[g, t] = acc[g, brows, pl.ds(t * LANES, LANES)].astype(BF16).astype(F32)

    def update(g):
        def rows_of(q, carry):
            rows = pl.ds(pl.multiple_of(q * 64, 64), 64)
            for t in range(TILES):
                k = g * TILES + t
                z = acc[g, rows, pl.ds(t * LANES, LANES)].astype(BF16).astype(F32)
                zf[k, pl.ds(pl.multiple_of(PAD + q * 64, PAD), 64)] = z
            return carry

        lax.fori_loop(0, CELLS // 64, rows_of, 0)

    for k in range(groups * TILES):
        zf[k, pl.ds(0, PAD)] = zero_row
        zf[k, pl.ds(PAD + CELLS, PAD)] = zero_row
    for g in range(groups):
        e_v[g, pl.ds(COLS_AT, ROWS_AT - COLS_AT)] = jnp.zeros((ROWS_AT - COLS_AT, GROUP), BF16)
        e_v[g, pl.ds(CORN_AT, DEPTH - CORN_AT)] = jnp.zeros((DEPTH - CORN_AT, GROUP), BF16)
    keep = (1.0 - jnp.where(jnp.logical_and(sub_id == 0, has[0]), 1.0, 0.0)
            - jnp.where(jnp.logical_and(sub_id == SUB - 1, has[1]), 1.0, 0.0))

    krow_copy().wait()
    rows_b = pl.ds(pl.multiple_of(PAD + brow * SUB, SUB), SUB)
    crow[0] = 0.5 * (kb[rows_b] + krow_r[...])
    crow[1] = om * crow[0]

    def send_bands(g, t, scaled):
        stencil_sides(g, scaled)
        zrow_copy(g).wait()
        row_fix(g, scaled)
        fill_half(g, closer)
        start(g, t, (1, 2))
        fill_half(g, far)
        start(g, t, (3, 4))

    for g in range(groups):
        for t in range(TILES):
            loads[g * TILES + t][0].wait()
        for t in range(TILES):
            zrow_s[g, t] = zf[g * TILES + t, rows_b]
        zrow_copy(g).start()
        fill_z(g, True)
        start(g, 0, (5,))
        for t in range(TILES):
            loads[g * TILES + t][1].wait()
        send_bands(g, 0, 0)

    def finish(g, scaled):
        stencil_middle(g, scaled)
        pack(g)

        def add_to_u(q, carry):
            rows = pl.ds(pl.multiple_of(q * SUB, SUB), SUB)
            for t in range(TILES):
                k = g * TILES + t
                u_v[k, rows] = u_v[k, rows] + om * zf[k, pl.ds(pl.multiple_of(PAD + q * SUB, PAD), SUB)]
            return carry

        if scaled:
            lax.fori_loop(0, SUB, add_to_u, 0, unroll=4)
        solve_own(g)

    mat_copy.wait()
    for at in range(0, EXT * EXT, 256):
        span = pl.ds(at, min(256, EXT * EXT - at))
        mat_t[:, span] = mat_v[span].T

    def place(at, width, start, window, source, ok=None, add=False):
        n = lax.broadcasted_iota(jnp.int32, (window, width), 1)
        k = lax.broadcasted_iota(jnp.int32, (window, width), 0) + start
        pick = source(n) == k
        if ok is not None:
            pick = jnp.logical_and(pick, ok(n))
        pick = jnp.where(pick, 1.0, 0.0).astype(BF16)

        wide[:, pl.ds(0, width)] = jnp.dot(mat_t[:, pl.ds(start, window)], pick, preferred_element_type=F32)
        placed = wide[:, pl.ds(0, width)].astype(BF16)
        if add:
            overlap = pl.ds(at, add)
            mat_p[:, overlap] = mat_p[:, overlap] + placed[:, :add]
            mat_p[:, pl.ds(at + add, width - add)] = placed[:, add:]
        else:
            mat_p[:, pl.ds(at, width)] = placed

    for q in range(4):
        low = (320 * q + 164) // 128 * 128
        high = -(-(320 * q + 476) // 128) * 128
        place(256 * q, 256, low, high - low, lambda n, q=q: own_source(n + 256 * q))

    pass_on(0, 0, FIRST_PARTS)
    finish(0, 0)

    def column(half):
        def source(n):
            r, c = column_source(n + 128 * half - HALF_COLS * half)
            return (MARGIN + 16 * half + r) * EXT + c
        return source

    place(COLS_AT, 256, 128, 768, column(0), lambda n: n < HALF_COLS)
    place(COLS_AT + 128, 256, 768, 768, column(1),
          lambda n: jnp.logical_and(n >= HALF_COLS - 128, n < 2 * HALF_COLS - 128), add=128)
    pass_on(1, 0, FIRST_PARTS)

    def halo(n):
        first_row = jnp.where(row == 0, MARGIN + SUB, 0)
        r, c = column_source(n - 128)
        corner_row = jnp.where(row == 0, MARGIN + SUB, -12) + r
        return jnp.where(n < 128, (first_row + (n >> 5)) * EXT + MARGIN + (n & 31), corner_row * EXT + c)

    def halo_ok(n):
        r = n & 15
        corner = jnp.logical_and(n < 128 + HALF_COLS, jnp.where(row == 0, r, 15 - r) < MARGIN)
        return jnp.logical_or(n < 128, corner)

    place(ROWS_AT, 384, pl.multiple_of(1408 * (1 - row), 128), 192, halo, halo_ok)

    for s in range(2):
        @pl.when(has[s])
        def _():
            kcol_copy(1 - s).wait_recv()
            cedge[s] = 0.5 * (kcol_s[s] + kcol_r[s])
            cedge_om[s] = om * cedge[s]
            kcol_copy(s).wait_send()
    for k in range(groups * TILES):
        loads[k][2].wait()

    def wait_sends(g, which):
        for s in range(2):
            @pl.when(has[s])
            def _():
                for i in which:
                    message(g, s, 0, i).wait_send()

        @pl.when(is_via)
        def _():
            for i in which:
                message_on(g, 0, i).wait_send()

    def advance(g, t, first, relay):
        if relay is not None:
            pass_on(relay[0], relay[1], (0, 1, 2))
        solve_rest(g)
        round_row(g)
        zrow_copy(g).start()
        update(g)
        wait_sends(g, FIRST_PARTS if first else SWEEP_PARTS)
        fill_z(g, False)
        start(g, t, (0,))
        if relay is not None:
            pass_on(relay[0], relay[1], (3, 4))
        send_bands(g, t, 1)

    assemble_closer(0, 0, True)
    finish(1, 0)
    assemble_far(0, 0, True)
    advance(0, 1, True, None)
    assemble_closer(1, 0, True)
    finish(0, 1)
    assemble_far(1, 0, True)
    advance(1, 1, True, (0, 1))

    def step(i, carry):
        t = i // groups
        g = lax.rem(i, groups)
        assemble_closer(g, t - 1, False)
        finish(1 - g, 1)
        assemble_far(g, t - 1, False)
        advance(g, t, False, (1 - g, jnp.where(g == 0, t - 1, t)))
        return carry

    lax.fori_loop(2 * groups, SWEEPS * groups, step, 0)

    u_copies = [pltpu.make_async_copy(u_v.at[k], u_out.at[:, pl.ds(k * LANES, LANES)], in_sem.at[0, k])
                for k in range(groups * TILES)]
    z_copies = [pltpu.make_async_copy(z_v.at[g], z_out.at[:, pl.ds(g * GROUP, GROUP)], out_sem.at[g])
                for g in range(groups)]
    for g in range(groups):
        for t in range(TILES):
            if g == 0:
                u_copies[t].start()
        assemble_closer(g, SWEEPS - 1, False)
        if g == 0:
            finish(1, 1)
            for t in range(TILES):
                u_copies[TILES + t].start()
        assemble_far(g, SWEEPS - 1, False)
        if g == 0:
            pass_on(1, SWEEPS - 1, (0, 1, 2))
        solve_rest(g)
        z_v[g] = acc[g].astype(BF16)
        z_copies[g].start()
        if g == 0:
            pass_on(1, SWEEPS - 1, (3, 4))
    for g in range(groups):
        wait_sends(g, SWEEP_PARTS)
    for c in u_copies + z_copies:
        c.wait()


def solution(mesh):
    col_count = mesh.shape['col']
    grid_spec = P('row', 'col', None)

    def device_fn(f_blk, u_blk, kappa_blk, mat_blk, omega_relax):
        rhs_count = u_blk.shape[2]
        groups = rhs_count // GROUP
        tiles = rhs_count // LANES
        vm = pltpu.VMEM
        dma = pltpu.SemaphoreType.DMA
        u_last, z_last = pl.pallas_call(
            functools.partial(kernel, groups, col_count),
            out_shape=(jax.ShapeDtypeStruct((CELLS, rhs_count), F32), jax.ShapeDtypeStruct((CELLS, rhs_count), BF16)),
            in_specs=[pl.BlockSpec(memory_space=pltpu.HBM), pl.BlockSpec(memory_space=pltpu.HBM),
                      pl.BlockSpec(memory_space=pltpu.VMEM), pl.BlockSpec(memory_space=pltpu.HBM),
                      pl.BlockSpec(memory_space=pltpu.SMEM)],
            out_specs=(pl.BlockSpec(memory_space=pl.ANY), pl.BlockSpec(memory_space=pl.ANY)),
            scratch_shapes=[
                vm((EXT * EXT, CELLS), BF16),
                vm((CELLS, EXT * EXT), BF16),
                vm((CELLS, DEPTH), BF16),
                vm((CELLS, 384), F32),
                vm((groups, CELLS, GROUP), F32),
                vm((tiles, CELLS, LANES), F32),
                vm((tiles, CELLS + 2 * PAD, LANES), F32),
                vm((tiles, CELLS, LANES), F32),
                vm((groups, DEPTH, GROUP), BF16),
                vm((groups, CELLS, GROUP), BF16),
                vm((CELLS + 2 * PAD, LANES), F32),
                vm((2, 5, CELLS, LANES), F32),
                vm((2, SUB, LANES), F32),
                vm((2, SUB, LANES), F32),
                vm((2, SUB, LANES), F32),
                vm((groups, 2, SUB, GROUP), F32),
                vm((groups, 2, 128, GROUP), BF16),
                vm((groups, 2, SUB, GROUP), F32),
                vm((2, groups, 2, SUB, GROUP), F32),
                vm((2, groups, 2, 128, GROUP), BF16),
                vm((1, groups, 2, SUB, GROUP), F32),
                vm((groups, TILES, SUB, LANES), F32),
                vm((groups, TILES, SUB, LANES), F32),
                vm((2, SUB, LANES), F32),
                vm((2, SUB, LANES), F32),
                vm((SUB, LANES), F32),
                vm((3, groups, SUB, GROUP), F32),
                vm((3, groups, 128, GROUP), BF16),
                vm((1, groups, SUB, GROUP), F32),
                dma((3, tiles)), dma, dma((groups,)),
                dma((groups, 2, 6)), dma((2, groups, 2, 6)),
                dma((groups,)), dma((groups,)),
                dma((groups, 2)), dma((groups, 2)),
                dma((3,)), dma((3,)),
                dma((groups, 6)), dma((3, groups, 6)),
            ],
            compiler_params=pltpu.CompilerParams(collective_id=0, has_side_effects=True,
                                                 vmem_limit_bytes=50 * 1024 * 1024),
        )(f_blk.reshape(CELLS, rhs_count), u_blk.reshape(CELLS, rhs_count), kappa_blk,
          mat_blk.reshape(CELLS, EXT * EXT).T, omega_relax.reshape(1))
        return (u_last + omega_relax * z_last.astype(F32)).reshape(SUB, SUB, rhs_count)

    return jax.shard_map(device_fn, mesh=mesh,
                         in_specs=(grid_spec, grid_spec, P('row', 'col'), P('row', 'col', None, None), P()),
                         out_specs=grid_spec, check_vma=False)
```

```python
import functools
import jax
import jax.numpy as jnp
from jax import lax
from jax.experimental import pallas as pl
from jax.experimental.pallas import tpu as pltpu
from jax.sharding import PartitionSpec as P

SWEEPS = 6
SUB = 32
MARGIN = 4
EXT = SUB + 2 * MARGIN
CELLS = SUB * SUB
LANES = 128
TILES = 2
GROUP = TILES * LANES
STEPS = MARGIN + 1
HALF_COLS = 2 * STEPS * 16
COLS_AT = CELLS
ROWS_AT = CELLS + 384
CORN_AT = ROWS_AT + 128
DEPTH = CORN_AT + 256
PAD = SUB
MESH = pl.DeviceIdType.MESH
F32 = jnp.float32
BF16 = jnp.bfloat16


def own_source(n):
    return ((n >> 5) + MARGIN) * EXT + (n & 31) + MARGIN


def mod(t, n):
    return t % n if isinstance(t, int) else lax.rem(t, n)


def column_source(m):
    side = m >= STEPS * 16
    k = jnp.where(side, m - STEPS * 16, m)
    return k & 15, jnp.where(side, MARGIN + SUB - 1 + (k >> 4), MARGIN - (k >> 4))


def kernel(groups, col_count,
           f_hbm, u_hbm, kap_ref, mat_hbm, om_ref, u_out, z_out,
           mat_v, mat_t, mat_p, wide, acc, res, zf, u_v, e_v, z_v, kb, coef, cedge, cedge_om, crow,
           send_p, send_b, send_u, recv_p, recv_b, recv_u, zrow_s, zrow, kcol_s, kcol_r, krow_r,
           via_p, via_b, via_u,
           in_sem, mat_sem, out_sem, s_sem, r_sem,
           sz_sem, rz_sem, sf_sem, rf_sem, sk_sem, rk_sem, vs_sem, vr_sem):
    col = lax.axis_index('col')
    row = lax.axis_index('row')
    has = (col > 0, col < col_count - 1)
    side_dev = ((col - 1, row), (col + 1, row))
    partner = (col, 1 - row)
    brow = (SUB - 1) * (1 - row)
    om = om_ref[0]

    routed = row == 1
    detour = (jnp.logical_and(routed, col == 2), jnp.logical_and(routed, col == 1))
    is_via = jnp.logical_and(routed, jnp.logical_or(col == 0, col == 3))
    mate = (lax.rem(col + 2, 4), row)
    via_to = (jnp.where(col == 0, 1, 2), row)
    via_side = jnp.where(col == 0, 1, 0)

    loads = []
    for g in range(groups):
        for t in range(TILES):
            k = g * TILES + t
            lanes = pl.ds(k * LANES, LANES)
            loads.append((
                pltpu.make_async_copy(u_hbm.at[:, lanes], zf.at[k, pl.ds(PAD, CELLS)], in_sem.at[0, k]),
                pltpu.make_async_copy(f_hbm.at[:, lanes], res.at[k], in_sem.at[1, k]),
                pltpu.make_async_copy(u_hbm.at[:, lanes], u_v.at[k], in_sem.at[2, k])))
    for a, b, c in loads:
        a.start()
        b.start()
    mat_copy = pltpu.make_async_copy(mat_hbm, mat_v, mat_sem)
    mat_copy.start()
    for a, b, c in loads:
        c.start()

    barrier = pltpu.get_barrier_semaphore()
    pl.semaphore_signal(barrier, inc=1, device_id=partner, device_id_type=MESH)
    for s in range(2):
        @pl.when(has[s])
        def _():
            pl.semaphore_signal(barrier, inc=1, device_id=side_dev[s], device_id_type=MESH)
    @pl.when(routed)
    def _():
        pl.semaphore_signal(barrier, inc=1, device_id=mate, device_id_type=MESH)
    waits = 1 + has[0].astype(jnp.int32) + has[1].astype(jnp.int32) + routed.astype(jnp.int32)
    pl.semaphore_wait(barrier, waits)

    zero_row = jnp.zeros((SUB, LANES), F32)
    kap_t = jnp.transpose(jnp.concatenate([kap_ref[...], jnp.zeros((LANES - SUB, SUB), F32)], axis=0))
    kb[pl.ds(0, SUB)] = zero_row
    kb[pl.ds(PAD + CELLS, SUB)] = zero_row
    for r in range(SUB):
        kb[pl.ds(PAD + r * SUB, SUB)] = jnp.broadcast_to(kap_t[:, r:r + 1], (SUB, LANES))

    def kcol_copy(s):
        return pltpu.make_async_remote_copy(kcol_s.at[s], kcol_r.at[1 - s], sk_sem.at[s], rk_sem.at[1 - s],
                                            device_id=side_dev[s], device_id_type=MESH)

    def krow_copy():
        return pltpu.make_async_remote_copy(kb.at[pl.ds(PAD + brow * SUB, SUB)], krow_r, sk_sem.at[2], rk_sem.at[2],
                                            device_id=partner, device_id_type=MESH)

    edge_col = (0, SUB - 1)

    def edge_cells(c, at=0):
        return pl.ds(at + c, SUB, stride=SUB)

    for s in range(2):
        kcol_s[s] = kb[edge_cells(edge_col[s], PAD), :]

        @pl.when(has[s])
        def _():
            kcol_copy(s).start()
    krow_copy().start()

    sub_id = lax.broadcasted_iota(jnp.int32, (SUB, LANES), 0)
    no_w = jnp.where(has[0], 0.0, 1.0)
    no_e = jnp.where(has[1], 0.0, 1.0)

    def coeff_row(q, carry):
        base = pl.multiple_of(q * SUB, SUB)
        here = kb[pl.ds(PAD + base, SUB)]
        up = kb[pl.ds(base, SUB)]
        down = kb[pl.ds(2 * PAD + base, SUB)]
        left = jnp.concatenate([here[:1], here[:-1]], axis=0)
        right = jnp.concatenate([here[1:], here[-1:]], axis=0)
        vn = jnp.where(q == 0, 0.0, 1.0) * (0.5 * (here + up))
        vs = jnp.where(q == SUB - 1, 0.0, 1.0) * (0.5 * (here + down))
        vw = jnp.where(sub_id == 0, 0.0, 0.5 * (here + left))
        ve = jnp.where(sub_id == SUB - 1, 0.0, 0.5 * (here + right))
        rim = jnp.where(jnp.logical_or(jnp.logical_and(q == 0, row == 0),
                                       jnp.logical_and(q == SUB - 1, row == 1)), 1.0, 0.0)
        rim_col = jnp.where(sub_id == 0, no_w, 0.0) + jnp.where(sub_id == SUB - 1, no_e, 0.0)
        rows = pl.ds(base, SUB)
        vd = vn + vs + vw + ve + (rim + rim_col) * here
        for j, v in enumerate((vd, vn, vs, vw, ve)):
            coef[0, j, rows] = v
            coef[1, j, rows] = om * v
        return carry

    lax.fori_loop(0, SUB, coeff_row, 0)

    def stencil(g, scaled):
        def one_row(q, carry):
            base = pl.multiple_of(q * SUB, SUB)
            rows = pl.ds(base, SUB)
            vd, vn, vs, vw, ve = (coef[scaled, j, rows] for j in range(5))
            for t in range(TILES):
                k = g * TILES + t
                part = (vd * zf[k, pl.ds(PAD + base, SUB)]
                        - vn * zf[k, pl.ds(base, SUB)]
                        - vs * zf[k, pl.ds(2 * PAD + base, SUB)]
                        - vw * zf[k, pl.ds(PAD - 1 + base, SUB)]
                        - ve * zf[k, pl.ds(PAD + 1 + base, SUB)])
                res[k, rows] = res[k, rows] - part
            return carry

        lax.fori_loop(0, SUB, one_row, 0, unroll=4)

    def zrow_copy(g):
        return pltpu.make_async_remote_copy(
            zrow_s.at[g], zrow.at[g], sz_sem.at[g], rz_sem.at[g], device_id=partner, device_id_type=MESH)

    brows = pl.ds(pl.multiple_of(brow * SUB, SUB), SUB)

    def row_fix(g, scaled):
        for t in range(TILES):
            k = g * TILES + t
            res[k, brows] = res[k, brows] - crow[scaled] * (zrow_s[g, t] - zrow[g, t])

    def near(s, dist):
        return dist if s == 0 else SUB - 1 - dist

    far = row
    closer = 1 - row

    def part(g, i):
        half = (closer, far)[(i - 1) // 2 % 2]
        if i in (1, 3):
            return 1, pl.ds(pl.multiple_of(16 * half, 16), 16)
        if i in (2, 4):
            return 0, pl.ds(pl.multiple_of(SUB + 48 * half, 16), 48)
        return (0 if i == 0 else 2), pl.ds(0, SUB)

    def message(g, s, t, i):
        kind, rows = part(g, i)
        slot = mod(t, 2)
        src = (send_b, send_p, send_u)[kind].at[g, s, rows]
        dst = (recv_b, recv_p, recv_u)[kind].at[slot, g, 1 - s, rows]
        return pltpu.make_async_remote_copy(src, dst, s_sem.at[g, s, i], r_sem.at[slot, g, 1 - s, i],
                                            device_id=side_dev[s], device_id_type=MESH)

    def message_out(g, s, t, i):
        kind, rows = part(g, i)
        slot = mod(t, 3)
        src = (send_b, send_p, send_u)[kind].at[g, s, rows]
        dst = (via_b, via_p, via_u)[kind].at[slot, g, rows]
        return pltpu.make_async_remote_copy(src, dst, s_sem.at[g, s, i], vr_sem.at[slot, g, i],
                                            device_id=mate, device_id_type=MESH)

    def message_on(g, t, i):
        kind, rows = part(g, i)
        slot = mod(t, 2)
        src = (via_b, via_p, via_u)[kind].at[mod(t, 3), g, rows]
        dst = (recv_b, recv_p, recv_u)[kind].at[slot, g, via_side, rows]
        return pltpu.make_async_remote_copy(src, dst, vs_sem.at[g, i], r_sem.at[slot, g, via_side, i],
                                            device_id=via_to, device_id_type=MESH)

    SWEEP_PARTS = (0, 1, 2, 3, 4)
    FIRST_PARTS = (5, 1, 2, 3, 4)

    def pass_on(g, t, parts):
        @pl.when(is_via)
        def _():
            for i in parts:
                message_out(g, 0, t, i).wait_recv()
                message_on(g, t, i).start()

    def fill_z(g, first):
        for s in range(2):
            for t in range(TILES):
                lanes = pl.ds(t * LANES, LANES)
                zedge = zf[g * TILES + t, edge_cells(near(s, 0), PAD), :]
                if first:
                    send_u[g, s, :, lanes] = zedge
                else:
                    send_b[g, s, pl.ds(0, SUB), lanes] = zedge.astype(BF16)

    def fill_half(g, h):
        at = pl.multiple_of(CELLS // 2 * h, CELLS // 2)
        p_at = pl.multiple_of(16 * h, 16)
        e_at = pl.multiple_of(SUB + 48 * h, 16)
        for s in range(2):
            for t in range(TILES):
                k = g * TILES + t
                lanes = pl.ds(t * LANES, LANES)
                for d in range(MARGIN):
                    part = res[k, pl.ds(at + near(s, d), 16, stride=SUB), :]
                    if d == 0:
                        send_p[g, s, pl.ds(p_at, 16), lanes] = part
                    else:
                        send_b[g, s, pl.ds(e_at + 16 * (d - 1), 16), lanes] = part.astype(BF16)

    def start(g, t, which):
        for s, turn in ((1, col < 2), (0, has[0]), (1, jnp.logical_and(col >= 2, has[1]))):
            @pl.when(jnp.logical_and(turn, jnp.logical_not(detour[s])))
            def _():
                for i in which:
                    message(g, s, t, i).start()

            @pl.when(jnp.logical_and(turn, detour[s]))
            def _():
                for i in which:
                    message_out(g, s, t, i).start()

    def fwd_rows(g):
        rows = pl.multiple_of((SUB - MARGIN) * SUB * (1 - row), 128)
        return pltpu.make_async_remote_copy(e_v.at[g, pl.ds(rows, 128)], e_v.at[g, pl.ds(ROWS_AT, 128)],
                                            sf_sem.at[g, 0], rf_sem.at[g, 0], device_id=partner, device_id_type=MESH)

    def fwd_corners(g):
        rows = pl.multiple_of(COLS_AT + HALF_COLS * closer, 32)
        return pltpu.make_async_remote_copy(e_v.at[g, pl.ds(rows, HALF_COLS)], e_v.at[g, pl.ds(CORN_AT, HALF_COLS)],
                                            sf_sem.at[g, 1], rf_sem.at[g, 1], device_id=partner, device_id_type=MESH)

    def assemble(g, sent, first, half, parts):
        slot = mod(sent, 2)
        for s in range(2):
            @pl.when(has[s])
            def _():
                for i in parts:
                    message(g, 1 - s, sent, i).wait_recv()
                rows = pl.ds(pl.multiple_of(16 * half, 16), 16)
                e_rows = pl.ds(pl.multiple_of(SUB + 48 * half, 16), 48)
                at = pl.multiple_of(CELLS // 2 * half, CELLS // 2)
                e_at = pl.multiple_of(COLS_AT + STEPS * 16 * s + HALF_COLS * half, 16)
                cells = pl.ds(at + edge_col[s], 16, stride=SUB)
                zcells = pl.ds(PAD + at + edge_col[s], 16, stride=SUB)
                coeff = (cedge if first else cedge_om)[s, rows]
                for t in range(TILES):
                    k = g * TILES + t
                    lanes = pl.ds(t * LANES, LANES)
                    if first:
                        theirs = recv_u[slot, g, s, rows, lanes]
                    else:
                        theirs = recv_b[slot, g, s, rows, lanes].astype(F32)
                    flux = coeff * (zf[k, zcells, :] - theirs)
                    own = res[k, cells, :] - flux
                    res[k, cells, :] = own
                    e_v[g, pl.ds(e_at, 16), lanes] = own.astype(BF16)
                    e_v[g, pl.ds(e_at + 16, 16), lanes] = (recv_p[slot, g, s, rows, lanes] + flux).astype(BF16)
                    e_v[g, pl.ds(e_at + 32, 48), lanes] = recv_b[slot, g, s, e_rows, lanes]

    def assemble_closer(g, sent, first):
        assemble(g, sent, first, closer, ((5 if first else 0), 1, 2))
        fwd_corners(g).start()

    def assemble_far(g, sent, first):
        assemble(g, sent, first, far, (3, 4))

    def pack(g, scaled):
        def one_row(q, carry):
            rows = pl.ds(pl.multiple_of(q * SUB, SUB), SUB)
            for t in range(TILES):
                k = g * TILES + t
                e_v[g, rows, pl.ds(t * LANES, LANES)] = (keep * res[k, rows]).astype(BF16)
                if scaled:
                    u_v[k, rows] = u_v[k, rows] + om * zf[k, pl.ds(pl.multiple_of(PAD + q * SUB, PAD), SUB)]
            return carry

        lax.fori_loop(0, SUB, one_row, 0, unroll=4)
        fwd_rows(g).start()

    def solve_own(g):
        def rows_of(m, carry):
            rows = pl.ds(pl.multiple_of(m * (CELLS // 2), CELLS // 2), CELLS // 2)
            acc[g, rows] = jnp.dot(mat_p[rows, :COLS_AT], e_v[g, pl.ds(0, COLS_AT)], preferred_element_type=F32)
            return carry

        lax.fori_loop(0, 2, rows_of, 0)

    def solve_rest(g):
        fwd_rows(g).wait()
        fwd_corners(g).wait()
        acc[g] += jnp.dot(mat_p[:, COLS_AT:], e_v[g, pl.ds(COLS_AT, DEPTH - COLS_AT)], preferred_element_type=F32)

    def round_row(g):
        for t in range(TILES):
            zrow_s[g, t] = acc[g, brows, pl.ds(t * LANES, LANES)].astype(BF16).astype(F32)

    def update(g):
        def rows_of(q, carry):
            rows = pl.ds(pl.multiple_of(q * 64, 64), 64)
            for t in range(TILES):
                k = g * TILES + t
                z = acc[g, rows, pl.ds(t * LANES, LANES)].astype(BF16).astype(F32)
                zf[k, pl.ds(pl.multiple_of(PAD + q * 64, PAD), 64)] = z
            return carry

        lax.fori_loop(0, CELLS // 64, rows_of, 0)

    for k in range(groups * TILES):
        zf[k, pl.ds(0, PAD)] = zero_row
        zf[k, pl.ds(PAD + CELLS, PAD)] = zero_row
    for g in range(groups):
        e_v[g, pl.ds(COLS_AT, ROWS_AT - COLS_AT)] = jnp.zeros((ROWS_AT - COLS_AT, GROUP), BF16)
        e_v[g, pl.ds(CORN_AT, DEPTH - CORN_AT)] = jnp.zeros((DEPTH - CORN_AT, GROUP), BF16)
    keep = (1.0 - jnp.where(jnp.logical_and(sub_id == 0, has[0]), 1.0, 0.0)
            - jnp.where(jnp.logical_and(sub_id == SUB - 1, has[1]), 1.0, 0.0))

    krow_copy().wait()
    rows_b = pl.ds(pl.multiple_of(PAD + brow * SUB, SUB), SUB)
    crow[0] = 0.5 * (kb[rows_b] + krow_r[...])
    crow[1] = om * crow[0]

    def send_bands(g, t, scaled):
        stencil(g, scaled)
        zrow_copy(g).wait()
        row_fix(g, scaled)
        fill_half(g, closer)
        start(g, t, (1, 2))
        fill_half(g, far)
        start(g, t, (3, 4))

    for g in range(groups):
        for t in range(TILES):
            loads[g * TILES + t][0].wait()
        for t in range(TILES):
            zrow_s[g, t] = zf[g * TILES + t, rows_b]
        zrow_copy(g).start()
        fill_z(g, True)
        start(g, 0, (5,))
        for t in range(TILES):
            loads[g * TILES + t][1].wait()
        send_bands(g, 0, 0)

    def finish(g, scaled):
        pack(g, scaled)
        solve_own(g)

    mat_copy.wait()
    for at in range(0, EXT * EXT, 256):
        span = pl.ds(at, min(256, EXT * EXT - at))
        mat_t[:, span] = mat_v[span].T

    def place(at, width, start, window, source, ok=None, add=False):
        n = lax.broadcasted_iota(jnp.int32, (window, width), 1)
        k = lax.broadcasted_iota(jnp.int32, (window, width), 0) + start
        pick = source(n) == k
        if ok is not None:
            pick = jnp.logical_and(pick, ok(n))
        pick = jnp.where(pick, 1.0, 0.0).astype(BF16)

        wide[:, pl.ds(0, width)] = jnp.dot(mat_t[:, pl.ds(start, window)], pick, preferred_element_type=F32)
        placed = wide[:, pl.ds(0, width)].astype(BF16)
        if add:
            overlap = pl.ds(at, add)
            mat_p[:, overlap] = mat_p[:, overlap] + placed[:, :add]
            mat_p[:, pl.ds(at + add, width - add)] = placed[:, add:]
        else:
            mat_p[:, pl.ds(at, width)] = placed

    for q in range(4):
        low = (320 * q + 164) // 128 * 128
        high = -(-(320 * q + 476) // 128) * 128
        place(256 * q, 256, low, high - low, lambda n, q=q: own_source(n + 256 * q))

    pass_on(0, 0, FIRST_PARTS)
    finish(0, 0)

    def column(half):
        def source(n):
            r, c = column_source(n + 128 * half - HALF_COLS * half)
            return (MARGIN + 16 * half + r) * EXT + c
        return source

    place(COLS_AT, 256, 128, 768, column(0), lambda n: n < HALF_COLS)
    place(COLS_AT + 128, 256, 768, 768, column(1),
          lambda n: jnp.logical_and(n >= HALF_COLS - 128, n < 2 * HALF_COLS - 128), add=128)
    pass_on(1, 0, FIRST_PARTS)

    def halo(n):
        first_row = jnp.where(row == 0, MARGIN + SUB, 0)
        r, c = column_source(n - 128)
        corner_row = jnp.where(row == 0, MARGIN + SUB, -12) + r
        return jnp.where(n < 128, (first_row + (n >> 5)) * EXT + MARGIN + (n & 31), corner_row * EXT + c)

    def halo_ok(n):
        r = n & 15
        corner = jnp.logical_and(n < 128 + HALF_COLS, jnp.where(row == 0, r, 15 - r) < MARGIN)
        return jnp.logical_or(n < 128, corner)

    place(ROWS_AT, 384, pl.multiple_of(1408 * (1 - row), 128), 192, halo, halo_ok)

    for s in range(2):
        @pl.when(has[s])
        def _():
            kcol_copy(1 - s).wait_recv()
            cedge[s] = 0.5 * (kcol_s[s] + kcol_r[s])
            cedge_om[s] = om * cedge[s]
            kcol_copy(s).wait_send()
    for k in range(groups * TILES):
        loads[k][2].wait()

    def wait_sends(g, which):
        for s in range(2):
            @pl.when(has[s])
            def _():
                for i in which:
                    message(g, s, 0, i).wait_send()

        @pl.when(is_via)
        def _():
            for i in which:
                message_on(g, 0, i).wait_send()

    def advance(g, t, first, relay):
        if relay is not None:
            pass_on(relay[0], relay[1], (0, 1, 2))
        solve_rest(g)
        round_row(g)
        zrow_copy(g).start()
        update(g)
        wait_sends(g, FIRST_PARTS if first else SWEEP_PARTS)
        fill_z(g, False)
        start(g, t, (0,))
        if relay is not None:
            pass_on(relay[0], relay[1], (3, 4))
        send_bands(g, t, 1)

    assemble_closer(0, 0, True)
    finish(1, 0)
    assemble_far(0, 0, True)
    advance(0, 1, True, None)
    assemble_closer(1, 0, True)
    finish(0, 1)
    assemble_far(1, 0, True)
    advance(1, 1, True, (0, 1))

    def step(i, carry):
        t = i // groups
        g = lax.rem(i, groups)
        assemble_closer(g, t - 1, False)
        finish(1 - g, 1)
        assemble_far(g, t - 1, False)
        advance(g, t, False, (1 - g, jnp.where(g == 0, t - 1, t)))
        return carry

    lax.fori_loop(2 * groups, SWEEPS * groups, step, 0)

    u_copies = [pltpu.make_async_copy(u_v.at[k], u_out.at[:, pl.ds(k * LANES, LANES)], in_sem.at[0, k])
                for k in range(groups * TILES)]
    z_copies = [pltpu.make_async_copy(z_v.at[g], z_out.at[:, pl.ds(g * GROUP, GROUP)], out_sem.at[g])
                for g in range(groups)]
    for g in range(groups):
        for t in range(TILES):
            if g == 0:
                u_copies[t].start()
        assemble_closer(g, SWEEPS - 1, False)
        if g == 0:
            finish(1, 1)
            for t in range(TILES):
                u_copies[TILES + t].start()
        assemble_far(g, SWEEPS - 1, False)
        if g == 0:
            pass_on(1, SWEEPS - 1, (0, 1, 2))
        solve_rest(g)
        z_v[g] = acc[g].astype(BF16)
        z_copies[g].start()
        if g == 0:
            pass_on(1, SWEEPS - 1, (3, 4))
    for g in range(groups):
        wait_sends(g, SWEEP_PARTS)
    for c in u_copies + z_copies:
        c.wait()


def solution(mesh):
    col_count = mesh.shape['col']
    grid_spec = P('row', 'col', None)

    def device_fn(f_blk, u_blk, kappa_blk, mat_blk, omega_relax):
        rhs_count = u_blk.shape[2]
        groups = rhs_count // GROUP
        tiles = rhs_count // LANES
        vm = pltpu.VMEM
        dma = pltpu.SemaphoreType.DMA
        u_last, z_last = pl.pallas_call(
            functools.partial(kernel, groups, col_count),
            out_shape=(jax.ShapeDtypeStruct((CELLS, rhs_count), F32), jax.ShapeDtypeStruct((CELLS, rhs_count), BF16)),
            in_specs=[pl.BlockSpec(memory_space=pltpu.HBM), pl.BlockSpec(memory_space=pltpu.HBM),
                      pl.BlockSpec(memory_space=pltpu.VMEM), pl.BlockSpec(memory_space=pltpu.HBM),
                      pl.BlockSpec(memory_space=pltpu.SMEM)],
            out_specs=(pl.BlockSpec(memory_space=pl.ANY), pl.BlockSpec(memory_space=pl.ANY)),
            scratch_shapes=[
                vm((EXT * EXT, CELLS), BF16),
                vm((CELLS, EXT * EXT), BF16),
                vm((CELLS, DEPTH), BF16),
                vm((CELLS, 384), F32),
                vm((groups, CELLS, GROUP), F32),
                vm((tiles, CELLS, LANES), F32),
                vm((tiles, CELLS + 2 * PAD, LANES), F32),
                vm((tiles, CELLS, LANES), F32),
                vm((groups, DEPTH, GROUP), BF16),
                vm((groups, CELLS, GROUP), BF16),
                vm((CELLS + 2 * PAD, LANES), F32),
                vm((2, 5, CELLS, LANES), F32),
                vm((2, SUB, LANES), F32),
                vm((2, SUB, LANES), F32),
                vm((2, SUB, LANES), F32),
                vm((groups, 2, SUB, GROUP), F32),
                vm((groups, 2, 128, GROUP), BF16),
                vm((groups, 2, SUB, GROUP), F32),
                vm((2, groups, 2, SUB, GROUP), F32),
                vm((2, groups, 2, 128, GROUP), BF16),
                vm((1, groups, 2, SUB, GROUP), F32),
                vm((groups, TILES, SUB, LANES), F32),
                vm((groups, TILES, SUB, LANES), F32),
                vm((2, SUB, LANES), F32),
                vm((2, SUB, LANES), F32),
                vm((SUB, LANES), F32),
                vm((3, groups, SUB, GROUP), F32),
                vm((3, groups, 128, GROUP), BF16),
                vm((1, groups, SUB, GROUP), F32),
                dma((3, tiles)), dma, dma((groups,)),
                dma((groups, 2, 6)), dma((2, groups, 2, 6)),
                dma((groups,)), dma((groups,)),
                dma((groups, 2)), dma((groups, 2)),
                dma((3,)), dma((3,)),
                dma((groups, 6)), dma((3, groups, 6)),
            ],
            compiler_params=pltpu.CompilerParams(collective_id=0, has_side_effects=True,
                                                 vmem_limit_bytes=50 * 1024 * 1024),
        )(f_blk.reshape(CELLS, rhs_count), u_blk.reshape(CELLS, rhs_count), kappa_blk,
          mat_blk.reshape(CELLS, EXT * EXT).T, omega_relax.reshape(1))
        return (u_last + omega_relax * z_last.astype(F32)).reshape(SUB, SUB, rhs_count)

    return jax.shard_map(device_fn, mesh=mesh,
                         in_specs=(grid_spec, grid_spec, P('row', 'col'), P('row', 'col', None, None), P()),
                         out_specs=grid_spec, check_vma=False)
```

```python
import functools
import jax
import jax.numpy as jnp
from jax import lax
from jax.experimental import pallas as pl
from jax.experimental.pallas import tpu as pltpu
from jax.sharding import PartitionSpec as P

SWEEPS = 6
SUB = 32
MARGIN = 4
EXT = SUB + 2 * MARGIN
CELLS = SUB * SUB
LANES = 128
TILES = 2
GROUP = TILES * LANES
STEPS = MARGIN + 1
HALF_COLS = 2 * STEPS * 16
COLS_AT = CELLS
ROWS_AT = CELLS + 384
CORN_AT = ROWS_AT + 128
DEPTH = CORN_AT + 256
PAD = SUB
MESH = pl.DeviceIdType.MESH
F32 = jnp.float32
BF16 = jnp.bfloat16


def own_source(n):
    return ((n >> 5) + MARGIN) * EXT + (n & 31) + MARGIN


def mod(t, n):
    return t % n if isinstance(t, int) else lax.rem(t, n)


def column_source(m):
    side = m >= STEPS * 16
    k = jnp.where(side, m - STEPS * 16, m)
    return k & 15, jnp.where(side, MARGIN + SUB - 1 + (k >> 4), MARGIN - (k >> 4))


def kernel(groups, col_count,
           f_hbm, u_hbm, kap_ref, mat_hbm, om_ref, u_out, z_out,
           mat_v, mat_t, mat_p, wide, acc, res, zf, u_v, e_v, z_v, kb, coef, cedge, cedge_om, crow,
           send_p, send_b, send_u, recv_p, recv_b, recv_u, zrow_s, zrow, kcol_s, kcol_r, krow_r,
           via_p, via_b, via_u,
           in_sem, mat_sem, out_sem, s_sem, r_sem,
           sz_sem, rz_sem, sf_sem, rf_sem, sk_sem, rk_sem, vs_sem, vr_sem):
    col = lax.axis_index('col')
    row = lax.axis_index('row')
    has = (col > 0, col < col_count - 1)
    side_dev = ((col - 1, row), (col + 1, row))
    partner = (col, 1 - row)
    brow = (SUB - 1) * (1 - row)
    om = om_ref[0]

    routed = row == 1
    detour = (jnp.logical_and(routed, col == 2), jnp.logical_and(routed, col == 1))
    is_via = jnp.logical_and(routed, jnp.logical_or(col == 0, col == 3))
    mate = (lax.rem(col + 2, 4), row)
    via_to = (jnp.where(col == 0, 1, 2), row)
    via_side = jnp.where(col == 0, 1, 0)

    loads = []
    for g in range(groups):
        for t in range(TILES):
            k = g * TILES + t
            lanes = pl.ds(k * LANES, LANES)
            loads.append((
                pltpu.make_async_copy(u_hbm.at[:, lanes], zf.at[k, pl.ds(PAD, CELLS)], in_sem.at[0, k]),
                pltpu.make_async_copy(f_hbm.at[:, lanes], res.at[k], in_sem.at[1, k])))
    mat_copy = pltpu.make_async_copy(mat_hbm, mat_v, mat_sem)
    for t in range(TILES):
        loads[t][0].start()
    for t in range(TILES):
        loads[t][1].start()

    barrier = pltpu.get_barrier_semaphore()
    pl.semaphore_signal(barrier, inc=1, device_id=partner, device_id_type=MESH)
    for s in range(2):
        @pl.when(has[s])
        def _():
            pl.semaphore_signal(barrier, inc=1, device_id=side_dev[s], device_id_type=MESH)
    @pl.when(routed)
    def _():
        pl.semaphore_signal(barrier, inc=1, device_id=mate, device_id_type=MESH)
    waits = 1 + has[0].astype(jnp.int32) + has[1].astype(jnp.int32) + routed.astype(jnp.int32)
    pl.semaphore_wait(barrier, waits)

    zero_row = jnp.zeros((SUB, LANES), F32)
    kap_t = jnp.transpose(jnp.concatenate([kap_ref[...], jnp.zeros((LANES - SUB, SUB), F32)], axis=0))
    kb[pl.ds(0, SUB)] = zero_row
    kb[pl.ds(PAD + CELLS, SUB)] = zero_row
    for r in range(SUB):
        kb[pl.ds(PAD + r * SUB, SUB)] = jnp.broadcast_to(kap_t[:, r:r + 1], (SUB, LANES))

    def kcol_copy(s):
        return pltpu.make_async_remote_copy(kcol_s.at[s], kcol_r.at[1 - s], sk_sem.at[s], rk_sem.at[1 - s],
                                            device_id=side_dev[s], device_id_type=MESH)

    def krow_copy():
        return pltpu.make_async_remote_copy(kb.at[pl.ds(PAD + brow * SUB, SUB)], krow_r, sk_sem.at[2], rk_sem.at[2],
                                            device_id=partner, device_id_type=MESH)

    edge_col = (0, SUB - 1)

    def edge_cells(c, at=0):
        return pl.ds(at + c, SUB, stride=SUB)

    for s in range(2):
        kcol_s[s] = kb[edge_cells(edge_col[s], PAD), :]

        @pl.when(has[s])
        def _():
            kcol_copy(s).start()
    krow_copy().start()

    sub_id = lax.broadcasted_iota(jnp.int32, (SUB, LANES), 0)
    no_w = jnp.where(has[0], 0.0, 1.0)
    no_e = jnp.where(has[1], 0.0, 1.0)

    def coeff_row(q, carry):
        base = pl.multiple_of(q * SUB, SUB)
        here = kb[pl.ds(PAD + base, SUB)]
        up = kb[pl.ds(base, SUB)]
        down = kb[pl.ds(2 * PAD + base, SUB)]
        left = jnp.concatenate([here[:1], here[:-1]], axis=0)
        right = jnp.concatenate([here[1:], here[-1:]], axis=0)
        vn = jnp.where(q == 0, 0.0, 1.0) * (0.5 * (here + up))
        vs = jnp.where(q == SUB - 1, 0.0, 1.0) * (0.5 * (here + down))
        vw = jnp.where(sub_id == 0, 0.0, 0.5 * (here + left))
        ve = jnp.where(sub_id == SUB - 1, 0.0, 0.5 * (here + right))
        rim = jnp.where(jnp.logical_or(jnp.logical_and(q == 0, row == 0),
                                       jnp.logical_and(q == SUB - 1, row == 1)), 1.0, 0.0)
        rim_col = jnp.where(sub_id == 0, no_w, 0.0) + jnp.where(sub_id == SUB - 1, no_e, 0.0)
        rows = pl.ds(base, SUB)
        vd = vn + vs + vw + ve + (rim + rim_col) * here
        for j, v in enumerate((vd, vn, vs, vw, ve)):
            coef[0, j, rows] = v
            coef[1, j, rows] = om * v
        return carry

    lax.fori_loop(0, SUB, coeff_row, 0)

    def stencil(g, scaled):
        def one_row(q, carry):
            base = pl.multiple_of(q * SUB, SUB)
            rows = pl.ds(base, SUB)
            vd, vn, vs, vw, ve = (coef[scaled, j, rows] for j in range(5))
            for t in range(TILES):
                k = g * TILES + t
                part = (vd * zf[k, pl.ds(PAD + base, SUB)]
                        - vn * zf[k, pl.ds(base, SUB)]
                        - vs * zf[k, pl.ds(2 * PAD + base, SUB)]
                        - vw * zf[k, pl.ds(PAD - 1 + base, SUB)]
                        - ve * zf[k, pl.ds(PAD + 1 + base, SUB)])
                res[k, rows] = res[k, rows] - part
            return carry

        lax.fori_loop(0, SUB, one_row, 0, unroll=4)

    def zrow_copy(g):
        return pltpu.make_async_remote_copy(
            zrow_s.at[g], zrow.at[g], sz_sem.at[g], rz_sem.at[g], device_id=partner, device_id_type=MESH)

    brows = pl.ds(pl.multiple_of(brow * SUB, SUB), SUB)

    def row_fix(g, scaled):
        for t in range(TILES):
            k = g * TILES + t
            res[k, brows] = res[k, brows] - crow[scaled] * (zrow_s[g, t] - zrow[g, t])

    def near(s, dist):
        return dist if s == 0 else SUB - 1 - dist

    far = row
    closer = 1 - row

    def part(i):
        return {0: (0, pl.ds(0, SUB)), 1: (1, pl.ds(0, 16)), 2: (0, pl.ds(SUB, 48)), 3: (1, pl.ds(16, 16)),
                4: (0, pl.ds(80, 48)), 5: (2, pl.ds(0, SUB))}[i]

    def message(g, s, t, i):
        kind, rows = part(i)
        slot = mod(t, 2)
        src = (send_b, send_p, send_u)[kind].at[g, s, rows]
        dst = (recv_b, recv_p, recv_u)[kind].at[slot, g, 1 - s, rows]
        return pltpu.make_async_remote_copy(src, dst, s_sem.at[g, s, i], r_sem.at[slot, g, 1 - s, i],
                                            device_id=side_dev[s], device_id_type=MESH)

    def message_out(g, s, t, i):
        kind, rows = part(i)
        slot = mod(t, 3)
        src = (send_b, send_p, send_u)[kind].at[g, s, rows]
        dst = (via_b, via_p, via_u)[kind].at[slot, g, rows]
        return pltpu.make_async_remote_copy(src, dst, s_sem.at[g, s, i], vr_sem.at[slot, g, i],
                                            device_id=mate, device_id_type=MESH)

    def message_on(g, t, i):
        kind, rows = part(i)
        slot = mod(t, 2)
        src = (via_b, via_p, via_u)[kind].at[mod(t, 3), g, rows]
        dst = (recv_b, recv_p, recv_u)[kind].at[slot, g, via_side, rows]
        return pltpu.make_async_remote_copy(src, dst, vs_sem.at[g, i], r_sem.at[slot, g, via_side, i],
                                            device_id=via_to, device_id_type=MESH)

    SWEEP_PARTS = (0, 2, 1, 4, 3)
    FIRST_PARTS = (5, 2, 1, 4, 3)

    def pass_on(g, t, parts):
        @pl.when(is_via)
        def _():
            for i in parts:
                message_out(g, 0, t, i).wait_recv()
                message_on(g, t, i).start()

    def fill_u(g):
        for s in range(2):
            for t in range(TILES):
                send_u[g, s, :, pl.ds(t * LANES, LANES)] = zf[g * TILES + t, edge_cells(near(s, 0), PAD), :]

    def fill_z(g):
        for j, h in enumerate((closer, far)):
            at = pl.multiple_of(CELLS // 2 * h, CELLS // 2)
            for s in range(2):
                for t in range(TILES):
                    zedge = zf[g * TILES + t, pl.ds(PAD + at + near(s, 0), 16, stride=SUB), :]
                    send_b[g, s, pl.ds(16 * j, 16), pl.ds(t * LANES, LANES)] = zedge.astype(BF16)

    def fill_half(g, h):
        at = pl.multiple_of(CELLS // 2 * h, CELLS // 2)
        j = 0 if h is closer else 1
        for s in range(2):
            for t in range(TILES):
                k = g * TILES + t
                lanes = pl.ds(t * LANES, LANES)
                for d in range(MARGIN):
                    band = res[k, pl.ds(at + near(s, d), 16, stride=SUB), :]
                    if d == 0:
                        send_p[g, s, pl.ds(16 * j, 16), lanes] = band
                    else:
                        send_b[g, s, pl.ds(SUB + 48 * j + 16 * (d - 1), 16), lanes] = band.astype(BF16)

    def start(g, t, which):
        for s, turn in ((1, col < 2), (0, has[0]), (1, jnp.logical_and(col >= 2, has[1]))):
            @pl.when(jnp.logical_and(turn, jnp.logical_not(detour[s])))
            def _():
                for i in which:
                    message(g, s, t, i).start()

            @pl.when(jnp.logical_and(turn, detour[s]))
            def _():
                for i in which:
                    message_out(g, s, t, i).start()

    def fwd_rows(g):
        rows = pl.multiple_of((SUB - MARGIN) * SUB * (1 - row), 128)
        return pltpu.make_async_remote_copy(e_v.at[g, pl.ds(rows, 128)], e_v.at[g, pl.ds(ROWS_AT, 128)],
                                            sf_sem.at[g, 0], rf_sem.at[g, 0], device_id=partner, device_id_type=MESH)

    def fwd_corners(g):
        rows = pl.multiple_of(COLS_AT + HALF_COLS * closer, 32)
        return pltpu.make_async_remote_copy(e_v.at[g, pl.ds(rows, HALF_COLS)], e_v.at[g, pl.ds(CORN_AT, HALF_COLS)],
                                            sf_sem.at[g, 1], rf_sem.at[g, 1], device_id=partner, device_id_type=MESH)

    def assemble(g, sent, first, half, parts):
        slot = mod(sent, 2)
        j = 0 if half is closer else 1
        j_rows = pl.ds(16 * j, 16)
        for s in range(2):
            @pl.when(has[s])
            def _():
                for i in parts:
                    message(g, 1 - s, sent, i).wait_recv()
                rows = pl.ds(pl.multiple_of(16 * half, 16), 16)
                e_rows = pl.ds(SUB + 48 * j, 48)
                at = pl.multiple_of(CELLS // 2 * half, CELLS // 2)
                e_at = pl.multiple_of(COLS_AT + STEPS * 16 * s + HALF_COLS * half, 16)
                cells = pl.ds(at + edge_col[s], 16, stride=SUB)
                zcells = pl.ds(PAD + at + edge_col[s], 16, stride=SUB)
                coeff = (cedge if first else cedge_om)[s, rows]
                for t in range(TILES):
                    k = g * TILES + t
                    lanes = pl.ds(t * LANES, LANES)
                    if first:
                        theirs = recv_u[slot, g, s, rows, lanes]
                    else:
                        theirs = recv_b[slot, g, s, j_rows, lanes].astype(F32)
                    flux = coeff * (zf[k, zcells, :] - theirs)
                    own = res[k, cells, :] - flux
                    res[k, cells, :] = own
                    e_v[g, pl.ds(e_at, 16), lanes] = own.astype(BF16)
                    e_v[g, pl.ds(e_at + 16, 16), lanes] = (recv_p[slot, g, s, j_rows, lanes] + flux).astype(BF16)
                    e_v[g, pl.ds(e_at + 32, 48), lanes] = recv_b[slot, g, s, e_rows, lanes]

    def assemble_closer(g, sent, first):
        assemble(g, sent, first, closer, (5 if first else 0, 2, 1))
        fwd_corners(g).start()

    def assemble_far(g, sent, first):
        assemble(g, sent, first, far, (4, 3))

    def pack(g, scaled):
        def one_row(q, carry):
            rows = pl.ds(pl.multiple_of(q * SUB, SUB), SUB)
            for t in range(TILES):
                k = g * TILES + t
                e_v[g, rows, pl.ds(t * LANES, LANES)] = (keep * res[k, rows]).astype(BF16)
                z = zf[k, pl.ds(pl.multiple_of(PAD + q * SUB, PAD), SUB)]
                u_v[k, rows] = u_v[k, rows] + om * z if scaled else z
            return carry

        lax.fori_loop(0, SUB, one_row, 0, unroll=4)
        fwd_rows(g).start()

    def solve_own(g):
        def rows_of(m, carry):
            rows = pl.ds(pl.multiple_of(m * (CELLS // 2), CELLS // 2), CELLS // 2)
            acc[g, rows] = jnp.dot(mat_p[rows, :COLS_AT], e_v[g, pl.ds(0, COLS_AT)], preferred_element_type=F32)
            return carry

        lax.fori_loop(0, 2, rows_of, 0)

    def solve_rest(g):
        fwd_rows(g).wait()
        fwd_corners(g).wait()
        acc[g] += jnp.dot(mat_p[:, COLS_AT:], e_v[g, pl.ds(COLS_AT, DEPTH - COLS_AT)], preferred_element_type=F32)

    def round_row(g):
        for t in range(TILES):
            zrow_s[g, t] = acc[g, brows, pl.ds(t * LANES, LANES)].astype(BF16).astype(F32)

    def update(g):
        def rows_of(q, carry):
            rows = pl.ds(pl.multiple_of(q * 64, 64), 64)
            for t in range(TILES):
                k = g * TILES + t
                z = acc[g, rows, pl.ds(t * LANES, LANES)].astype(BF16).astype(F32)
                zf[k, pl.ds(pl.multiple_of(PAD + q * 64, PAD), 64)] = z
            return carry

        lax.fori_loop(0, CELLS // 64, rows_of, 0)

    for k in range(groups * TILES):
        zf[k, pl.ds(0, PAD)] = zero_row
        zf[k, pl.ds(PAD + CELLS, PAD)] = zero_row
    for g in range(groups):
        e_v[g, pl.ds(COLS_AT, ROWS_AT - COLS_AT)] = jnp.zeros((ROWS_AT - COLS_AT, GROUP), BF16)
        e_v[g, pl.ds(CORN_AT, DEPTH - CORN_AT)] = jnp.zeros((DEPTH - CORN_AT, GROUP), BF16)
    keep = (1.0 - jnp.where(jnp.logical_and(sub_id == 0, has[0]), 1.0, 0.0)
            - jnp.where(jnp.logical_and(sub_id == SUB - 1, has[1]), 1.0, 0.0))

    krow_copy().wait()
    rows_b = pl.ds(pl.multiple_of(PAD + brow * SUB, SUB), SUB)
    crow[0] = 0.5 * (kb[rows_b] + krow_r[...])
    crow[1] = om * crow[0]

    def send_bands(g, t, scaled):
        stencil(g, scaled)
        zrow_copy(g).wait()
        row_fix(g, scaled)
        fill_half(g, closer)
        start(g, t, (2, 1))
        fill_half(g, far)
        start(g, t, (4, 3))

    for g in range(groups):
        for t in range(TILES):
            loads[g * TILES + t][0].wait()
        for t in range(TILES):
            zrow_s[g, t] = zf[g * TILES + t, rows_b]
        zrow_copy(g).start()
        fill_u(g)
        start(g, 0, (5,))
        for t in range(TILES):
            loads[g * TILES + t][1].wait()
        if g == 0:
            for a, b in loads[TILES:]:
                a.start()
                b.start()
            mat_copy.start()
        send_bands(g, 0, 0)

    def finish(g, scaled):
        pack(g, scaled)
        solve_own(g)

    mat_copy.wait()
    for at in range(0, EXT * EXT, 256):
        span = pl.ds(at, min(256, EXT * EXT - at))
        mat_t[:, span] = mat_v[span].T

    def place(at, width, start, window, source, ok=None, add=False):
        n = lax.broadcasted_iota(jnp.int32, (window, width), 1)
        k = lax.broadcasted_iota(jnp.int32, (window, width), 0) + start
        pick = source(n) == k
        if ok is not None:
            pick = jnp.logical_and(pick, ok(n))
        pick = jnp.where(pick, 1.0, 0.0).astype(BF16)

        wide[:, pl.ds(0, width)] = jnp.dot(mat_t[:, pl.ds(start, window)], pick, preferred_element_type=F32)
        placed = wide[:, pl.ds(0, width)].astype(BF16)
        if add:
            overlap = pl.ds(at, add)
            mat_p[:, overlap] = mat_p[:, overlap] + placed[:, :add]
            mat_p[:, pl.ds(at + add, width - add)] = placed[:, add:]
        else:
            mat_p[:, pl.ds(at, width)] = placed

    for q in range(4):
        low = (320 * q + 164) // 128 * 128
        high = -(-(320 * q + 476) // 128) * 128
        place(256 * q, 256, low, high - low, lambda n, q=q: own_source(n + 256 * q))

    pass_on(0, 0, FIRST_PARTS)
    finish(0, 0)

    def column(half):
        def source(n):
            r, c = column_source(n + 128 * half - HALF_COLS * half)
            return (MARGIN + 16 * half + r) * EXT + c
        return source

    place(COLS_AT, 256, 128, 768, column(0), lambda n: n < HALF_COLS)
    place(COLS_AT + 128, 256, 768, 768, column(1),
          lambda n: jnp.logical_and(n >= HALF_COLS - 128, n < 2 * HALF_COLS - 128), add=128)
    pass_on(1, 0, FIRST_PARTS)

    def halo(n):
        first_row = jnp.where(row == 0, MARGIN + SUB, 0)
        r, c = column_source(n - 128)
        corner_row = jnp.where(row == 0, MARGIN + SUB, -12) + r
        return jnp.where(n < 128, (first_row + (n >> 5)) * EXT + MARGIN + (n & 31), corner_row * EXT + c)

    def halo_ok(n):
        r = n & 15
        corner = jnp.logical_and(n < 128 + HALF_COLS, jnp.where(row == 0, r, 15 - r) < MARGIN)
        return jnp.logical_or(n < 128, corner)

    place(ROWS_AT, 384, pl.multiple_of(1408 * (1 - row), 128), 192, halo, halo_ok)

    for s in range(2):
        @pl.when(has[s])
        def _():
            kcol_copy(1 - s).wait_recv()
            cedge[s] = 0.5 * (kcol_s[s] + kcol_r[s])
            cedge_om[s] = om * cedge[s]
            kcol_copy(s).wait_send()

    def wait_sends(g, which):
        for s in range(2):
            @pl.when(has[s])
            def _():
                for i in which:
                    message(g, s, 0, i).wait_send()

        @pl.when(is_via)
        def _():
            for i in which:
                message_on(g, 0, i).wait_send()

    def advance(g, t, first, relay):
        if relay is not None:
            pass_on(relay[0], relay[1], (0, 2, 1))
        solve_rest(g)
        round_row(g)
        zrow_copy(g).start()
        update(g)
        wait_sends(g, FIRST_PARTS if first else SWEEP_PARTS)
        fill_z(g)
        start(g, t, (0,))
        if relay is not None:
            pass_on(relay[0], relay[1], (4, 3))
        send_bands(g, t, 1)

    assemble_closer(0, 0, True)
    finish(1, 0)
    assemble_far(0, 0, True)
    advance(0, 1, True, None)
    assemble_closer(1, 0, True)
    finish(0, 1)
    assemble_far(1, 0, True)
    advance(1, 1, True, (0, 1))

    def step(i, carry):
        t = i // groups
        g = lax.rem(i, groups)
        assemble_closer(g, t - 1, False)
        finish(1 - g, 1)
        assemble_far(g, t - 1, False)
        advance(g, t, False, (1 - g, jnp.where(g == 0, t - 1, t)))
        return carry

    lax.fori_loop(2 * groups, SWEEPS * groups, step, 0)

    u_copies = [pltpu.make_async_copy(u_v.at[k], u_out.at[:, pl.ds(k * LANES, LANES)], in_sem.at[0, k])
                for k in range(groups * TILES)]
    z_copies = [pltpu.make_async_copy(z_v.at[g], z_out.at[:, pl.ds(g * GROUP, GROUP)], out_sem.at[g])
                for g in range(groups)]
    for g in range(groups):
        for t in range(TILES):
            if g == 0:
                u_copies[t].start()
        assemble_closer(g, SWEEPS - 1, False)
        if g == 0:
            finish(1, 1)
            for t in range(TILES):
                u_copies[TILES + t].start()
        assemble_far(g, SWEEPS - 1, False)
        if g == 0:
            pass_on(1, SWEEPS - 1, (0, 2, 1))
        solve_rest(g)
        z_v[g] = acc[g].astype(BF16)
        z_copies[g].start()
        if g == 0:
            pass_on(1, SWEEPS - 1, (4, 3))
    for g in range(groups):
        wait_sends(g, SWEEP_PARTS)
    for c in u_copies + z_copies:
        c.wait()


def solution(mesh):
    col_count = mesh.shape['col']
    grid_spec = P('row', 'col', None)

    def device_fn(f_blk, u_blk, kappa_blk, mat_blk, omega_relax):
        rhs_count = u_blk.shape[2]
        groups = rhs_count // GROUP
        tiles = rhs_count // LANES
        vm = pltpu.VMEM
        dma = pltpu.SemaphoreType.DMA
        u_last, z_last = pl.pallas_call(
            functools.partial(kernel, groups, col_count),
            out_shape=(jax.ShapeDtypeStruct((CELLS, rhs_count), F32), jax.ShapeDtypeStruct((CELLS, rhs_count), BF16)),
            in_specs=[pl.BlockSpec(memory_space=pltpu.HBM), pl.BlockSpec(memory_space=pltpu.HBM),
                      pl.BlockSpec(memory_space=pltpu.VMEM), pl.BlockSpec(memory_space=pltpu.HBM),
                      pl.BlockSpec(memory_space=pltpu.SMEM)],
            out_specs=(pl.BlockSpec(memory_space=pl.ANY), pl.BlockSpec(memory_space=pl.ANY)),
            scratch_shapes=[
                vm((EXT * EXT, CELLS), BF16),
                vm((CELLS, EXT * EXT), BF16),
                vm((CELLS, DEPTH), BF16),
                vm((CELLS, 384), F32),
                vm((groups, CELLS, GROUP), F32),
                vm((tiles, CELLS, LANES), F32),
                vm((tiles, CELLS + 2 * PAD, LANES), F32),
                vm((tiles, CELLS, LANES), F32),
                vm((groups, DEPTH, GROUP), BF16),
                vm((groups, CELLS, GROUP), BF16),
                vm((CELLS + 2 * PAD, LANES), F32),
                vm((2, 5, CELLS, LANES), F32),
                vm((2, SUB, LANES), F32),
                vm((2, SUB, LANES), F32),
                vm((2, SUB, LANES), F32),
                vm((groups, 2, SUB, GROUP), F32),
                vm((groups, 2, 128, GROUP), BF16),
                vm((groups, 2, SUB, GROUP), F32),
                vm((2, groups, 2, SUB, GROUP), F32),
                vm((2, groups, 2, 128, GROUP), BF16),
                vm((1, groups, 2, SUB, GROUP), F32),
                vm((groups, TILES, SUB, LANES), F32),
                vm((groups, TILES, SUB, LANES), F32),
                vm((2, SUB, LANES), F32),
                vm((2, SUB, LANES), F32),
                vm((SUB, LANES), F32),
                vm((3, groups, SUB, GROUP), F32),
                vm((3, groups, 128, GROUP), BF16),
                vm((1, groups, SUB, GROUP), F32),
                dma((2, tiles)), dma, dma((groups,)),
                dma((groups, 2, 6)), dma((2, groups, 2, 6)),
                dma((groups,)), dma((groups,)),
                dma((groups, 2)), dma((groups, 2)),
                dma((3,)), dma((3,)),
                dma((groups, 6)), dma((3, groups, 6)),
            ],
            compiler_params=pltpu.CompilerParams(collective_id=0, has_side_effects=True,
                                                 vmem_limit_bytes=50 * 1024 * 1024),
        )(f_blk.reshape(CELLS, rhs_count), u_blk.reshape(CELLS, rhs_count), kappa_blk,
          mat_blk.reshape(CELLS, EXT * EXT).T, omega_relax.reshape(1))
        return (u_last + omega_relax * z_last.astype(F32)).reshape(SUB, SUB, rhs_count)

    return jax.shard_map(device_fn, mesh=mesh,
                         in_specs=(grid_spec, grid_spec, P('row', 'col'), P('row', 'col', None, None), P()),
                         out_specs=grid_spec, check_vma=False)
```

```python
import functools
import jax
import jax.numpy as jnp
from jax import lax
from jax.experimental import pallas as pl
from jax.experimental.pallas import tpu as pltpu
from jax.sharding import PartitionSpec as P

SWEEPS = 6
SUB = 32
MARGIN = 4
EXT = SUB + 2 * MARGIN
CELLS = SUB * SUB
LANES = 128
TILES = 2
GROUP = TILES * LANES
STEPS = MARGIN + 1
HALF_COLS = 2 * STEPS * 16
COLS_AT = CELLS
ROWS_AT = CELLS + 384
CORN_AT = ROWS_AT + 128
DEPTH = CORN_AT + 256
PAD = SUB
MESH = pl.DeviceIdType.MESH
F32 = jnp.float32
BF16 = jnp.bfloat16


def own_source(n):
    return ((n >> 5) + MARGIN) * EXT + (n & 31) + MARGIN


def mod(t, n):
    return t % n if isinstance(t, int) else lax.rem(t, n)


def column_source(m):
    side = m >= STEPS * 16
    k = jnp.where(side, m - STEPS * 16, m)
    return k & 15, jnp.where(side, MARGIN + SUB - 1 + (k >> 4), MARGIN - (k >> 4))


def kernel(groups, col_count,
           f_hbm, u_hbm, kap_ref, mat_hbm, om_ref, u_out, z_out,
           mat_v, mat_t, mat_p, wide, acc, res, zf, u_v, e_v, z_v, kb, coef, cedge, cedge_om, crow,
           send_p, send_b, send_u, recv_p, recv_b, recv_u, zrow_s, zrow, kcol_s, kcol_r, krow_r,
           via_p, via_b, via_u,
           in_sem, mat_sem, out_sem, s_sem, r_sem,
           sz_sem, rz_sem, sf_sem, rf_sem, sk_sem, rk_sem, vs_sem, vr_sem):
    col = lax.axis_index('col')
    row = lax.axis_index('row')
    has = (col > 0, col < col_count - 1)
    side_dev = ((col - 1, row), (col + 1, row))
    partner = (col, 1 - row)
    brow = (SUB - 1) * (1 - row)
    om = om_ref[0]

    routed = row == 1
    detour = (jnp.logical_and(routed, col == 2), jnp.logical_and(routed, col == 1))
    is_via = jnp.logical_and(routed, jnp.logical_or(col == 0, col == 3))
    mate = (lax.rem(col + 2, 4), row)
    via_to = (jnp.where(col == 0, 1, 2), row)
    via_side = jnp.where(col == 0, 1, 0)

    loads = []
    for g in range(groups):
        for t in range(TILES):
            k = g * TILES + t
            lanes = pl.ds(k * LANES, LANES)
            loads.append((
                pltpu.make_async_copy(u_hbm.at[:, lanes], zf.at[k, pl.ds(PAD, CELLS)], in_sem.at[0, k]),
                pltpu.make_async_copy(f_hbm.at[:, lanes], res.at[k], in_sem.at[1, k])))
    mat_copy = pltpu.make_async_copy(mat_hbm, mat_v, mat_sem)
    for t in range(TILES):
        loads[t][0].start()
    for t in range(TILES):
        loads[t][1].start()

    barrier = pltpu.get_barrier_semaphore()
    pl.semaphore_signal(barrier, inc=1, device_id=partner, device_id_type=MESH)
    for s in range(2):
        @pl.when(has[s])
        def _():
            pl.semaphore_signal(barrier, inc=1, device_id=side_dev[s], device_id_type=MESH)
    @pl.when(routed)
    def _():
        pl.semaphore_signal(barrier, inc=1, device_id=mate, device_id_type=MESH)
    waits = 1 + has[0].astype(jnp.int32) + has[1].astype(jnp.int32) + routed.astype(jnp.int32)
    pl.semaphore_wait(barrier, waits)

    zero_row = jnp.zeros((SUB, LANES), F32)
    kap_t = jnp.transpose(jnp.concatenate([kap_ref[...], jnp.zeros((LANES - SUB, SUB), F32)], axis=0))
    kb[pl.ds(0, SUB)] = zero_row
    kb[pl.ds(PAD + CELLS, SUB)] = zero_row
    for r in range(SUB):
        kb[pl.ds(PAD + r * SUB, SUB)] = jnp.broadcast_to(kap_t[:, r:r + 1], (SUB, LANES))

    def kcol_copy(s):
        return pltpu.make_async_remote_copy(kcol_s.at[s], kcol_r.at[1 - s], sk_sem.at[s], rk_sem.at[1 - s],
                                            device_id=side_dev[s], device_id_type=MESH)

    def krow_copy():
        return pltpu.make_async_remote_copy(kb.at[pl.ds(PAD + brow * SUB, SUB)], krow_r, sk_sem.at[2], rk_sem.at[2],
                                            device_id=partner, device_id_type=MESH)

    edge_col = (0, SUB - 1)

    def edge_cells(c, at=0):
        return pl.ds(at + c, SUB, stride=SUB)

    for s in range(2):
        kcol_s[s] = kb[edge_cells(edge_col[s], PAD), :]

        @pl.when(has[s])
        def _():
            kcol_copy(s).start()
    krow_copy().start()

    sub_id = lax.broadcasted_iota(jnp.int32, (SUB, LANES), 0)
    no_w = jnp.where(has[0], 0.0, 1.0)
    no_e = jnp.where(has[1], 0.0, 1.0)

    def coeff_row(q, carry):
        base = pl.multiple_of(q * SUB, SUB)
        here = kb[pl.ds(PAD + base, SUB)]
        up = kb[pl.ds(base, SUB)]
        down = kb[pl.ds(2 * PAD + base, SUB)]
        left = jnp.concatenate([here[:1], here[:-1]], axis=0)
        right = jnp.concatenate([here[1:], here[-1:]], axis=0)
        vn = jnp.where(q == 0, 0.0, 1.0) * (0.5 * (here + up))
        vs = jnp.where(q == SUB - 1, 0.0, 1.0) * (0.5 * (here + down))
        vw = jnp.where(sub_id == 0, 0.0, 0.5 * (here + left))
        ve = jnp.where(sub_id == SUB - 1, 0.0, 0.5 * (here + right))
        rim = jnp.where(jnp.logical_or(jnp.logical_and(q == 0, row == 0),
                                       jnp.logical_and(q == SUB - 1, row == 1)), 1.0, 0.0)
        rim_col = jnp.where(sub_id == 0, no_w, 0.0) + jnp.where(sub_id == SUB - 1, no_e, 0.0)
        rows = pl.ds(base, SUB)
        vd = vn + vs + vw + ve + (rim + rim_col) * here
        for j, v in enumerate((vd, vn, vs, vw, ve)):
            coef[0, j, rows] = v
            coef[1, j, rows] = om * v
        return carry

    lax.fori_loop(0, SUB, coeff_row, 0)

    def stencil(g, scaled):
        def one_row(q, carry):
            base = pl.multiple_of(q * SUB, SUB)
            rows = pl.ds(base, SUB)
            vd, vn, vs, vw, ve = (coef[scaled, j, rows] for j in range(5))
            for t in range(TILES):
                k = g * TILES + t
                part = (vd * zf[k, pl.ds(PAD + base, SUB)]
                        - vn * zf[k, pl.ds(base, SUB)]
                        - vs * zf[k, pl.ds(2 * PAD + base, SUB)]
                        - vw * zf[k, pl.ds(PAD - 1 + base, SUB)]
                        - ve * zf[k, pl.ds(PAD + 1 + base, SUB)])
                res[k, rows] = res[k, rows] - part
            return carry

        lax.fori_loop(0, SUB, one_row, 0, unroll=4)

    def zrow_copy(g):
        return pltpu.make_async_remote_copy(
            zrow_s.at[g], zrow.at[g], sz_sem.at[g], rz_sem.at[g], device_id=partner, device_id_type=MESH)

    brows = pl.ds(pl.multiple_of(brow * SUB, SUB), SUB)

    def row_fix(g, scaled):
        for t in range(TILES):
            k = g * TILES + t
            res[k, brows] = res[k, brows] - crow[scaled] * (zrow_s[g, t] - zrow[g, t])

    def near(s, dist):
        return dist if s == 0 else SUB - 1 - dist

    far = row
    closer = 1 - row

    def part(i):
        return {0: (0, pl.ds(0, SUB)), 1: (1, pl.ds(0, 16)), 2: (0, pl.ds(SUB, 48)), 3: (1, pl.ds(16, 16)),
                4: (0, pl.ds(80, 48)), 5: (2, pl.ds(0, SUB))}[i]

    def message(g, s, t, i):
        kind, rows = part(i)
        slot = mod(t, 2)
        src = (send_b, send_p, send_u)[kind].at[g, s, rows]
        dst = (recv_b, recv_p, recv_u)[kind].at[slot, g, 1 - s, rows]
        return pltpu.make_async_remote_copy(src, dst, s_sem.at[g, s, i], r_sem.at[slot, g, 1 - s, i],
                                            device_id=side_dev[s], device_id_type=MESH)

    def message_out(g, s, t, i):
        kind, rows = part(i)
        slot = mod(t, 3)
        src = (send_b, send_p, send_u)[kind].at[g, s, rows]
        dst = (via_b, via_p, via_u)[kind].at[slot, g, rows]
        return pltpu.make_async_remote_copy(src, dst, s_sem.at[g, s, i], vr_sem.at[slot, g, i],
                                            device_id=mate, device_id_type=MESH)

    def message_on(g, t, i):
        kind, rows = part(i)
        slot = mod(t, 2)
        src = (via_b, via_p, via_u)[kind].at[mod(t, 3), g, rows]
        dst = (recv_b, recv_p, recv_u)[kind].at[slot, g, via_side, rows]
        return pltpu.make_async_remote_copy(src, dst, vs_sem.at[g, i], r_sem.at[slot, g, via_side, i],
                                            device_id=via_to, device_id_type=MESH)

    SWEEP_PARTS = (0, 2, 1, 4, 3)
    FIRST_PARTS = (5, 2, 1, 4, 3)

    def pass_on(g, t, parts):
        @pl.when(is_via)
        def _():
            for i in parts:
                message_out(g, 0, t, i).wait_recv()
                message_on(g, t, i).start()

    def fill_u(g):
        for s in range(2):
            for t in range(TILES):
                send_u[g, s, :, pl.ds(t * LANES, LANES)] = zf[g * TILES + t, edge_cells(near(s, 0), PAD), :]

    def fill_z(g):
        for j, h in enumerate((closer, far)):
            at = pl.multiple_of(CELLS // 2 * h, CELLS // 2)
            for s in range(2):
                for t in range(TILES):
                    zedge = zf[g * TILES + t, pl.ds(PAD + at + near(s, 0), 16, stride=SUB), :]
                    send_b[g, s, pl.ds(16 * j, 16), pl.ds(t * LANES, LANES)] = zedge.astype(BF16)

    def fill_half(g, h):
        at = pl.multiple_of(CELLS // 2 * h, CELLS // 2)
        j = 0 if h is closer else 1
        for s in range(2):
            for t in range(TILES):
                k = g * TILES + t
                lanes = pl.ds(t * LANES, LANES)
                for d in range(MARGIN):
                    band = res[k, pl.ds(at + near(s, d), 16, stride=SUB), :]
                    if d == 0:
                        send_p[g, s, pl.ds(16 * j, 16), lanes] = band
                    else:
                        send_b[g, s, pl.ds(SUB + 48 * j + 16 * (d - 1), 16), lanes] = band.astype(BF16)

    def start(g, t, which):
        for s, turn in ((1, col < 2), (0, has[0]), (1, jnp.logical_and(col >= 2, has[1]))):
            @pl.when(jnp.logical_and(turn, jnp.logical_not(detour[s])))
            def _():
                for i in which:
                    message(g, s, t, i).start()

            @pl.when(jnp.logical_and(turn, detour[s]))
            def _():
                for i in which:
                    (message if i == 0 else message_out)(g, s, t, i).start()

    def fwd_rows(g):
        rows = pl.multiple_of((SUB - MARGIN) * SUB * (1 - row), 128)
        return pltpu.make_async_remote_copy(e_v.at[g, pl.ds(rows, 128)], e_v.at[g, pl.ds(ROWS_AT, 128)],
                                            sf_sem.at[g, 0], rf_sem.at[g, 0], device_id=partner, device_id_type=MESH)

    def fwd_corners(g):
        rows = pl.multiple_of(COLS_AT + HALF_COLS * closer, 32)
        return pltpu.make_async_remote_copy(e_v.at[g, pl.ds(rows, HALF_COLS)], e_v.at[g, pl.ds(CORN_AT, HALF_COLS)],
                                            sf_sem.at[g, 1], rf_sem.at[g, 1], device_id=partner, device_id_type=MESH)

    def assemble(g, sent, first, half, parts):
        slot = mod(sent, 2)
        j = 0 if half is closer else 1
        j_rows = pl.ds(16 * j, 16)
        for s in range(2):
            @pl.when(has[s])
            def _():
                for i in parts:
                    message(g, 1 - s, sent, i).wait_recv()
                rows = pl.ds(pl.multiple_of(16 * half, 16), 16)
                e_rows = pl.ds(SUB + 48 * j, 48)
                at = pl.multiple_of(CELLS // 2 * half, CELLS // 2)
                e_at = pl.multiple_of(COLS_AT + STEPS * 16 * s + HALF_COLS * half, 16)
                cells = pl.ds(at + edge_col[s], 16, stride=SUB)
                zcells = pl.ds(PAD + at + edge_col[s], 16, stride=SUB)
                coeff = (cedge if first else cedge_om)[s, rows]
                for t in range(TILES):
                    k = g * TILES + t
                    lanes = pl.ds(t * LANES, LANES)
                    if first:
                        theirs = recv_u[slot, g, s, rows, lanes]
                    else:
                        theirs = recv_b[slot, g, s, j_rows, lanes].astype(F32)
                    flux = coeff * (zf[k, zcells, :] - theirs)
                    own = res[k, cells, :] - flux
                    res[k, cells, :] = own
                    e_v[g, pl.ds(e_at, 16), lanes] = own.astype(BF16)
                    e_v[g, pl.ds(e_at + 16, 16), lanes] = (recv_p[slot, g, s, j_rows, lanes] + flux).astype(BF16)
                    e_v[g, pl.ds(e_at + 32, 48), lanes] = recv_b[slot, g, s, e_rows, lanes]

    def assemble_closer(g, sent, first):
        assemble(g, sent, first, closer, (5 if first else 0, 2, 1))
        fwd_corners(g).start()

    def assemble_far(g, sent, first):
        assemble(g, sent, first, far, (4, 3))

    def pack(g):
        def one_row(q, carry):
            rows = pl.ds(pl.multiple_of(q * SUB, SUB), SUB)
            for t in range(TILES):
                k = g * TILES + t
                e_v[g, rows, pl.ds(t * LANES, LANES)] = (keep * res[k, rows]).astype(BF16)
            return carry

        lax.fori_loop(0, SUB, one_row, 0, unroll=4)
        fwd_rows(g).start()

    def solve_own(g, scaled):
        def rows_of(m, carry):
            rows = pl.ds(pl.multiple_of(m * (CELLS // 2), CELLS // 2), CELLS // 2)
            acc[g, rows] = jnp.dot(mat_p[rows, :COLS_AT], e_v[g, pl.ds(0, COLS_AT)], preferred_element_type=F32)
            for t in range(TILES):
                k = g * TILES + t
                z = zf[k, pl.ds(pl.multiple_of(PAD + m * (CELLS // 2), PAD), CELLS // 2)]
                u_v[k, rows] = u_v[k, rows] + om * z if scaled else z
            return carry

        lax.fori_loop(0, 2, rows_of, 0)

    def solve_rest(g):
        fwd_rows(g).wait()
        fwd_corners(g).wait()
        acc[g] += jnp.dot(mat_p[:, COLS_AT:], e_v[g, pl.ds(COLS_AT, DEPTH - COLS_AT)], preferred_element_type=F32)

    def round_row(g):
        for t in range(TILES):
            zrow_s[g, t] = acc[g, brows, pl.ds(t * LANES, LANES)].astype(BF16).astype(F32)

    def update(g):
        def rows_of(q, carry):
            rows = pl.ds(pl.multiple_of(q * 64, 64), 64)
            for t in range(TILES):
                k = g * TILES + t
                z = acc[g, rows, pl.ds(t * LANES, LANES)].astype(BF16).astype(F32)
                zf[k, pl.ds(pl.multiple_of(PAD + q * 64, PAD), 64)] = z
            return carry

        lax.fori_loop(0, CELLS // 64, rows_of, 0)

    for k in range(groups * TILES):
        zf[k, pl.ds(0, PAD)] = zero_row
        zf[k, pl.ds(PAD + CELLS, PAD)] = zero_row
    for g in range(groups):
        e_v[g, pl.ds(COLS_AT, ROWS_AT - COLS_AT)] = jnp.zeros((ROWS_AT - COLS_AT, GROUP), BF16)
        e_v[g, pl.ds(CORN_AT, DEPTH - CORN_AT)] = jnp.zeros((DEPTH - CORN_AT, GROUP), BF16)
    keep = (1.0 - jnp.where(jnp.logical_and(sub_id == 0, has[0]), 1.0, 0.0)
            - jnp.where(jnp.logical_and(sub_id == SUB - 1, has[1]), 1.0, 0.0))

    krow_copy().wait()
    rows_b = pl.ds(pl.multiple_of(PAD + brow * SUB, SUB), SUB)
    crow[0] = 0.5 * (kb[rows_b] + krow_r[...])
    crow[1] = om * crow[0]

    def send_bands(g, t, scaled):
        stencil(g, scaled)
        zrow_copy(g).wait()
        row_fix(g, scaled)
        fill_half(g, closer)
        start(g, t, (2, 1))
        fill_half(g, far)
        start(g, t, (4, 3))

    for g in range(groups):
        for t in range(TILES):
            loads[g * TILES + t][0].wait()
        for t in range(TILES):
            zrow_s[g, t] = zf[g * TILES + t, rows_b]
        zrow_copy(g).start()
        fill_u(g)
        start(g, 0, (5,))
        for t in range(TILES):
            loads[g * TILES + t][1].wait()
        if g == 0:
            for a, b in loads[TILES:]:
                a.start()
                b.start()
            mat_copy.start()
        send_bands(g, 0, 0)

    def finish(g, scaled):
        pack(g)
        solve_own(g, scaled)

    mat_copy.wait()
    for at in range(0, EXT * EXT, 256):
        span = pl.ds(at, min(256, EXT * EXT - at))
        mat_t[:, span] = mat_v[span].T

    def place(at, width, start, window, source, ok=None, add=False):
        n = lax.broadcasted_iota(jnp.int32, (window, width), 1)
        k = lax.broadcasted_iota(jnp.int32, (window, width), 0) + start
        pick = source(n) == k
        if ok is not None:
            pick = jnp.logical_and(pick, ok(n))
        pick = jnp.where(pick, 1.0, 0.0).astype(BF16)

        wide[:, pl.ds(0, width)] = jnp.dot(mat_t[:, pl.ds(start, window)], pick, preferred_element_type=F32)
        placed = wide[:, pl.ds(0, width)].astype(BF16)
        if add:
            overlap = pl.ds(at, add)
            mat_p[:, overlap] = mat_p[:, overlap] + placed[:, :add]
            mat_p[:, pl.ds(at + add, width - add)] = placed[:, add:]
        else:
            mat_p[:, pl.ds(at, width)] = placed

    for q in range(4):
        low = (320 * q + 164) // 128 * 128
        high = -(-(320 * q + 476) // 128) * 128
        place(256 * q, 256, low, high - low, lambda n, q=q: own_source(n + 256 * q))

    pass_on(0, 0, FIRST_PARTS)
    finish(0, 0)

    def column(half):
        def source(n):
            r, c = column_source(n + 128 * half - HALF_COLS * half)
            return (MARGIN + 16 * half + r) * EXT + c
        return source

    place(COLS_AT, 256, 128, 768, column(0), lambda n: n < HALF_COLS)
    place(COLS_AT + 128, 256, 768, 768, column(1),
          lambda n: jnp.logical_and(n >= HALF_COLS - 128, n < 2 * HALF_COLS - 128), add=128)
    pass_on(1, 0, FIRST_PARTS)

    def halo(n):
        first_row = jnp.where(row == 0, MARGIN + SUB, 0)
        r, c = column_source(n - 128)
        corner_row = jnp.where(row == 0, MARGIN + SUB, -12) + r
        return jnp.where(n < 128, (first_row + (n >> 5)) * EXT + MARGIN + (n & 31), corner_row * EXT + c)

    def halo_ok(n):
        r = n & 15
        corner = jnp.logical_and(n < 128 + HALF_COLS, jnp.where(row == 0, r, 15 - r) < MARGIN)
        return jnp.logical_or(n < 128, corner)

    place(ROWS_AT, 384, pl.multiple_of(1408 * (1 - row), 128), 192, halo, halo_ok)

    for s in range(2):
        @pl.when(has[s])
        def _():
            kcol_copy(1 - s).wait_recv()
            cedge[s] = 0.5 * (kcol_s[s] + kcol_r[s])
            cedge_om[s] = om * cedge[s]
            kcol_copy(s).wait_send()

    def wait_sends(g, which):
        for s in range(2):
            @pl.when(has[s])
            def _():
                for i in which:
                    message(g, s, 0, i).wait_send()

        @pl.when(is_via)
        def _():
            for i in which:
                if i != 0:
                    message_on(g, 0, i).wait_send()

    def advance(g, t, first, relay):
        if relay is not None:
            pass_on(relay[0], relay[1], (2, 1))
        solve_rest(g)
        round_row(g)
        zrow_copy(g).start()
        update(g)
        wait_sends(g, FIRST_PARTS if first else SWEEP_PARTS)
        fill_z(g)
        start(g, t, (0,))
        if relay is not None:
            pass_on(relay[0], relay[1], (4, 3))
        send_bands(g, t, 1)

    assemble_closer(0, 0, True)
    finish(1, 0)
    assemble_far(0, 0, True)
    advance(0, 1, True, None)
    assemble_closer(1, 0, True)
    finish(0, 1)
    assemble_far(1, 0, True)
    advance(1, 1, True, (0, 1))

    def step(i, carry):
        t = i // groups
        g = lax.rem(i, groups)
        assemble_closer(g, t - 1, False)
        finish(1 - g, 1)
        assemble_far(g, t - 1, False)
        advance(g, t, False, (1 - g, jnp.where(g == 0, t - 1, t)))
        return carry

    lax.fori_loop(2 * groups, SWEEPS * groups, step, 0)

    u_copies = [pltpu.make_async_copy(u_v.at[k], u_out.at[:, pl.ds(k * LANES, LANES)], in_sem.at[0, k])
                for k in range(groups * TILES)]
    z_copies = [pltpu.make_async_copy(z_v.at[g], z_out.at[:, pl.ds(g * GROUP, GROUP)], out_sem.at[g])
                for g in range(groups)]
    for g in range(groups):
        for t in range(TILES):
            if g == 0:
                u_copies[t].start()
        assemble_closer(g, SWEEPS - 1, False)
        if g == 0:
            finish(1, 1)
            for t in range(TILES):
                u_copies[TILES + t].start()
        assemble_far(g, SWEEPS - 1, False)
        if g == 0:
            pass_on(1, SWEEPS - 1, (2, 1))
        solve_rest(g)
        z_v[g] = acc[g].astype(BF16)
        z_copies[g].start()
        if g == 0:
            pass_on(1, SWEEPS - 1, (4, 3))
    for g in range(groups):
        wait_sends(g, SWEEP_PARTS)
    for c in u_copies + z_copies:
        c.wait()


def solution(mesh):
    col_count = mesh.shape['col']
    grid_spec = P('row', 'col', None)

    def device_fn(f_blk, u_blk, kappa_blk, mat_blk, omega_relax):
        rhs_count = u_blk.shape[2]
        groups = rhs_count // GROUP
        tiles = rhs_count // LANES
        vm = pltpu.VMEM
        dma = pltpu.SemaphoreType.DMA
        u_last, z_last = pl.pallas_call(
            functools.partial(kernel, groups, col_count),
            out_shape=(jax.ShapeDtypeStruct((CELLS, rhs_count), F32), jax.ShapeDtypeStruct((CELLS, rhs_count), BF16)),
            in_specs=[pl.BlockSpec(memory_space=pltpu.HBM), pl.BlockSpec(memory_space=pltpu.HBM),
                      pl.BlockSpec(memory_space=pltpu.VMEM), pl.BlockSpec(memory_space=pltpu.HBM),
                      pl.BlockSpec(memory_space=pltpu.SMEM)],
            out_specs=(pl.BlockSpec(memory_space=pl.ANY), pl.BlockSpec(memory_space=pl.ANY)),
            scratch_shapes=[
                vm((EXT * EXT, CELLS), BF16),
                vm((CELLS, EXT * EXT), BF16),
                vm((CELLS, DEPTH), BF16),
                vm((CELLS, 384), F32),
                vm((groups, CELLS, GROUP), F32),
                vm((tiles, CELLS, LANES), F32),
                vm((tiles, CELLS + 2 * PAD, LANES), F32),
                vm((tiles, CELLS, LANES), F32),
                vm((groups, DEPTH, GROUP), BF16),
                vm((groups, CELLS, GROUP), BF16),
                vm((CELLS + 2 * PAD, LANES), F32),
                vm((2, 5, CELLS, LANES), F32),
                vm((2, SUB, LANES), F32),
                vm((2, SUB, LANES), F32),
                vm((2, SUB, LANES), F32),
                vm((groups, 2, SUB, GROUP), F32),
                vm((groups, 2, 128, GROUP), BF16),
                vm((groups, 2, SUB, GROUP), F32),
                vm((2, groups, 2, SUB, GROUP), F32),
                vm((2, groups, 2, 128, GROUP), BF16),
                vm((1, groups, 2, SUB, GROUP), F32),
                vm((groups, TILES, SUB, LANES), F32),
                vm((groups, TILES, SUB, LANES), F32),
                vm((2, SUB, LANES), F32),
                vm((2, SUB, LANES), F32),
                vm((SUB, LANES), F32),
                vm((3, groups, SUB, GROUP), F32),
                vm((3, groups, 128, GROUP), BF16),
                vm((1, groups, SUB, GROUP), F32),
                dma((2, tiles)), dma, dma((groups,)),
                dma((groups, 2, 6)), dma((2, groups, 2, 6)),
                dma((groups,)), dma((groups,)),
                dma((groups, 2)), dma((groups, 2)),
                dma((3,)), dma((3,)),
                dma((groups, 6)), dma((3, groups, 6)),
            ],
            compiler_params=pltpu.CompilerParams(collective_id=0, has_side_effects=True,
                                                 vmem_limit_bytes=50 * 1024 * 1024),
        )(f_blk.reshape(CELLS, rhs_count), u_blk.reshape(CELLS, rhs_count), kappa_blk,
          mat_blk.reshape(CELLS, EXT * EXT).T, omega_relax.reshape(1))
        return (u_last + omega_relax * z_last.astype(F32)).reshape(SUB, SUB, rhs_count)

    return jax.shard_map(device_fn, mesh=mesh,
                         in_specs=(grid_spec, grid_spec, P('row', 'col'), P('row', 'col', None, None), P()),
                         out_specs=grid_spec, check_vma=False)
```
